256 devices in a mesh: gx: 4 (over x_lo, core), gy: 16 (over z, x_hi), gz: 4 (over y).
Axes of the slice: x: 4 (x_hi: 2, x_lo: 2; x = x_hi * 2 + x_lo), y: 4, z: 8, core: 2. Of those that a mesh axis runs over, the one named last changes fastest.
Arguments:
- fields: float32 [5, 64, 128, 512], P(None, 'gz', 'gy', 'gx'), may hold values from -4 to 4
- radius: float32 [8, 64, 128, 512], P(None, 'gz', 'gy', 'gx'), may hold values from 0.4 to 1.5
- weight: float32 [8, 64, 128, 512], P(None, 'gz', 'gy', 'gx'), may hold values from 0.05 to 0.5
- column: int32 [8, 64, 128, 512], P(None, 'gz', 'gy', 'gx'), may hold values from 0 to 127
- counts: int32 [64, 128, 512], P('gz', 'gy', 'gx'), may hold values from 1 to 8
- fall_depth: int32 [8, 64, 128, 4], P(None, 'gz', 'gy', 'gx'), may hold values from 0 to 8, as said below
Outputs:
- new_fields: float32 [5, 64, 128, 512], P(None, 'gz', 'gy', 'gx')
- moments: float32 [3, 64, 128, 512], P(None, 'gz', 'gy', 'gx')
The draws below stay inside these ranges and needn't reach their ends.
Inputs may be any that keep to these rules, and one draw needn't show every extreme that they name: The droplet in slot s of cell (k, j, i) sits in x cell (i // 128) * 128 + column[s, k, j, i]. Slots s < counts[k, j, i] hold live droplets. The droplets of slot s in cells (k, j, b * 128) to (k, j, (b + 1) * 128 - 1) fall together by fall_depth[s, k, j, b] levels, never below the lowest level: fall_depth[s, k, j, b] <= k; 8 is reached in every draw.
All inputs are finite; a program needn't handle non-finite values. Where the reference program divides by a largest or mean magnitude, that divisor is 1e-20 or more.
Results may differ from the reference program's by a relative error of at most 0.00021.
Values sent between devices are 32-bit elements; how exact they have to be, the bound alone decides.
No kernel may reach another device: no remote copies, remote signals or barrier semaphores. Data moves between devices by JAX's collectives and lax.ppermute only.
A program may use at most 64 MiB of HBM per device.

```python
import math
import jax
import jax.numpy as jnp
from jax import lax

CX = 128
SLOTS = 8
NS = 4
FMAX = 8
NX = 512
NY = 128
NZ = 64
XBLOCKS = 4


def draw_fall_depth(key, part):
    drawn = jax.random.randint(key, (SLOTS, NZ, NY, XBLOCKS), 0, FMAX + 1, dtype=jnp.int32)
    drawn = drawn.at[0, NZ - 1, 0, 0].set(FMAX)
    levels = jnp.arange(NZ, dtype=jnp.int32)[None, :, None, None]
    return jnp.minimum(drawn, levels).astype(jnp.int32)


def set_ends(values, own_key, least, largest):
    shape = values.shape
    index_at = [jax.random.randint(jax.random.fold_in(own_key, axis), (), 0, shape[axis]) for axis in range(len(shape))]
    values = values.at[tuple(index_at)].set(least)
    longest = shape.index(max(shape))
    index_at[longest] = (index_at[longest] + 1) % shape[longest]
    return values.at[tuple(index_at)].set(largest)


def shard_levels(key, shape, cuts, smallest, high):
    loudness = 1.0
    for position, shards_of in cuts:
        steps = jax.random.uniform(jax.random.fold_in(jax.random.fold_in(key, 6), position), (shards_of,), jnp.float32, smallest / len(cuts), high / len(cuts))
        loudness = loudness * jnp.repeat(jnp.exp(steps), shape[position] // shards_of).reshape((-1,) + (1,) * (len(shape) - 1 - position))
    return loudness


def centred(rng, dims, spread, reach, cuts=(), held_as=jnp.bfloat16):
    entries = spread * jax.random.normal(rng, dims, jnp.float32)
    if cuts:
        entries = entries * shard_levels(rng, dims, cuts, -0.22, 0.18)
    return jnp.clip(entries, -reach, reach).astype(held_as)


def setup_inputs(seed: int = 0) -> dict:
    splits = jax.random.split(jax.random.key(seed), 7)
    fields = centred(splits[0], (5, NZ, NY, NX), 0.5, 4.0, ((1, 4), (2, 16), (3, 4)), jnp.float32)
    radius = jnp.clip(jnp.exp(math.log(1.5) - 1.3217558 * jax.random.uniform(splits[1], (SLOTS, NZ, NY, NX), jnp.float32) ** shard_levels(splits[1], (SLOTS, NZ, NY, NX), ((1, 4), (2, 16), (3, 4)), -0.2, 0.2)), 0.4, 1.5)
    weight = jnp.clip(jnp.exp(math.log(0.5) - 2.3025851 * jax.random.uniform(splits[2], (SLOTS, NZ, NY, NX), jnp.float32) ** shard_levels(splits[2], (SLOTS, NZ, NY, NX), ((1, 4), (2, 16), (3, 4)), -0.2, 0.2)), 0.05, 0.5)
    column = set_ends(jax.random.randint(splits[3], (SLOTS, NZ, NY, NX), 0, CX), jax.random.fold_in(splits[3], 1), 0, CX - 1).astype(jnp.int32)
    counts = set_ends(jax.random.randint(splits[4], (NZ, NY, NX), 1, SLOTS + 1), jax.random.fold_in(splits[4], 1), 1, SLOTS).astype(jnp.int32)
    fall_depth = draw_fall_depth(jax.random.fold_in(splits[6], 71), 0)
    return dict(fields=fields, radius=radius, weight=weight, column=column, counts=counts, fall_depth=fall_depth)


sound_speed = 10.0
buoyancy = 0.5
courant_goal = 0.6
growth = 0.3

def window(padded, margin, direction, offset, length):
    cut = []
    for dimension in range(3):
        if dimension == direction:
            cut.append(slice(margin + offset, margin + offset + length))
        else:
            cut.append(slice(margin, padded.shape[dimension] - margin))
    return padded[tuple(cut)]

def advect(quantity, margin, wind_pad, wind_margin):
    tendency = jnp.zeros(tuple((quantity.shape[dimension] - 2 * margin for dimension in range(3))), jnp.float32)
    for direction in range(3):
        cells_along = quantity.shape[direction] - 2 * margin
        stencil = [window(quantity, margin, direction, offset - 1, cells_along + 1) for offset in range(-2, 4)]
        face_wind = window(wind_pad[2 - direction], wind_margin, direction, -1, cells_along + 1)
        central = 37.0 * (stencil[2] + stencil[3]) - 8.0 * (stencil[1] + stencil[4]) + (stencil[0] + stencil[5])
        upwind = 10.0 * (stencil[3] - stencil[2]) - 5.0 * (stencil[4] - stencil[1]) + (stencil[5] - stencil[0])
        face_flux = (face_wind * central - jnp.abs(face_wind) * upwind) / 60.0
        upper_flux = lax.slice_in_dim(face_flux, 1, cells_along + 1, axis=direction)
        lower_flux = lax.slice_in_dim(face_flux, 0, cells_along, axis=direction)
        tendency = tendency - (upper_flux - lower_flux)
    return tendency

def extend(fields, margin):
    fields = jnp.pad(fields, ((0, 0), (margin, margin), (0, 0), (0, 0)))
    return jnp.pad(fields, ((0, 0), (0, 0), (margin, margin), (margin, margin)), mode='wrap')

def acoustic(fast_fields, lift_term, pressure_rate, sub_step, lid_mask):
    grid_levels, grid_rows, grid_cols = (fast_fields.shape[1], fast_fields.shape[2], fast_fields.shape[3])
    pressure_pad = extend(fast_fields[0:1], 1)[0]
    pressure = fast_fields[0]
    east_wind = fast_fields[1] - sub_step * sound_speed * (window(pressure_pad, 1, 2, 1, grid_cols) - pressure)
    north_wind = fast_fields[2] - sub_step * sound_speed * (window(pressure_pad, 1, 1, 1, grid_rows) - pressure)
    vertical_wind = (fast_fields[3] + sub_step * (lift_term - sound_speed * (window(pressure_pad, 1, 0, 1, grid_levels) - pressure))) * lid_mask
    wind_halo = extend(jnp.stack([east_wind, north_wind, vertical_wind]), 1)
    divergence = east_wind - window(wind_halo[0], 1, 2, -1, grid_cols) + (north_wind - window(wind_halo[1], 1, 1, -1, grid_rows)) + (vertical_wind - window(wind_halo[2], 1, 0, -1, grid_levels))
    pressure = pressure + sub_step * (pressure_rate - sound_speed * divergence)
    return jnp.stack([pressure, east_wind, north_wind, vertical_wind])

def reference(fields, radius, weight, column, counts, fall_depth):
    grid_levels, grid_rows, grid_cols = (fields.shape[1], fields.shape[2], fields.shape[3])
    lid_mask = (jnp.arange(grid_levels, dtype=jnp.int32) < grid_levels - 1).astype(jnp.float32)[:, None, None]
    initial = jnp.concatenate([fields[0:4], (fields[4] * lid_mask)[None]])
    top_speed = jnp.max(jnp.abs(initial[2]) + jnp.abs(initial[3]) + jnp.abs(initial[4]))
    time_step = courant_goal / (1.0 + top_speed)
    current = initial
    for fraction, substeps in ((1.0 / 3.0, 1), (0.5, NS // 2), (1.0, NS)):
        padded = extend(current, 3)
        tracer_rate = advect(padded[0], 3, padded[2:5], 3)
        pressure_rate = advect(padded[1], 3, padded[2:5], 3)
        lift_term = buoyancy * 0.5 * (window(padded[0], 3, 0, 0, grid_levels) + window(padded[0], 3, 0, 1, grid_levels)) * lid_mask
        sub_step = fraction * time_step / substeps
        fast_fields = initial[1:5]
        for repeat in range(substeps):
            fast_fields = acoustic(fast_fields, lift_term, pressure_rate, sub_step, lid_mask)
        tracer = initial[0] + fraction * time_step * tracer_rate
        current = jnp.concatenate([tracer[None], fast_fields])
    tracer = current[0]
    block_start = jnp.arange(grid_cols, dtype=jnp.int32) // CX * CX
    levels = jnp.arange(grid_levels, dtype=jnp.int32)[:, None, None]
    row_index = jnp.arange(grid_rows, dtype=jnp.int32)[None, :, None]
    moments = jnp.zeros((3, grid_levels * grid_rows * grid_cols), jnp.float32)
    for slot_index in range(SLOTS):
        cell_column = (block_start[None, None, :] + column[slot_index]).astype(jnp.int32)
        near_tracer = jnp.take_along_axis(tracer, cell_column, axis=2)
        squared = radius[slot_index] * radius[slot_index] * jnp.exp(growth * near_tracer)
        number = weight[slot_index] * (slot_index < counts).astype(jnp.float32)
        area_term = number * squared
        mass_term = area_term * jnp.sqrt(squared)
        fall_cells = jnp.repeat(fall_depth[slot_index], CX, axis=2).astype(jnp.int32)
        flat_index = (((levels - fall_cells) * grid_rows + row_index) * grid_cols + cell_column).astype(jnp.int32)
        moments = moments.at[:, flat_index.reshape(-1)].add(jnp.stack([number, area_term, mass_term]).reshape(3, -1))
    return (current, moments.reshape(3, grid_levels, grid_rows, grid_cols))
```

```python
import jax
import jax.numpy as jnp
from jax import lax
from jax.experimental import pallas as pl
from jax.experimental.pallas import tpu as pltpu
from jax.sharding import PartitionSpec as P

NS = 4
FMAX = 8
GRID_AXES = ("gx", "gy", "gz")

sound_speed = 10.0
buoyancy = 0.5
courant_goal = 0.6
growth = 0.3

LEVELS, ROWS, COLS = 16, 8, 128
TALL, WIDE = 24, 256
REACH = 7
DEPTH = LEVELS + 2 * REACH
EDGE = 8
F32 = jnp.float32
ANY = pltpu.VMEM


def lanes(shape):
    return lax.broadcasted_iota(jnp.int32, shape, len(shape) - 1)


def pack_columns(own, above, below, to_left, to_right):
    blocks = (own, above, below)
    lane = lanes((ROWS, COLS))

    def one(k, _):
        left = jnp.zeros((ROWS, COLS), F32)
        right = jnp.zeros((ROWS, COLS), F32)
        for tile in range(3):
            for field in range(5):
                start = tile * 40 + field * EDGE
                here = (lane >= start) & (lane < start + EDGE)
                value = blocks[tile][field, k]
                first = pltpu.roll(value, start, 1) if start else value
                last = pltpu.roll(value, (start + EDGE) % COLS, 1)
                left = jnp.where(here, first, left)
                right = jnp.where(here, last, right)
        to_left[k] = left
        to_right[k] = right
        return 0

    lax.fori_loop(0, LEVELS, one, 0)


def halo_columns(from_right, from_left, tile, field):
    start = tile * 40 + field * EDGE
    right = pltpu.roll(from_right, COLS - start, 1) if start else from_right
    left = pltpu.roll(from_left, (COLS - EDGE - start) % COLS, 1)
    return jnp.where(lanes((ROWS, COLS)) < COLS // 2, right, left)


def pack_levels(reach):
    def kernel(own, above, below, from_right, from_left, to_down, to_up):
        for a in range(reach):
            for out, k in ((to_down, a), (to_up, LEVELS - reach + a)):
                for tile, block in enumerate((own, above, below)):
                    for field in range(5):
                        out[a, field * 3 + tile] = block[field, k]
                out[a, 15] = from_right[k]
                out[a, 16] = from_left[k]

    return kernel


def assemble(refs, ext, reach, place, last):
    own, above, below, from_right, from_left, from_up, from_down = refs
    blocks = (own, above, below)

    def middle(k, _):
        right, left = from_right[k], from_left[k]
        for field in range(5):
            for tile in range(3):
                at = pl.ds(tile * ROWS, ROWS)
                ext[field, REACH + k, at, 0:COLS] = blocks[tile][field, k]
                ext[field, REACH + k, at, COLS:WIDE] = halo_columns(right, left, tile, field)
        return 0

    lax.fori_loop(0, LEVELS, middle, 0)
    for message, first, there in (
        (from_down, REACH - reach, place > 0),
        (from_up, REACH + LEVELS, place < last),
    ):
        keep = jnp.where(there, 1.0, 0.0).astype(F32)

        def outer(a, _, message=message, first=first, keep=keep):
            right, left = message[a, 15], message[a, 16]
            for field in range(5):
                for tile in range(3):
                    at = pl.ds(tile * ROWS, ROWS)
                    ext[field, first + a, at, 0:COLS] = message[a, field * 3 + tile] * keep
                    ext[field, first + a, at, COLS:WIDE] = (
                        halo_columns(right, left, tile, field) * keep
                    )
            return 0

        lax.fori_loop(0, reach, outer, 0)


def shift(value, by, axis):
    return pltpu.roll(value, (-by) % value.shape[axis], axis)


def face_flux(q, wind):
    central = 37.0 * (q[2] + q[3]) - 8.0 * (q[1] + q[4]) + (q[0] + q[5])
    upwind = 10.0 * (q[3] - q[2]) - 5.0 * (q[4] - q[1]) + (q[5] - q[0])
    return wind * central - jnp.abs(wind) * upwind


def flat_flux(q, wind, axis):
    flux = face_flux([shift(q, by, axis) if by else q for by in range(-2, 4)], wind)
    return flux - shift(flux, -1, axis)


def level_flux(read, wind, l):
    return face_flux([read(l + by) for by in range(-2, 4)], wind)


def in_domain(l, place, last, lid):
    g = place * LEVELS + l - REACH
    top = (last + 1) * LEVELS - (1 if lid else 0)
    return jnp.where((g >= 0) & (g < top), 1.0, 0.0).astype(F32)


def first_rates(
    place_ref, own, above, below, from_right, from_left, from_up, from_down, ext, rate
):
    place, last = place_ref[0], place_ref[1]
    assemble(
        (own, above, below, from_right, from_left, from_up, from_down), ext, REACH, place, last
    )

    @pl.when(place == last)
    def _():
        ext[4, REACH + LEVELS - 1] = jnp.zeros((TALL, WIDE), F32)

    read_c = lambda l: ext[0, l]
    read_p = lambda l: ext[1, l]

    def one(l, carry):
        low_c, low_p = carry
        u, v, w = ext[2, l], ext[3, l], ext[4, l]
        high_c = level_flux(read_c, w, l)
        high_p = level_flux(read_p, w, l)
        c, p = ext[0, l], ext[1, l]
        rate[0, l] = -(flat_flux(c, u, 1) + flat_flux(c, v, 0) + (high_c - low_c)) / 60.0
        rate[1, l] = -(flat_flux(p, u, 1) + flat_flux(p, v, 0) + (high_p - low_p)) / 60.0
        return high_c, high_p

    start = REACH - 4
    w = ext[4, start - 1]
    lax.fori_loop(
        start,
        REACH + LEVELS + 4,
        one,
        (level_flux(read_c, w, start - 1), level_flux(read_p, w, start - 1)),
    )


def acoustic(p, u, v, w, read_c, rate, step, first, count, place, last, out=None):
    pull = step * sound_speed

    def wind_w(l, p_here):
        lift = (buoyancy * 0.5) * (read_c(l) + read_c(l + 1))
        return (w[0](l) + step * lift - pull * (p[0](l + 1) - p_here)) * in_domain(
            l, place, last, True
        )

    def one(l, w_low):
        p_here = p[0](l)
        w_new = wind_w(l, p_here)
        u_new = u[0](l) - pull * (shift(p_here, 1, 1) - p_here)
        v_new = v[0](l) - pull * (shift(p_here, 1, 0) - p_here)
        divergence = (
            (u_new - shift(u_new, -1, 1)) + (v_new - shift(v_new, -1, 0)) + (w_new - w_low)
        )
        p_new = (p_here + step * rate(l) - pull * divergence) * in_domain(l, place, last, False)
        p[1](l, p_new)
        u[1](l, u_new)
        v[1](l, v_new)
        w[1](l, w_new)
        return w_new

    w_low = wind_w(first - 1, p[0](first - 1))
    w[1](first - 1, w_low)
    lax.fori_loop(first, first + count, one, w_low)


def access(ref, *lead):
    def read(l):
        return ref[(*lead, l)]

    def write(l, value):
        ref[(*lead, l)] = value

    return read, write


def own_write(ref, field):
    def write(l, value):
        if not isinstance(l, int):
            ref[field, l - REACH] = value[0:ROWS, 0:COLS]

    return write


def tracer_rate(ext, l, low):
    c_all, v = ext[0, l], ext[3, l]
    rows = flat_flux(c_all[:, 0:COLS], v[:, 0:COLS], 0)[0:ROWS]
    cols = flat_flux(ext[0, l, 0:ROWS, :], ext[2, l, 0:ROWS, :], 1)[:, 0:COLS]
    high = tracer_high(ext, l)
    return -(rows + cols + (high - low)) / 60.0, high


def tracer_high(ext, l):
    return level_flux(lambda m: ext[0, m, 0:ROWS, 0:COLS], ext[4, l, 0:ROWS, 0:COLS], l)


def pressure_rates(ext, rate, first, count):
    read_p = lambda l: ext[1, l]

    def one(l, low):
        p = ext[1, l]
        high = level_flux(read_p, ext[4, l], l)
        rate[l] = -(flat_flux(p, ext[2, l], 1) + flat_flux(p, ext[3, l], 0) + (high - low)) / 60.0
        return high

    lax.fori_loop(first, first + count, one, level_flux(read_p, ext[4, first - 1], first - 1))


def two_sections(place_ref, speed, start, rate0, s2, dt_out, s1, rate1, fast):
    place, last = place_ref[0], place_ref[1]
    dt = courant_goal / (1.0 + jnp.max(speed[...]))
    dt_out[0] = dt
    third = dt * (1.0 / 3.0)

    def tracer(l, _):
        s1[0, l] = (start[0, l] + third * rate0[0, l]) * in_domain(l, place, last, False)
        return 0

    lax.fori_loop(REACH - 4, REACH + LEVELS + 4, tracer, 0)
    acoustic(
        (access(start, 1)[0], access(s1, 1)[1]),
        (access(start, 2)[0], access(s1, 2)[1]),
        (access(start, 3)[0], access(s1, 3)[1]),
        (access(start, 4)[0], access(s1, 4)[1]),
        access(start, 0)[0],
        access(rate0, 1)[0],
        third,
        REACH - 4,
        LEVELS + 8,
        place,
        last,
    )
    half = dt * 0.5

    def own_tracer(l, low):
        tendency, high = tracer_rate(s1, l, low)
        s2[0, l - REACH] = start[0, l, 0:ROWS, 0:COLS] + half * tendency
        return high

    lax.fori_loop(REACH, REACH + LEVELS, own_tracer, tracer_high(s1, REACH - 1))
    pressure_rates(s1, rate1, REACH - 1, LEVELS + 2)
    step = half / (NS // 2)
    acoustic(
        (access(start, 1)[0], access(fast, 0)[1]),
        (access(start, 2)[0], access(fast, 1)[1]),
        (access(start, 3)[0], access(fast, 2)[1]),
        (access(start, 4)[0], access(fast, 3)[1]),
        access(s1, 0)[0],
        access(rate1)[0],
        step,
        REACH - 1,
        LEVELS + 2,
        place,
        last,
    )
    acoustic(
        (access(fast, 0)[0], own_write(s2, 1)),
        (access(fast, 1)[0], own_write(s2, 2)),
        (access(fast, 2)[0], own_write(s2, 3)),
        (access(fast, 3)[0], own_write(s2, 4)),
        access(s1, 0)[0],
        access(rate1)[0],
        step,
        REACH,
        LEVELS,
        place,
        last,
    )


def last_tracer(
    place_ref,
    dt_ref,
    own,
    above,
    below,
    from_right,
    from_left,
    from_up,
    from_down,
    fields,
    by_depth,
    ext,
    tracer,
    landed,
    fallen,
    total,
):
    place, last = place_ref[0], place_ref[1]
    dt = dt_ref[0]
    assemble((own, above, below, from_right, from_left, from_up, from_down), ext, 6, place, last)
    total[...] = jnp.zeros(total.shape, F32)

    def one(l, low):
        k = l - REACH
        tendency, high = tracer_rate(ext, l, low)
        c = fields[0, k] + dt * tendency
        tracer[k] = c
        grown = jnp.exp(growth * c)
        weights = (None, grown, grown * jnp.exp((0.5 * growth) * c))
        for depth in range(FMAX + 1):
            for moment in range(3):
                value = by_depth[k, depth, moment]
                if moment:
                    value = value * weights[moment]
                total[moment, k + FMAX - depth] += value
        return high

    lax.fori_loop(REACH, REACH + LEVELS, one, tracer_high(ext, REACH - 1))
    landed[...] = total[:, FMAX:]
    fallen[...] = total[:, 0:FMAX]


def last_section(place_ref, dt_ref, ext, start, tracer, out, rate, fast):
    place, last = place_ref[0], place_ref[1]
    step = dt_ref[0] / NS
    pressure_rates(ext, rate, REACH - 3, LEVELS + 6)
    out[0] = tracer[...]
    for repeat in range(NS):
        reads = [access(start, f + 1)[0] if repeat == 0 else access(fast, f)[0] for f in range(4)]
        writes = [
            own_write(out, f + 1) if repeat == NS - 1 else access(fast, f)[1] for f in range(4)
        ]
        acoustic(
            (reads[0], writes[0]),
            (reads[1], writes[1]),
            (reads[2], writes[2]),
            (reads[3], writes[3]),
            access(ext, 0)[0],
            access(rate)[0],
            step,
            REACH - 3 + repeat,
            LEVELS + 6 - 2 * repeat,
            place,
            last,
        )


def deposit(radius, weight, column, counts, fall_depth, out):
    slots, levels = radius.shape[0], radius.shape[1]
    target = lax.broadcasted_iota(jnp.int32, (COLS, COLS), 0)
    row = lax.broadcasted_iota(jnp.int32, (ROWS, COLS), 0)
    per_step = 4

    for k in range(levels):
        out[k] = jnp.zeros(out.shape[1:], F32)
        live = counts[k]

        def some(step, _, k=k, live=live):
            sums = [[None] * 3 for _ in range(FMAX + 1)]
            for part in range(per_step):
                s = step * per_step + part
                r = radius[s, k]
                number = jnp.where(s < live, weight[s, k], 0.0)
                area = number * r * r
                terms = []
                for t in (number, area, area * r):
                    high = t.astype(jnp.bfloat16).astype(F32)
                    terms += [high, t - high]
                cols = column[s, k]
                left, right = [], []
                for j in range(ROWS):
                    left.append(
                        jnp.concatenate([jnp.where(row == j, t, 0.0) for t in terms], axis=0)
                    )
                    right.append(jnp.where(cols[j : j + 1] == target, 1.0, 0.0).astype(F32))
                sent = lax.dot_general(
                    jnp.concatenate(left, axis=1),
                    jnp.concatenate(right, axis=1),
                    (((1,), (1,)), ((), ())),
                    preferred_element_type=F32,
                )
                depth = jnp.broadcast_to(fall_depth[s, k], (ROWS, COLS))
                for d in range(FMAX + 1):
                    falls = depth == d
                    for m in range(3):
                        both = sent[16 * m : 16 * m + 8] + sent[16 * m + 8 : 16 * m + 16]
                        value = jnp.where(falls, both, 0.0)
                        sums[d][m] = value if sums[d][m] is None else sums[d][m] + value
            for d in range(FMAX + 1):
                for m in range(3):
                    out[k, d, m] += sums[d][m]
            return 0

        lax.fori_loop(0, slots // per_step, some, 0)


def vmem(n):
    return [pl.BlockSpec(memory_space=pltpu.VMEM)] * n


def smem(n):
    return [pl.BlockSpec(memory_space=pltpu.SMEM)] * n


def shaped(*dims):
    return jax.ShapeDtypeStruct(dims, F32)


PARAMS = pltpu.CompilerParams(vmem_limit_bytes=60 * 1024 * 1024)


def call(kernel, name, ins, outs, scratch=(), out_specs=None, flops=None):
    return pl.pallas_call(
        kernel,
        name=name,
        in_specs=ins,
        out_specs=tuple(out_specs or vmem(len(outs))),
        out_shape=tuple(outs),
        scratch_shapes=list(scratch),
        compiler_params=PARAMS,
        cost_estimate=(
            pl.CostEstimate(flops=flops, bytes_accessed=0, transcendentals=0) if flops else None
        ),
    )


def both_ways(value, axis, low=None):
    count = lax.axis_size(axis)
    down = [((i + 1) % count, i) for i in range(count)]
    up = [(i, (i + 1) % count) for i in range(count)]
    return (
        lax.ppermute(value, axis, down),
        lax.ppermute(value if low is None else low, axis, up),
    )


def exchange(block, reach, after_rows=None):
    above, below = both_ways(block, "gy")
    if after_rows is not None:
        above, below, after_rows = lax.optimization_barrier((above, below, after_rows))
    to_left, to_right = call(
        pack_columns, "pack_columns", vmem(3), [shaped(LEVELS, ROWS, COLS)] * 2
    )(block, above, below)
    from_right, from_left = both_ways(to_left, "gx", to_right)
    to_down, to_up = call(
        pack_levels(reach), "pack_levels", vmem(5), [shaped(reach, 17, ROWS, COLS)] * 2
    )(block, above, below, from_right, from_left)
    from_up, from_down = both_ways(to_down, "gz", to_up)
    return above, below, from_right, from_left, from_up, from_down


def top_speed(fields, place, last):
    w = fields[4] * (
        (jnp.arange(LEVELS) < LEVELS - 1) | (place != last)
    ).astype(F32)[:, None, None]
    local = jnp.max(jnp.abs(fields[2]) + jnp.abs(fields[3]) + jnp.abs(w))
    devices = lax.axis_size(GRID_AXES)
    everywhere = jnp.broadcast_to(local, (devices, 1, COLS))
    return lax.all_to_all(everywhere, GRID_AXES, 0, 0)


def per_device(fields, radius, weight, column, counts, fall_depth):
    place = lax.axis_index("gz")
    last = lax.axis_size("gz") - 1
    where = jnp.stack([place, jnp.int32(last)]).astype(jnp.int32)

    chunk = 2
    by_depth = []
    for n in range(LEVELS // chunk):
        by_depth.append(
            pl.pallas_call(
                deposit,
                name="deposit",
                grid=(1,),
                in_specs=[
                    pl.BlockSpec((8, chunk, ROWS, COLS), lambda i, n=n: (0, n, 0, 0)),
                    pl.BlockSpec((8, chunk, ROWS, COLS), lambda i, n=n: (0, n, 0, 0)),
                    pl.BlockSpec((8, chunk, ROWS, COLS), lambda i, n=n: (0, n, 0, 0)),
                    pl.BlockSpec((chunk, ROWS, COLS), lambda i, n=n: (n, 0, 0)),
                    pl.BlockSpec((8, chunk, ROWS, 1), lambda i, n=n: (0, n, 0, 0)),
                ],
                out_specs=pl.BlockSpec(
                    (chunk, FMAX + 1, 3, ROWS, COLS), lambda i: (0, 0, 0, 0, 0)
                ),
                out_shape=shaped(chunk, FMAX + 1, 3, ROWS, COLS),
                compiler_params=PARAMS,
                cost_estimate=pl.CostEstimate(
                    flops=200_000_000, bytes_accessed=0, transcendentals=0
                ),
            )(radius, weight, column, counts, fall_depth)
        )
    by_depth = jnp.concatenate(by_depth, axis=0)

    speed = top_speed(fields, place, last)
    halos = exchange(fields, REACH)
    start, rate0 = call(
        first_rates,
        "first_rates",
        smem(1) + vmem(7),
        [shaped(5, DEPTH, TALL, WIDE), shaped(2, DEPTH, TALL, WIDE)],
    )(where, fields, *halos)
    s2, dt = call(
        two_sections,
        "two_sections",
        smem(1) + vmem(3),
        [shaped(5, LEVELS, ROWS, COLS), shaped(1)],
        scratch=[
            pltpu.VMEM((5, DEPTH, TALL, WIDE), F32),
            pltpu.VMEM((DEPTH, TALL, WIDE), F32),
            pltpu.VMEM((4, DEPTH, TALL, WIDE), F32),
        ],
        out_specs=vmem(1) + smem(1),
    )(where, speed, start, rate0)
    halos = exchange(s2, 6)
    ext, tracer, landed, fallen = call(
        last_tracer,
        "last_tracer",
        smem(2) + vmem(9),
        [
            shaped(5, DEPTH, TALL, WIDE),
            shaped(LEVELS, ROWS, COLS),
            shaped(3, LEVELS, ROWS, COLS),
            shaped(3, FMAX, ROWS, COLS),
        ],
        scratch=[pltpu.VMEM((3, LEVELS + FMAX, ROWS, COLS), F32)],
    )(where, dt, s2, *halos, fields, by_depth)
    count = lax.axis_size("gz")
    arrived = lax.ppermute(fallen, "gz", [((i + 1) % count, i) for i in range(count)])
    (new_fields,) = call(
        last_section,
        "last_section",
        smem(2) + vmem(3),
        [shaped(5, LEVELS, ROWS, COLS)],
        scratch=[
            pltpu.VMEM((DEPTH, TALL, WIDE), F32),
            pltpu.VMEM((4, DEPTH, TALL, WIDE), F32),
        ],
        flops=1_000_000_000,
    )(where, dt, ext, start, tracer)
    arrived = jnp.where(place == last, 0.0, arrived)
    moments = landed.at[:, LEVELS - FMAX :].add(arrived)
    return (new_fields, moments)


def solution(mesh):
    spread = P(None, "gz", "gy", "gx")
    return jax.shard_map(
        per_device,
        mesh=mesh,
        in_specs=(spread, spread, spread, spread, P("gz", "gy", "gx"), spread),
        out_specs=(spread, spread),
        check_vma=False,
    )
```

```python
import jax
import jax.numpy as jnp
from jax import lax
from jax.experimental import pallas as pl
from jax.experimental.pallas import tpu as pltpu
from jax.sharding import PartitionSpec as P

NS = 4
FMAX = 8
GRID_AXES = ("gx", "gy", "gz")

sound_speed = 10.0
buoyancy = 0.5
courant_goal = 0.6
growth = 0.3

LEVELS, ROWS, COLS = 16, 8, 128
WIDE = 2 * COLS
REACH = 7
DEPTH = LEVELS + 2 * REACH
EDGE = 8
F32 = jnp.float32
C, PR, U, V, W = range(5)


class Plan:
    def __init__(self, tall, reach, short):
        self.tiles = [
            (field, part)
            for field in range(5)
            for part in ("oab" if field in tall else "on")
        ]
        self.at = {tile: n for n, tile in enumerate(self.tiles)}
        self.tall, self.reach, self.short = tall, reach, short
        far = [t for t in self.tiles if t[0] in (C, PR)] if C in tall else [
            t for t in self.tiles if t[0] == PR
        ]
        self.carried = []
        for a in range(reach):
            names = self.tiles if a < short else far
            self.carried += [(a, self.at[t]) for t in names] + [(a, -1), (a, -2)]

    def rows(self, ref, field, l):
        return jnp.concatenate(
            [
                ref[self.at[field, part], l]
                for part in ("oab" if field in self.tall else "on")
            ],
            axis=0,
        )

    def sixteen(self, ref, field, l):
        value = self.rows(ref, field, l)
        return sixteen(value) if field in self.tall else value


def lanes(shape):
    return lax.broadcasted_iota(jnp.int32, shape, len(shape) - 1)


def lower_rows(shape):
    return lax.broadcasted_iota(jnp.int32, shape, 0) < ROWS // 2


def around(above, below):
    return jnp.where(lower_rows(above.shape), above, below)


def sixteen(value):
    return jnp.concatenate(
        [value[0:ROWS], around(value[ROWS : 2 * ROWS], value[2 * ROWS :])], axis=0
    )


def raw_tile(refs, field, part, k):
    own, above, below = refs
    if part == "o":
        return own[field, k]
    if part == "n":
        return around(above[field, k], below[field, k])
    return (above if part == "a" else below)[field, k]


SHARED = {C: (1, 0), U: (1, 1), V: (2, 0), W: (2, 1)}


def shared_rows(read):
    down, up = [read(PR)], [read(PR)]
    for first, second in ((C, U), (V, W)):
        one, other = read(first), pltpu.roll(read(second), ROWS // 2, 0)
        down.append(around(one, other))
        up.append(around(other, one))
    return down, up


def shared_tile(refs, field, part, k):
    own, above, below = refs
    if part == "o":
        return own[field, k]
    if part == "n":
        index, half = SHARED[field]
        if half == 0:
            return around(above[index, k], below[index, k])
        return pltpu.roll(around(below[index, k], above[index, k]), ROWS // 2, 0)
    return (above if part == "a" else below)[0, k]


FIRST = Plan((C, PR, V), 7, 5)
SECOND = Plan((PR,), 6, 4)
TILE_OF = {FIRST: raw_tile, SECOND: shared_tile}


def pack_columns(plan):
    def kernel(own, above, below, speed, to_left, to_right):
        lane = lanes((ROWS, COLS))

        def one(k, _):
            left = jnp.zeros((ROWS, COLS), F32)
            right = jnp.zeros((ROWS, COLS), F32)
            for n, (field, part) in enumerate(plan.tiles):
                start = n * EDGE
                here = (lane >= start) & (lane < start + EDGE)
                value = TILE_OF[plan]((own, above, below), field, part, k)
                first = pltpu.roll(value, start, 1) if start else value
                last = pltpu.roll(value, (start + EDGE) % COLS, 1)
                left = jnp.where(here, first, left)
                right = jnp.where(here, last, right)
            to_left[k] = left
            to_right[k] = right
            return 0

        def pair(i, _):
            one(2 * i, 0)
            return one(2 * i + 1, 0)

        lax.fori_loop(0, LEVELS // 2, pair, 0)

    return kernel


def halo_columns(from_right, from_left, n):
    start = n * EDGE
    right = pltpu.roll(from_right, COLS - start, 1) if start else from_right
    left = pltpu.roll(from_left, (COLS - EDGE - start) % COLS, 1)
    return jnp.where(lanes((ROWS, COLS)) < COLS // 2, right, left)


def pack_levels(plan):
    def kernel(own, above, below, from_right, from_left, to_down, to_up):
        for place, (a, n) in enumerate(plan.carried):
            for out, k in ((to_down, a), (to_up, LEVELS - 1 - a)):
                if n >= 0:
                    out[place] = TILE_OF[plan]((own, above, below), *plan.tiles[n], k)
                else:
                    out[place] = (from_right if n == -1 else from_left)[k]

    return kernel


def assemble(plan, refs, ext, place, last):
    own, above, below, from_right, from_left, from_up, from_down = refs

    def middle(k, _):
        right, left = from_right[k], from_left[k]
        for n, (field, part) in enumerate(plan.tiles):
            ext[n, REACH + k, :, 0:COLS] = TILE_OF[plan]((own, above, below), field, part, k)
            ext[n, REACH + k, :, COLS:WIDE] = halo_columns(right, left, n)
        return 0

    lax.fori_loop(0, LEVELS, middle, 0)
    columns = {}
    for index, (a, n) in enumerate(plan.carried):
        if n < 0:
            columns[a, n] = index
    for message, level, there in (
        (from_down, lambda a: REACH - 1 - a, place > 0),
        (from_up, lambda a: REACH + LEVELS + a, place < last),
    ):
        keep = jnp.where(there, 1.0, 0.0).astype(F32)
        for index, (a, n) in enumerate(plan.carried):
            if n >= 0:
                ext[n, level(a), :, 0:COLS] = message[index] * keep
                ext[n, level(a), :, COLS:WIDE] = (
                    halo_columns(message[columns[a, -1]], message[columns[a, -2]], n) * keep
                )


def shift(value, by, axis):
    return pltpu.roll(value, (-by) % value.shape[axis], axis)


def face_flux(q, wind):
    central = 37.0 * (q[2] + q[3]) - 8.0 * (q[1] + q[4]) + (q[0] + q[5])
    upwind = 10.0 * (q[3] - q[2]) - 5.0 * (q[4] - q[1]) + (q[5] - q[0])
    return wind * central - jnp.abs(wind) * upwind


def flat_flux(q, wind, axis):
    flux = face_flux([shift(q, by, axis) if by else q for by in range(-2, 4)], wind)
    return flux - shift(flux, -1, axis)


def rows_flux(q, wind):
    if wind.shape[0] == 24:
        return sixteen(flat_flux(q, wind, 0))
    if q.shape[0] == 24:
        flux = face_flux([sixteen(shift(q, by, 0) if by else q) for by in range(-2, 4)], wind)
        return flux - shift(flux, -1, 0)
    return flat_flux(q, wind, 0)


def level_flux(read, wind, l):
    return face_flux([read(l + by) for by in range(-2, 4)], wind)


def in_domain(l, place, last, lid):
    g = place * LEVELS + l - REACH
    top = (last + 1) * LEVELS - (1 if lid else 0)
    return jnp.where((g >= 0) & (g < top), 1.0, 0.0).astype(F32)


SIXTIETH = -1.0 / 60.0


def rates(plan, ext, fields, write, first, count):
    reads = [lambda l, f=f: plan.sixteen(ext, f, l) for f in fields]

    def one(l, lows):
        u, v, w = (
            plan.sixteen(ext, U, l),
            plan.rows(ext, V, l),
            plan.sixteen(ext, W, l),
        )
        highs = []
        for n, f in enumerate(fields):
            high = level_flux(reads[n], w, l)
            here = plan.rows(ext, f, l)
            cells = reads[n](l)
            total = flat_flux(cells, u, 1) + rows_flux(here, v) + (high - lows[n])
            write(n, l, total * SIXTIETH)
            highs.append(high)
        return tuple(highs)

    w = plan.sixteen(ext, W, first - 1)
    lax.fori_loop(
        first, first + count, one, tuple(level_flux(read, w, first - 1) for read in reads)
    )


def first_rates(
    place_ref, own, above, below, from_right, from_left, from_up, from_down, ext, rate
):
    place, last = place_ref[0], place_ref[1]
    assemble(
        FIRST, (own, above, below, from_right, from_left, from_up, from_down), ext, place, last
    )

    @pl.when(place == last)
    def _():
        for part in "on":
            ext[FIRST.at[W, part], REACH + LEVELS - 1] = jnp.zeros((ROWS, WIDE), F32)

    def write(n, l, value):
        rate[n, l] = value

    rates(FIRST, ext, (C, PR), write, REACH - 4, LEVELS + 8)


def acoustic(p, u, v, w, read_c, rate, step, first, count, place, last):
    pull = step * sound_speed

    def wind_w(l):
        lift = (buoyancy * 0.5) * (read_c(l) + read_c(l + 1))
        return (w[0](l) + step * lift - pull * (level(l + 1) - level(l))) * in_domain(
            l, place, last, True
        )

    def level(l):
        value = p[0](l)
        return sixteen(value) if value.shape[0] == 24 else value

    def one(l, w_low):
        tall = p[0](l)
        p_here = level(l)
        w_new = wind_w(l)
        u_new = u[0](l) - pull * (shift(p_here, 1, 1) - p_here)
        v_old = v[0](l)
        if v_old.shape[0] == 24:
            v_tall = v_old - pull * (shift(tall, 1, 0) - tall)
            v_new, v_flow = sixteen(v_tall), sixteen(v_tall - shift(v_tall, -1, 0))
        else:
            v_new = v_old - pull * (shift(p_here, 1, 0) - p_here)
            v_flow = v_new - shift(v_new, -1, 0)
        divergence = (u_new - shift(u_new, -1, 1)) + v_flow + (w_new - w_low)
        p_new = (p_here + step * rate(l) - pull * divergence) * in_domain(l, place, last, False)
        p[1](l, p_new)
        u[1](l, u_new)
        v[1](l, v_new)
        w[1](l, w_new)
        return w_new

    w_low = wind_w(first - 1)
    w[1](first - 1, w_low)
    lax.fori_loop(first, first + count, one, w_low)


def access(ref, *lead):
    def read(l):
        return ref[(*lead, l)]

    def write(l, value):
        ref[(*lead, l)] = value

    return read, write


def begin(start, field, tall=False):
    return lambda l: (FIRST.rows if tall else FIRST.sixteen)(start, field, l)


def own_write(ref, field):
    def write(l, value):
        if not isinstance(l, int):
            ref[field, l - REACH] = value[0:ROWS, 0:COLS]

    return write


def tracer_rate(tiles, winds, l, low):
    u, v, w = winds
    rows = flat_flux(tiles(l)[:, 0:COLS], v(l)[:, 0:COLS], 0)[0:ROWS]
    cols = flat_flux(tiles(l)[0:ROWS], u(l)[0:ROWS], 1)[:, 0:COLS]
    high = tracer_high(tiles, w, l)
    return (rows + cols + (high - low)) * SIXTIETH, high


def tracer_high(tiles, w, l):
    return level_flux(lambda m: tiles(m)[0:ROWS, 0:COLS], w(l)[0:ROWS, 0:COLS], l)


def two_sections(place_ref, speed, start, rate0, s2, down, up, dt_out, s1, rate1, fast):
    place, last = place_ref[0], place_ref[1]
    dt = courant_goal / (1.0 + jnp.max(speed[...]))
    dt_out[0] = dt
    third = dt * (1.0 / 3.0)

    def tracer(l, _):
        s1[C, l] = (FIRST.sixteen(start, C, l) + third * rate0[0, l]) * in_domain(
            l, place, last, False
        )
        return 0

    lax.fori_loop(REACH - 4, REACH + LEVELS + 4, tracer, 0)
    acoustic(
        (begin(start, PR, True), access(s1, PR)[1]),
        (begin(start, U), access(s1, U)[1]),
        (begin(start, V, True), access(s1, V)[1]),
        (begin(start, W), access(s1, W)[1]),
        begin(start, C),
        access(rate0, 1)[0],
        third,
        REACH - 4,
        LEVELS + 8,
        place,
        last,
    )
    half = dt * 0.5
    tiles = access(s1, C)[0]
    winds = [access(s1, f)[0] for f in (U, V, W)]

    def own_tracer(l, low):
        tendency, high = tracer_rate(tiles, winds, l, low)
        s2[C, l - REACH] = start[FIRST.at[C, "o"], l, :, 0:COLS] + half * tendency
        return high

    lax.fori_loop(REACH, REACH + LEVELS, own_tracer, tracer_high(tiles, winds[2], REACH - 1))

    def write(n, l, value):
        rate1[l] = value

    rates(SECTION, s1, (PR,), write, REACH - 1, LEVELS + 2)
    step = half / (NS // 2)
    acoustic(
        (begin(start, PR), access(fast, 0)[1]),
        (begin(start, U), access(fast, 1)[1]),
        (begin(start, V), access(fast, 2)[1]),
        (begin(start, W), access(fast, 3)[1]),
        access(s1, C)[0],
        access(rate1)[0],
        step,
        REACH - 1,
        LEVELS + 2,
        place,
        last,
    )
    acoustic(
        (access(fast, 0)[0], own_write(s2, PR)),
        (access(fast, 1)[0], own_write(s2, U)),
        (access(fast, 2)[0], own_write(s2, V)),
        (access(fast, 3)[0], own_write(s2, W)),
        access(s1, C)[0],
        access(rate1)[0],
        step,
        REACH,
        LEVELS,
        place,
        last,
    )

    def share(k, _):
        to_down, to_up = shared_rows(lambda f: s2[f, k])
        for n in range(3):
            down[n, k] = to_down[n]
            up[n, k] = to_up[n]
        return 0

    lax.fori_loop(0, LEVELS, share, 0)


class Whole:
    def rows(self, ref, field, l):
        return ref[field, l]

    sixteen = rows


SECTION = Whole()


def last_tracer(
    place_ref,
    dt_ref,
    own,
    above,
    below,
    from_right,
    from_left,
    from_up,
    from_down,
    fields,
    *rest,
):
    *chunks, ext, tracer, landed, fallen, total, by_depth, sem = rest
    place, last = place_ref[0], place_ref[1]
    dt = dt_ref[0]
    each = LEVELS // len(chunks)
    copies = [
        pltpu.make_async_copy(chunk, by_depth.at[pl.ds(n * each, each)], sem.at[n])
        for n, chunk in enumerate(chunks)
    ]
    for copy in copies:
        copy.start()
    assemble(
        SECOND, (own, above, below, from_right, from_left, from_up, from_down), ext, place, last
    )
    total[...] = jnp.zeros(total.shape, F32)
    for copy in copies:
        copy.wait()
    tiles = lambda l: SECOND.rows(ext, C, l)
    winds = [lambda l, f=f: SECOND.rows(ext, f, l) for f in (U, V, W)]

    def one(l, low):
        k = l - REACH
        tendency, high = tracer_rate(tiles, winds, l, low)
        c = fields[C, k] + dt * tendency
        tracer[k] = c
        grown = jnp.exp(growth * c)
        weights = (None, grown, grown * jnp.exp((0.5 * growth) * c))
        for depth in range(FMAX + 1):
            for moment in range(3):
                value = by_depth[k, depth, moment]
                if moment:
                    value = value * weights[moment]
                total[moment, k + FMAX - depth] += value
        return high

    lax.fori_loop(REACH, REACH + LEVELS, one, tracer_high(tiles, winds[2], REACH - 1))
    landed[...] = total[:, FMAX:]
    fallen[...] = total[:, 0:FMAX]


def last_section(place_ref, dt_ref, ext, start, tracer, out, rate, fast):
    place, last = place_ref[0], place_ref[1]
    step = dt_ref[0] / NS

    def write(n, l, value):
        rate[l] = value

    rates(SECOND, ext, (PR,), write, REACH - 3, LEVELS + 6)
    out[C] = tracer[...]
    names = (PR, U, V, W)
    for repeat in range(NS):
        reads = [
            begin(start, f) if repeat == 0 else access(fast, n)[0] for n, f in enumerate(names)
        ]
        writes = [
            own_write(out, f) if repeat == NS - 1 else access(fast, n)[1]
            for n, f in enumerate(names)
        ]
        acoustic(
            *zip(reads, writes),
            lambda l: SECOND.rows(ext, C, l),
            access(rate)[0],
            step,
            REACH - 3 + repeat,
            LEVELS + 6 - 2 * repeat,
            place,
            last,
        )


def deposit(radius, weight, column, counts, fall_depth, out):
    slots, levels = radius.shape[0], radius.shape[1]
    target = lax.broadcasted_iota(jnp.int32, (COLS, COLS), 0)
    row = lax.broadcasted_iota(jnp.int32, (ROWS, COLS), 0)
    per_step = 4

    for k in range(levels):
        out[k] = jnp.zeros(out.shape[1:], F32)
        live = counts[k]

        def some(step, _, k=k, live=live):
            sums = [[None] * 3 for _ in range(FMAX + 1)]
            for part in range(per_step):
                s = step * per_step + part
                r = radius[s, k]
                number = jnp.where(s < live, weight[s, k], 0.0)
                area = number * r * r
                terms = []
                for t in (number, area, area * r):
                    high = t.astype(jnp.bfloat16).astype(F32)
                    terms += [high, t - high]
                cols = column[s, k]
                left, right = [], []
                for j in range(ROWS):
                    left.append(
                        jnp.concatenate([jnp.where(row == j, t, 0.0) for t in terms], axis=0)
                    )
                    right.append(jnp.where(cols[j : j + 1] == target, 1.0, 0.0).astype(F32))
                sent = lax.dot_general(
                    jnp.concatenate(left, axis=1),
                    jnp.concatenate(right, axis=1),
                    (((1,), (1,)), ((), ())),
                    preferred_element_type=F32,
                )
                depth = jnp.broadcast_to(fall_depth[s, k], (ROWS, COLS))
                for d in range(FMAX + 1):
                    falls = depth == d
                    for m in range(3):
                        both = sent[16 * m : 16 * m + 8] + sent[16 * m + 8 : 16 * m + 16]
                        value = jnp.where(falls, both, 0.0)
                        sums[d][m] = value if sums[d][m] is None else sums[d][m] + value
            for d in range(FMAX + 1):
                for m in range(3):
                    out[k, d, m] += sums[d][m]
            return 0

        lax.fori_loop(0, slots // per_step, some, 0)


def vmem(n):
    return [pl.BlockSpec(memory_space=pltpu.VMEM)] * n


def smem(n):
    return [pl.BlockSpec(memory_space=pltpu.SMEM)] * n


def anywhere(n):
    return [pl.BlockSpec(memory_space=pl.ANY)] * n


def shaped(*dims):
    return jax.ShapeDtypeStruct(dims, F32)


def held(*dims):
    return pltpu.VMEM(dims, F32)


def call(kernel, name, ins, outs, scratch=(), out_specs=None, flops=None, grant=4):
    made = pl.pallas_call(
        kernel,
        name=name,
        in_specs=ins,
        out_specs=tuple(out_specs or vmem(len(outs))),
        out_shape=tuple(outs),
        scratch_shapes=list(scratch),
        compiler_params=pltpu.CompilerParams(vmem_limit_bytes=grant << 20),
        cost_estimate=(
            pl.CostEstimate(flops=flops, bytes_accessed=0, transcendentals=0) if flops else None
        ),
    )

    def run(*operands):
        return made(
            *(
                pltpu.with_memory_space_constraint(value, pltpu.VMEM)
                if spec.memory_space == pltpu.VMEM
                else value
                for spec, value in zip(ins, operands)
            )
        )

    return run


def both_ways(down, axis, up):
    count = lax.axis_size(axis)
    return (
        lax.ppermute(down, axis, [((i + 1) % count, i) for i in range(count)]),
        lax.ppermute(up, axis, [(i, (i + 1) % count) for i in range(count)]),
    )


def exchange(plan, own, down, up, token):
    above, below = both_ways(down, "gy", up)
    to_left, to_right = call(
        pack_columns(plan),
        "pack_columns",
        vmem(3) + anywhere(1),
        [held(LEVELS, ROWS, COLS)] * 2,
    )(own, above, below, token)
    from_right, from_left = both_ways(to_left, "gx", to_right)
    tiles = len(plan.carried)
    to_down, to_up = call(
        pack_levels(plan), "pack_levels", vmem(5), [held(tiles, ROWS, COLS)] * 2
    )(own, above, below, from_right, from_left)
    from_up, from_down = both_ways(to_down, "gz", to_up)
    return above, below, from_right, from_left, from_up, from_down


def top_speed(fields, place, last):
    w = fields[4] * (
        (jnp.arange(LEVELS) < LEVELS - 1) | (place != last)
    ).astype(F32)[:, None, None]
    local = jnp.max(jnp.abs(fields[2]) + jnp.abs(fields[3]) + jnp.abs(w))
    devices = lax.axis_size(GRID_AXES)
    everywhere = jnp.broadcast_to(local, (devices, 1, COLS))
    return lax.all_to_all(everywhere, GRID_AXES, 0, 0)


def droplets(radius, weight, column, counts, fall_depth, chunk):
    slots = radius.shape[0]
    made = []
    for n in range(LEVELS // chunk):
        whole = pl.BlockSpec((slots, chunk, ROWS, COLS), lambda i, n=n: (0, n, 0, 0))
        made.append(
            pl.pallas_call(
                deposit,
                name="deposit",
                grid=(1,),
                in_specs=[
                    whole,
                    whole,
                    whole,
                    pl.BlockSpec((chunk, ROWS, COLS), lambda i, n=n: (n, 0, 0)),
                    pl.BlockSpec((slots, chunk, ROWS, 1), lambda i, n=n: (0, n, 0, 0)),
                ],
                out_specs=pl.BlockSpec(
                    (chunk, FMAX + 1, 3, ROWS, COLS), lambda i: (0, 0, 0, 0, 0)
                ),
                out_shape=shaped(chunk, FMAX + 1, 3, ROWS, COLS),
                compiler_params=pltpu.CompilerParams(vmem_limit_bytes=12 << 20),
                cost_estimate=pl.CostEstimate(
                    flops=200_000_000, bytes_accessed=0, transcendentals=0
                ),
            )(radius, weight, column, counts, fall_depth)
        )
    return made


def per_device(fields, radius, weight, column, counts, fall_depth):
    place = lax.axis_index("gz")
    last = lax.axis_size("gz") - 1
    where = jnp.stack([place, jnp.int32(last)]).astype(jnp.int32)
    by_depth = droplets(radius, weight, column, counts, fall_depth, 2)
    speed = top_speed(fields, place, last)
    halos = exchange(FIRST, fields, fields, fields, speed)
    start, rate0 = call(
        first_rates,
        "first_rates",
        smem(1) + vmem(7),
        [held(len(FIRST.tiles), DEPTH, ROWS, WIDE), held(2, DEPTH, 2 * ROWS, WIDE)],
    )(where, fields, *halos)
    s2, down, up, dt = call(
        two_sections,
        "two_sections",
        smem(1) + vmem(3),
        [held(5, LEVELS, ROWS, COLS)] + [held(3, LEVELS, ROWS, COLS)] * 2 + [shaped(1)],
        scratch=[
            pltpu.VMEM((5, DEPTH, 2 * ROWS, WIDE), F32),
            pltpu.VMEM((DEPTH, 2 * ROWS, WIDE), F32),
            pltpu.VMEM((4, DEPTH, 2 * ROWS, WIDE), F32),
        ],
        out_specs=vmem(3) + smem(1),
        grant=10,
    )(where, speed, start, rate0)
    halos = exchange(SECOND, s2, down, up, speed)
    ext, tracer, landed, fallen = call(
        last_tracer,
        "last_tracer",
        smem(2) + vmem(8) + anywhere(len(by_depth)),
        [
            held(len(SECOND.tiles), DEPTH, ROWS, WIDE),
            held(LEVELS, ROWS, COLS),
            held(3, LEVELS, ROWS, COLS),
            held(3, FMAX, ROWS, COLS),
        ],
        scratch=[
            pltpu.VMEM((3, LEVELS + FMAX, ROWS, COLS), F32),
            pltpu.VMEM((LEVELS, FMAX + 1, 3, ROWS, COLS), F32),
            pltpu.SemaphoreType.DMA((len(by_depth),)),
        ],
    )(where, dt, s2, *halos, fields, *by_depth)
    count = lax.axis_size("gz")
    arrived = lax.ppermute(fallen, "gz", [((i + 1) % count, i) for i in range(count)])
    (new_fields,) = call(
        last_section,
        "last_section",
        smem(2) + vmem(3),
        [shaped(5, LEVELS, ROWS, COLS)],
        scratch=[
            pltpu.VMEM((DEPTH, 2 * ROWS, WIDE), F32),
            pltpu.VMEM((4, DEPTH, 2 * ROWS, WIDE), F32),
        ],
        flops=1_000_000_000,
        grant=8,
    )(where, dt, ext, start, tracer)
    arrived = jnp.where(place == last, 0.0, arrived)
    moments = landed.at[:, LEVELS - FMAX :].add(arrived)
    return (new_fields, moments)


def solution(mesh):
    spread = P(None, "gz", "gy", "gx")
    return jax.shard_map(
        per_device,
        mesh=mesh,
        in_specs=(spread, spread, spread, spread, P("gz", "gy", "gx"), spread),
        out_specs=(spread, spread),
        check_vma=False,
    )
```

```python
import jax
import jax.numpy as jnp
from jax import lax
from jax.experimental import pallas as pl
from jax.experimental.pallas import tpu as pltpu
from jax.sharding import PartitionSpec as P

NS = 4
FMAX = 8
EARLY = 5
GRID_AXES = ("gx", "gy", "gz")

sound_speed = 10.0
buoyancy = 0.5
courant_goal = 0.6
growth = 0.3

LEVELS, ROWS, COLS = 16, 8, 128
WIDE = 2 * COLS
REACH = 7
DEPTH = LEVELS + 2 * REACH
EDGE = 8
F32 = jnp.float32
C, PR, U, V, W = range(5)


class Plan:
    def __init__(self, tall, reach, short):
        self.tiles = [
            (field, part)
            for field in range(5)
            for part in ("oab" if field in tall else "on")
        ]
        self.at = {tile: n for n, tile in enumerate(self.tiles)}
        self.tall, self.reach, self.short = tall, reach, short
        far = [t for t in self.tiles if t[0] in (C, PR)] if C in tall else [
            t for t in self.tiles if t[0] == PR
        ]
        self.carried = []
        for a in range(reach):
            names = self.tiles if a < short else far
            self.carried += [(a, self.at[t]) for t in names] + [(a, -1), (a, -2)]

    def rows(self, ref, field, l):
        return jnp.concatenate(
            [
                ref[self.at[field, part], l]
                for part in ("oab" if field in self.tall else "on")
            ],
            axis=0,
        )

    def sixteen(self, ref, field, l):
        value = self.rows(ref, field, l)
        return sixteen(value) if field in self.tall else value


def lanes(shape):
    return lax.broadcasted_iota(jnp.int32, shape, len(shape) - 1)


def lower_rows(shape):
    return lax.broadcasted_iota(jnp.int32, shape, 0) < ROWS // 2


def around(above, below):
    return jnp.where(lower_rows(above.shape), above, below)


def sixteen(value):
    return jnp.concatenate(
        [value[0:ROWS], around(value[ROWS : 2 * ROWS], value[2 * ROWS :])], axis=0
    )


def raw_tile(refs, field, part, k):
    own, above, below = refs
    if part == "o":
        return own[field, k]
    if part == "n":
        return around(above[field, k], below[field, k])
    return (above if part == "a" else below)[field, k]


SHARED = {C: (1, 0), U: (1, 1), V: (2, 0), W: (2, 1)}


def shared_rows(read):
    down, up = [read(PR)], [read(PR)]
    for first, second in ((C, U), (V, W)):
        one, other = read(first), pltpu.roll(read(second), ROWS // 2, 0)
        down.append(around(one, other))
        up.append(around(other, one))
    return down, up


def shared_tile(refs, field, part, k):
    own, above, below = refs
    if part == "o":
        return own[field, k]
    if part == "n":
        index, half = SHARED[field]
        if half == 0:
            return around(above[index, k], below[index, k])
        return pltpu.roll(around(below[index, k], above[index, k]), ROWS // 2, 0)
    return (above if part == "a" else below)[0, k]


FIRST = Plan((C, PR, V), 7, 5)
SECOND = Plan((PR,), 6, 4)
TILE_OF = {FIRST: raw_tile, SECOND: shared_tile}


def pack_columns(plan):
    def kernel(own, above, below, *rest):
        to_left, to_right = rest[-2:]
        lane = lanes((ROWS, COLS))

        def one(k, _):
            left = jnp.zeros((ROWS, COLS), F32)
            right = jnp.zeros((ROWS, COLS), F32)
            for n, (field, part) in enumerate(plan.tiles):
                start = n * EDGE
                here = (lane >= start) & (lane < start + EDGE)
                value = TILE_OF[plan]((own, above, below), field, part, k)
                first = pltpu.roll(value, start, 1) if start else value
                last = pltpu.roll(value, (start + EDGE) % COLS, 1)
                left = jnp.where(here, first, left)
                right = jnp.where(here, last, right)
            to_left[k] = left
            to_right[k] = right
            return 0

        def pair(i, _):
            one(2 * i, 0)
            return one(2 * i + 1, 0)

        lax.fori_loop(0, LEVELS // 2, pair, 0)

    return kernel


def halo_columns(from_right, from_left, n):
    start = n * EDGE
    right = pltpu.roll(from_right, COLS - start, 1) if start else from_right
    left = pltpu.roll(from_left, (COLS - EDGE - start) % COLS, 1)
    return jnp.where(lanes((ROWS, COLS)) < COLS // 2, right, left)


def pack_levels(plan):
    def kernel(own, above, below, from_right, from_left, to_down, to_up):
        for place, (a, n) in enumerate(plan.carried):
            for out, k in ((to_down, a), (to_up, LEVELS - 1 - a)):
                if n >= 0:
                    out[place] = TILE_OF[plan]((own, above, below), *plan.tiles[n], k)
                else:
                    out[place] = (from_right if n == -1 else from_left)[k]

    return kernel


def assemble(plan, refs, ext, place, last):
    own, above, below, from_right, from_left, from_up, from_down = refs

    def middle(levels, _):
        for k in levels:
            right, left = from_right[k], from_left[k]
            for n, (field, part) in enumerate(plan.tiles):
                ext[n, REACH + k, :, 0:COLS] = TILE_OF[plan]((own, above, below), field, part, k)
                ext[n, REACH + k, :, COLS:WIDE] = halo_columns(right, left, n)
        return 0

    sweep(0, LEVELS, 4, middle)
    columns = {}
    for index, (a, n) in enumerate(plan.carried):
        if n < 0:
            columns[a, n] = index
    for message, level, there in (
        (from_down, lambda a: REACH - 1 - a, place > 0),
        (from_up, lambda a: REACH + LEVELS + a, place < last),
    ):
        keep = jnp.where(there, 1.0, 0.0).astype(F32)
        for index, (a, n) in enumerate(plan.carried):
            if n >= 0:
                ext[n, level(a), :, 0:COLS] = message[index] * keep
                ext[n, level(a), :, COLS:WIDE] = (
                    halo_columns(message[columns[a, -1]], message[columns[a, -2]], n) * keep
                )


def shift(value, by, axis):
    return pltpu.roll(value, (-by) % value.shape[axis], axis)


def face_flux(q, wind):
    central = 37.0 * (q[2] + q[3]) - 8.0 * (q[1] + q[4]) + (q[0] + q[5])
    upwind = 10.0 * (q[3] - q[2]) - 5.0 * (q[4] - q[1]) + (q[5] - q[0])
    return wind * central - jnp.abs(wind) * upwind


def flat_flux(q, wind, axis):
    flux = face_flux([shift(q, by, axis) if by else q for by in range(-2, 4)], wind)
    return flux - shift(flux, -1, axis)


def rows_flux(q, wind):
    if wind.shape[0] == 24:
        return sixteen(flat_flux(q, wind, 0))
    if q.shape[0] == 24:
        flux = face_flux([sixteen(shift(q, by, 0) if by else q) for by in range(-2, 4)], wind)
        return flux - shift(flux, -1, 0)
    return flat_flux(q, wind, 0)


def level_flux(read, wind, l):
    return face_flux([read(l + by) for by in range(-2, 4)], wind)


def in_domain(l, place, last, lid):
    g = place * LEVELS + l - REACH
    top = (last + 1) * LEVELS - (1 if lid else 0)
    return jnp.where((g >= 0) & (g < top), 1.0, 0.0).astype(F32)


SIXTIETH = -1.0 / 60.0


def sweep(first, count, most, body, carry=0):
    size = max(n for n in range(1, most + 1) if count % n == 0)

    def run(i, carry):
        start = first + i * size
        return body([start + n for n in range(size)], carry)

    return lax.fori_loop(0, count // size, run, carry)


def rates(plan, ext, fields, write, first, count, most):
    reads = [lambda l, f=f: plan.sixteen(ext, f, l) for f in fields]

    def some(levels, lows):
        results = []
        for l in levels:
            u, v, w = (
                plan.sixteen(ext, U, l),
                plan.rows(ext, V, l),
                plan.sixteen(ext, W, l),
            )
            highs = []
            for n, f in enumerate(fields):
                high = level_flux(reads[n], w, l)
                here = plan.rows(ext, f, l)
                total = (
                    flat_flux(reads[n](l), u, 1) + rows_flux(here, v) + (high - lows[n])
                )
                results.append((n, l, total * SIXTIETH))
                highs.append(high)
            lows = tuple(highs)
        for result in results:
            write(*result)
        return lows

    w = plan.sixteen(ext, W, first - 1)
    sweep(first, count, most, some, tuple(level_flux(read, w, first - 1) for read in reads))


def first_rates(
    place_ref, own, above, below, from_right, from_left, from_up, from_down, speed, ext, rate
):
    place, last = place_ref[0], place_ref[1]
    assemble(
        FIRST, (own, above, below, from_right, from_left, from_up, from_down), ext, place, last
    )

    @pl.when(place == last)
    def _():
        for part in "on":
            ext[FIRST.at[W, part], REACH + LEVELS - 1] = jnp.zeros((ROWS, WIDE), F32)

    def write(n, l, value):
        rate[n, l] = value

    rates(FIRST, ext, (C, PR), write, REACH - 4, LEVELS + 8, 2)


def acoustic(p, u, v, w, read_c, rate, step, first, count, place, last):
    pull = step * sound_speed

    def level(value):
        return sixteen(value) if value.shape[0] == 24 else value

    def wind_w(l, lift_low, lift_high, p_here, p_above):
        lift = (buoyancy * 0.5) * (lift_low + lift_high)
        return (w[0](l) + step * lift - pull * (p_above - p_here)) * in_domain(l, place, last, True)

    def some(levels, w_low):
        talls = [p[0](l) for l in (*levels, levels[-1] + 1)]
        cells = [level(value) for value in talls]
        warm = [read_c(l) for l in (*levels, levels[-1] + 1)]
        results = []
        for n, l in enumerate(levels):
            p_here = cells[n]
            w_new = wind_w(l, warm[n], warm[n + 1], p_here, cells[n + 1])
            u_new = u[0](l) - pull * (shift(p_here, 1, 1) - p_here)
            v_old = v[0](l)
            if v_old.shape[0] == 24:
                v_tall = v_old - pull * (shift(talls[n], 1, 0) - talls[n])
                v_new, v_flow = sixteen(v_tall), sixteen(v_tall - shift(v_tall, -1, 0))
            else:
                v_new = v_old - pull * (shift(p_here, 1, 0) - p_here)
                v_flow = v_new - shift(v_new, -1, 0)
            divergence = (u_new - shift(u_new, -1, 1)) + v_flow + (w_new - w_low)
            p_new = (p_here + step * rate(l) - pull * divergence) * in_domain(
                l, place, last, False
            )
            results.append((l, p_new, u_new, v_new, w_new))
            w_low = w_new
        for l, *news in results:
            for target, value in zip((p, u, v, w), news):
                target[1](l, value)
        return w_low

    low = first - 1
    w_low = wind_w(low, read_c(low), read_c(first), level(p[0](low)), level(p[0](first)))
    w[1](low, w_low)
    sweep(first, count, 6, some, w_low)


def access(ref, *lead):
    def read(l):
        return ref[(*lead, l)]

    def write(l, value):
        ref[(*lead, l)] = value

    return read, write


def begin(start, field, tall=False):
    return lambda l: (FIRST.rows if tall else FIRST.sixteen)(start, field, l)


def own_write(ref, field):
    def write(l, value):
        if not isinstance(l, int):
            ref[field, l - REACH] = value[0:ROWS, 0:COLS]

    return write


def tracer_rate(tiles, winds, l, low):
    u, v, w = winds
    rows = flat_flux(tiles(l)[:, 0:COLS], v(l)[:, 0:COLS], 0)[0:ROWS]
    cols = flat_flux(tiles(l)[0:ROWS], u(l)[0:ROWS], 1)[:, 0:COLS]
    high = tracer_high(tiles, w, l)
    return (rows + cols + (high - low)) * SIXTIETH, high


def tracer_high(tiles, w, l):
    return level_flux(lambda m: tiles(m)[0:ROWS, 0:COLS], w(l)[0:ROWS, 0:COLS], l)


def two_sections(place_ref, speed, start, rate0, s2, down, up, dt_out, s1, rate1, fast):
    place, last = place_ref[0], place_ref[1]
    dt = courant_goal / (1.0 + jnp.max(speed[...]))
    dt_out[0] = dt
    third = dt * (1.0 / 3.0)

    def tracer(levels, _):
        for l in levels:
            s1[C, l] = (FIRST.sixteen(start, C, l) + third * rate0[0, l]) * in_domain(
                l, place, last, False
            )
        return 0

    sweep(REACH - 4, LEVELS + 8, 4, tracer)
    acoustic(
        (begin(start, PR, True), access(s1, PR)[1]),
        (begin(start, U), access(s1, U)[1]),
        (begin(start, V, True), access(s1, V)[1]),
        (begin(start, W), access(s1, W)[1]),
        begin(start, C),
        access(rate0, 1)[0],
        third,
        REACH - 4,
        LEVELS + 8,
        place,
        last,
    )
    half = dt * 0.5
    tiles = access(s1, C)[0]
    winds = [access(s1, f)[0] for f in (U, V, W)]

    def own_tracer(levels, low):
        results = []
        for l in levels:
            tendency, low = tracer_rate(tiles, winds, l, low)
            results.append(start[FIRST.at[C, "o"], l, :, 0:COLS] + half * tendency)
        for l, value in zip(levels, results):
            s2[C, l - REACH] = value
        return low

    sweep(REACH, LEVELS, 4, own_tracer, tracer_high(tiles, winds[2], REACH - 1))

    def write(n, l, value):
        rate1[l] = value

    rates(SECTION, s1, (PR,), write, REACH - 1, LEVELS + 2, 3)
    step = half / (NS // 2)
    acoustic(
        (begin(start, PR), access(fast, 0)[1]),
        (begin(start, U), access(fast, 1)[1]),
        (begin(start, V), access(fast, 2)[1]),
        (begin(start, W), access(fast, 3)[1]),
        access(s1, C)[0],
        access(rate1)[0],
        step,
        REACH - 1,
        LEVELS + 2,
        place,
        last,
    )
    acoustic(
        (access(fast, 0)[0], own_write(s2, PR)),
        (access(fast, 1)[0], own_write(s2, U)),
        (access(fast, 2)[0], own_write(s2, V)),
        (access(fast, 3)[0], own_write(s2, W)),
        access(s1, C)[0],
        access(rate1)[0],
        step,
        REACH,
        LEVELS,
        place,
        last,
    )

    def share(levels, _):
        made = [shared_rows(lambda f, k=k: s2[f, k]) for k in levels]
        for k, (to_down, to_up) in zip(levels, made):
            for n in range(3):
                down[n, k] = to_down[n]
                up[n, k] = to_up[n]
        return 0

    sweep(0, LEVELS, 4, share)


class Whole:
    def rows(self, ref, field, l):
        return ref[field, l]

    sixteen = rows


SECTION = Whole()


def last_tracer(
    place_ref,
    dt_ref,
    own,
    above,
    below,
    from_right,
    from_left,
    from_up,
    from_down,
    start,
    *rest,
):
    *chunks, ext, tracer, landed, fallen, factor, by_depth, sem = rest
    place, last = place_ref[0], place_ref[1]
    dt = dt_ref[0]
    each = LEVELS // len(chunks)
    copies = [
        pltpu.make_async_copy(chunk, by_depth.at[pl.ds(n * each, each)], sem.at[n])
        for n, chunk in enumerate(chunks)
    ]
    for copy in copies:
        copy.start()
    assemble(
        SECOND, (own, above, below, from_right, from_left, from_up, from_down), ext, place, last
    )
    tiles = lambda l: SECOND.rows(ext, C, l)
    winds = [lambda l, f=f: SECOND.rows(ext, f, l) for f in (U, V, W)]

    def some(levels, low):
        results = []
        for l in levels:
            tendency, low = tracer_rate(tiles, winds, l, low)
            c = start[FIRST.at[C, "o"], l, :, 0:COLS] + dt * tendency
            grown = jnp.exp(growth * c)
            results.append((c, grown, grown * jnp.exp((0.5 * growth) * c)))
        for l, (c, second, third) in zip(levels, results):
            tracer[l - REACH] = c
            factor[0, l - REACH] = second
            factor[1, l - REACH] = third
        return low

    sweep(REACH, LEVELS, 4, some, tracer_high(tiles, winds[2], REACH - 1))
    for copy in copies:
        copy.wait()
    for target in range(-FMAX, LEVELS):
        for moment in range(3):
            total = None
            for depth in range(FMAX + 1):
                k = target + depth
                if 0 <= k < LEVELS:
                    value = by_depth[k, depth, moment]
                    if moment:
                        value = value * factor[moment - 1, k]
                    total = value if total is None else total + value
            if target < 0:
                fallen[moment, target + FMAX] = total
            else:
                landed[moment, target] = total


def last_section(place_ref, dt_ref, ext, start, tracer, out, rate, fast):
    place, last = place_ref[0], place_ref[1]
    step = dt_ref[0] / NS

    def write(n, l, value):
        rate[l] = value

    rates(SECOND, ext, (PR,), write, REACH - 3, LEVELS + 6, 2)
    out[C] = tracer[...]
    names = (PR, U, V, W)
    for repeat in range(NS):
        reads = [
            begin(start, f) if repeat == 0 else access(fast, n)[0] for n, f in enumerate(names)
        ]
        writes = [
            own_write(out, f) if repeat == NS - 1 else access(fast, n)[1]
            for n, f in enumerate(names)
        ]
        acoustic(
            *zip(reads, writes),
            lambda l: SECOND.rows(ext, C, l),
            access(rate)[0],
            step,
            REACH - 3 + repeat,
            LEVELS + 6 - 2 * repeat,
            place,
            last,
        )


def deposit(radius, weight, column, counts, fall_depth, out):
    slots, levels = radius.shape[0], radius.shape[1]
    target = lax.broadcasted_iota(jnp.int32, (COLS, COLS), 0)
    row = lax.broadcasted_iota(jnp.int32, (ROWS, COLS), 0)
    per_step = 4

    for k in range(levels):
        out[k] = jnp.zeros(out.shape[1:], F32)
        live = counts[k]

        def some(step, _, k=k, live=live):
            sums = [[None] * 3 for _ in range(FMAX + 1)]
            for part in range(per_step):
                s = step * per_step + part
                r = radius[s, k]
                number = jnp.where(s < live, weight[s, k], 0.0)
                area = number * r * r
                terms = []
                for t in (number, area, area * r):
                    high = t.astype(jnp.bfloat16).astype(F32)
                    terms += [high, t - high]
                cols = column[s, k]
                left, right = [], []
                for j in range(ROWS):
                    left.append(
                        jnp.concatenate([jnp.where(row == j, t, 0.0) for t in terms], axis=0)
                    )
                    right.append(jnp.where(cols[j : j + 1] == target, 1.0, 0.0).astype(F32))
                sent = lax.dot_general(
                    jnp.concatenate(left, axis=1),
                    jnp.concatenate(right, axis=1),
                    (((1,), (1,)), ((), ())),
                    preferred_element_type=F32,
                )
                depth = jnp.broadcast_to(fall_depth[s, k], (ROWS, COLS))
                for d in range(FMAX + 1):
                    falls = depth == d
                    for m in range(3):
                        both = sent[16 * m : 16 * m + 8] + sent[16 * m + 8 : 16 * m + 16]
                        value = jnp.where(falls, both, 0.0)
                        sums[d][m] = value if sums[d][m] is None else sums[d][m] + value
            for d in range(FMAX + 1):
                for m in range(3):
                    out[k, d, m] += sums[d][m]
            return 0

        lax.fori_loop(0, slots // per_step, some, 0)


def vmem(n):
    return [pl.BlockSpec(memory_space=pltpu.VMEM)] * n


def smem(n):
    return [pl.BlockSpec(memory_space=pltpu.SMEM)] * n


def anywhere(n):
    return [pl.BlockSpec(memory_space=pl.ANY)] * n


def shaped(*dims):
    return jax.ShapeDtypeStruct(dims, F32)


def held(*dims):
    return pltpu.VMEM(dims, F32)


def call(kernel, name, ins, outs, scratch=(), out_specs=None, flops=None, grant=4):
    made = pl.pallas_call(
        kernel,
        name=name,
        in_specs=ins,
        out_specs=tuple(out_specs or vmem(len(outs))),
        out_shape=tuple(outs),
        scratch_shapes=list(scratch),
        compiler_params=pltpu.CompilerParams(vmem_limit_bytes=grant << 20),
        cost_estimate=(
            pl.CostEstimate(flops=flops, bytes_accessed=0, transcendentals=0) if flops else None
        ),
    )

    def run(*operands):
        return made(
            *(
                pltpu.with_memory_space_constraint(value, pltpu.VMEM)
                if spec.memory_space == pltpu.VMEM
                else value
                for spec, value in zip(ins, operands)
            )
        )

    return run


def both_ways(down, axis, up):
    count = lax.axis_size(axis)
    return (
        lax.ppermute(down, axis, [((i + 1) % count, i) for i in range(count)]),
        lax.ppermute(up, axis, [(i, (i + 1) % count) for i in range(count)]),
    )


def exchange(plan, own, down, up, tokens=()):
    above, below = both_ways(down, "gy", up)
    to_left, to_right = call(
        pack_columns(plan),
        "pack_columns",
        vmem(3) + anywhere(len(tokens)),
        [held(LEVELS, ROWS, COLS)] * 2,
    )(own, above, below, *tokens)
    from_right, from_left = both_ways(to_left, "gx", to_right)
    tiles = len(plan.carried)
    to_down, to_up = call(
        pack_levels(plan), "pack_levels", vmem(5), [held(tiles, ROWS, COLS)] * 2
    )(own, above, below, from_right, from_left)
    from_up, from_down = both_ways(to_down, "gz", to_up)
    return above, below, from_right, from_left, from_up, from_down


def prepare(place_ref, fields, own, speed):
    own[...] = fields[...]
    keep = jnp.where(place_ref[0] == place_ref[1], 0.0, 1.0).astype(F32)
    most = jnp.zeros((ROWS, COLS), F32)
    for k in range(LEVELS):
        w = jnp.abs(fields[W, k])
        if k == LEVELS - 1:
            w = w * keep
        most = jnp.maximum(most, jnp.abs(fields[U, k]) + jnp.abs(fields[V, k]) + w)
    speed[...] = jnp.broadcast_to(jnp.max(most), speed.shape)


def droplets(radius, weight, column, counts, fall_depth, chunk):
    slots = radius.shape[0]
    made = []
    for n in range(LEVELS // chunk):
        whole = pl.BlockSpec((slots, chunk, ROWS, COLS), lambda i, n=n: (0, n, 0, 0))
        made.append(
            pl.pallas_call(
                deposit,
                name="deposit",
                grid=(1,),
                in_specs=[
                    whole,
                    whole,
                    whole,
                    pl.BlockSpec((chunk, ROWS, COLS), lambda i, n=n: (n, 0, 0)),
                    pl.BlockSpec((slots, chunk, ROWS, 1), lambda i, n=n: (0, n, 0, 0)),
                ],
                out_specs=pl.BlockSpec(
                    (chunk, FMAX + 1, 3, ROWS, COLS), lambda i: (0, 0, 0, 0, 0)
                ),
                out_shape=shaped(chunk, FMAX + 1, 3, ROWS, COLS),
                compiler_params=pltpu.CompilerParams(vmem_limit_bytes=12 << 20),
                cost_estimate=pl.CostEstimate(
                    flops=200_000_000, bytes_accessed=0, transcendentals=0
                ),
            )(radius, weight, column, counts, fall_depth)
        )
    return made


def per_device(fields, radius, weight, column, counts, fall_depth):
    place = lax.axis_index("gz")
    last = lax.axis_size("gz") - 1
    where = jnp.stack([place, jnp.int32(last)]).astype(jnp.int32)
    by_depth = droplets(radius, weight, column, counts, fall_depth, 2)
    devices = lax.axis_size(GRID_AXES)
    own, speed = pl.pallas_call(
        prepare,
        name="prepare",
        in_specs=smem(1) + vmem(1),
        out_specs=tuple(vmem(2)),
        out_shape=(held(5, LEVELS, ROWS, COLS), shaped(devices, 1, COLS)),
        compiler_params=pltpu.CompilerParams(vmem_limit_bytes=4 << 20),
    )(where, fields)
    early = EARLY
    halos = exchange(FIRST, own, fields, fields, by_depth[:early])
    speed, _ = lax.optimization_barrier((speed, halos[2]))
    speed = lax.all_to_all(speed, GRID_AXES, 0, 0)
    start, rate0 = call(
        first_rates,
        "first_rates",
        smem(1) + vmem(7) + anywhere(1),
        [held(len(FIRST.tiles), DEPTH, ROWS, WIDE), held(2, DEPTH, 2 * ROWS, WIDE)],
    )(where, own, *halos, speed)
    s2, down, up, dt = call(
        two_sections,
        "two_sections",
        smem(1) + vmem(3),
        [held(5, LEVELS, ROWS, COLS)] + [held(3, LEVELS, ROWS, COLS)] * 2 + [shaped(1)],
        scratch=[
            pltpu.VMEM((5, DEPTH, 2 * ROWS, WIDE), F32),
            pltpu.VMEM((DEPTH, 2 * ROWS, WIDE), F32),
            pltpu.VMEM((4, DEPTH, 2 * ROWS, WIDE), F32),
        ],
        out_specs=vmem(3) + smem(1),
        grant=10,
    )(where, speed, start, rate0)
    halos = exchange(SECOND, s2, down, up, by_depth[early:])
    ext, tracer, landed, fallen = call(
        last_tracer,
        "last_tracer",
        smem(2) + vmem(8) + anywhere(len(by_depth)),
        [
            held(len(SECOND.tiles), DEPTH, ROWS, WIDE),
            held(LEVELS, ROWS, COLS),
            held(3, LEVELS, ROWS, COLS),
            held(3, FMAX, ROWS, COLS),
        ],
        scratch=[
            pltpu.VMEM((2, LEVELS, ROWS, COLS), F32),
            pltpu.VMEM((LEVELS, FMAX + 1, 3, ROWS, COLS), F32),
            pltpu.SemaphoreType.DMA((len(by_depth),)),
        ],
    )(where, dt, s2, *halos, start, *by_depth)
    count = lax.axis_size("gz")
    arrived = lax.ppermute(fallen, "gz", [((i + 1) % count, i) for i in range(count)])
    (new_fields,) = call(
        last_section,
        "last_section",
        smem(2) + vmem(3),
        [shaped(5, LEVELS, ROWS, COLS)],
        scratch=[
            pltpu.VMEM((DEPTH, 2 * ROWS, WIDE), F32),
            pltpu.VMEM((4, DEPTH, 2 * ROWS, WIDE), F32),
        ],
        flops=1_000_000_000,
        grant=8,
    )(where, dt, ext, start, tracer)
    arrived = jnp.where(place == last, 0.0, arrived)
    moments = landed.at[:, LEVELS - FMAX :].add(arrived)
    return (new_fields, moments)


def solution(mesh):
    spread = P(None, "gz", "gy", "gx")
    return jax.shard_map(
        per_device,
        mesh=mesh,
        in_specs=(spread, spread, spread, spread, P("gz", "gy", "gx"), spread),
        out_specs=(spread, spread),
        check_vma=False,
    )
```

```python
import jax
import jax.numpy as jnp
from jax import lax
from jax.experimental import pallas as pl
from jax.experimental.pallas import tpu as pltpu
from jax.sharding import PartitionSpec as P

NS = 4
FMAX = 8
EARLY, LATE = 4, 7
GRID_AXES = ("gx", "gy", "gz")

sound_speed = 10.0
buoyancy = 0.5
courant_goal = 0.6
growth = 0.3

LEVELS, ROWS, COLS = 16, 8, 128
WIDE = 2 * COLS
REACH = 7
DEPTH = LEVELS + 2 * REACH
EDGE = 8
F32 = jnp.float32
C, PR, U, V, W = range(5)


class Plan:
    def __init__(self, tall, reach, sent):
        self.tall, self.reach = tall, reach
        self.tiles = [
            (field, part)
            for field in range(5)
            for part in ("oab" if field in tall else "on")
        ]
        self.at = {tile: n for n, tile in enumerate(self.tiles)}
        self.carried = []
        for a in range(reach):
            for field in range(5):
                for part in sent[field][a] if a < len(sent[field]) else "":
                    self.carried.append((a, (field, part), 0))
            if a < reach - 1:
                self.carried += [(a, None, 0), (a, None, 1)]

    def rows(self, ref, field, l):
        return jnp.concatenate(
            [
                ref[self.at[field, part], l]
                for part in ("oab" if field in self.tall else "on")
            ],
            axis=0,
        )

    def sixteen(self, ref, field, l):
        value = self.rows(ref, field, l)
        return sixteen(value) if field in self.tall else value


def lanes(shape):
    return lax.broadcasted_iota(jnp.int32, shape, len(shape) - 1)


def lower_rows(shape):
    return lax.broadcasted_iota(jnp.int32, shape, 0) < ROWS // 2


def around(above, below):
    return jnp.where(lower_rows(above.shape), above, below)


def sixteen(value):
    return jnp.concatenate(
        [value[0:ROWS], around(value[ROWS : 2 * ROWS], value[2 * ROWS :])], axis=0
    )


def raw_tile(refs, field, part, k):
    own, above, below = refs
    if part == "o":
        return own[field, k]
    if part == "n":
        return around(above[field, k], below[field, k])
    return (above if part == "a" else below)[field, k]


SHARED = {C: (1, 0), U: (1, 1), V: (2, 0), W: (2, 1)}


def shared_rows(read):
    down, up = [read(PR)], [read(PR)]
    for first, second in ((C, U), (V, W)):
        one, other = read(first), pltpu.roll(read(second), ROWS // 2, 0)
        down.append(around(one, other))
        up.append(around(other, one))
    return down, up


def shared_tile(refs, field, part, k):
    own, above, below = refs
    if part == "o":
        return own[field, k]
    if part == "n" and field == PR:
        return around(above[0, k], below[0, k])
    if part == "n":
        index, half = SHARED[field]
        if half == 0:
            return around(above[index, k], below[index, k])
        return pltpu.roll(around(below[index, k], above[index, k]), ROWS // 2, 0)
    return (above if part == "a" else below)[0, k]


THREE, TWO, ONE = "oab", "on", "o"
FIRST = Plan(
    (C, PR, V),
    7,
    {
        C: [THREE] + [TWO] * 4 + [ONE],
        PR: [THREE] * 2 + [TWO] * 4 + [ONE],
        U: [TWO] * 4,
        V: [TWO] * 4,
        W: [TWO] * 4 + [ONE],
    },
)
SECOND = Plan(
    (PR,),
    6,
    {
        C: [TWO] * 3 + [ONE],
        PR: [THREE] + [TWO] * 4 + [ONE],
        U: [TWO] * 3,
        V: [TWO] * 3,
        W: [TWO] * 3 + [ONE],
    },
)
TILE_OF = {FIRST: raw_tile, SECOND: shared_tile}


def pack_columns(plan):
    def kernel(own, above, below, *rest):
        to_left, to_right = rest[-2:]
        lane = lanes((ROWS, COLS))

        def one(k, _):
            left = jnp.zeros((ROWS, COLS), F32)
            right = jnp.zeros((ROWS, COLS), F32)
            for n, (field, part) in enumerate(plan.tiles):
                start = n * EDGE
                here = (lane >= start) & (lane < start + EDGE)
                value = TILE_OF[plan]((own, above, below), field, part, k)
                first = pltpu.roll(value, start, 1) if start else value
                last = pltpu.roll(value, (start + EDGE) % COLS, 1)
                left = jnp.where(here, first, left)
                right = jnp.where(here, last, right)
            to_left[k] = left
            to_right[k] = right
            return 0

        def pair(i, _):
            one(2 * i, 0)
            return one(2 * i + 1, 0)

        lax.fori_loop(0, LEVELS // 2, pair, 0)

    return kernel


def halo_columns(from_right, from_left, n):
    start = n * EDGE
    right = pltpu.roll(from_right, COLS - start, 1) if start else from_right
    left = pltpu.roll(from_left, (COLS - EDGE - start) % COLS, 1)
    return jnp.where(lanes((ROWS, COLS)) < COLS // 2, right, left)


def pack_levels(plan):
    def kernel(own, above, below, from_right, from_left, to_down, to_up):
        for index, (a, tile, side) in enumerate(plan.carried):
            for out, k in ((to_down, a), (to_up, LEVELS - 1 - a)):
                if tile:
                    out[index] = TILE_OF[plan]((own, above, below), *tile, k)
                else:
                    out[index] = (from_left if side else from_right)[k]

    return kernel


def place_own(plan, refs, ext):
    own, above, below, from_right, from_left = refs

    def middle(levels, _):
        for k in levels:
            right, left = from_right[k], from_left[k]
            for n, (field, part) in enumerate(plan.tiles):
                ext[n, REACH + k, :, 0:COLS] = TILE_OF[plan]((own, above, below), field, part, k)
                ext[n, REACH + k, :, COLS:WIDE] = halo_columns(right, left, n)
        return 0

    sweep(0, LEVELS, 4, middle)


def place_halo(plan, from_up, from_down, ext, place, last):
    columns = {(a, side): i for i, (a, tile, side) in enumerate(plan.carried) if not tile}
    for message, level, there in (
        (from_down, lambda a: REACH - 1 - a, place > 0),
        (from_up, lambda a: REACH + LEVELS + a, place < last),
    ):
        keep = jnp.where(there, 1.0, 0.0).astype(F32)
        for index, (a, tile, _) in enumerate(plan.carried):
            if not tile:
                continue
            field, part = tile
            value = message[index] * keep
            for kept in "ab" if part == "n" and field in plan.tall else part:
                n = plan.at[field, kept]
                ext[n, level(a), :, 0:COLS] = value
                if (a, 0) in columns:
                    ext[n, level(a), :, COLS:WIDE] = (
                        halo_columns(message[columns[a, 0]], message[columns[a, 1]], n) * keep
                    )


def shift(value, by, axis):
    return pltpu.roll(value, (-by) % value.shape[axis], axis)


def face_flux(q, wind):
    central = 37.0 * (q[2] + q[3]) - 8.0 * (q[1] + q[4]) + (q[0] + q[5])
    upwind = 10.0 * (q[3] - q[2]) - 5.0 * (q[4] - q[1]) + (q[5] - q[0])
    return wind * central - jnp.abs(wind) * upwind


def flat_flux(q, wind, axis):
    flux = face_flux([shift(q, by, axis) if by else q for by in range(-2, 4)], wind)
    return flux - shift(flux, -1, axis)


def rows_flux(q, wind):
    if wind.shape[0] == 24:
        return sixteen(flat_flux(q, wind, 0))
    if q.shape[0] == 24:
        flux = face_flux([sixteen(shift(q, by, 0) if by else q) for by in range(-2, 4)], wind)
        return flux - shift(flux, -1, 0)
    return flat_flux(q, wind, 0)


def level_flux(read, wind, l):
    return face_flux([read(l + by) for by in range(-2, 4)], wind)


def in_domain(l, place, last, lid):
    g = place * LEVELS + l - REACH
    top = (last + 1) * LEVELS - (1 if lid else 0)
    return jnp.where((g >= 0) & (g < top), 1.0, 0.0).astype(F32)


SIXTIETH = -1.0 / 60.0


def sweep(first, count, most, body, carry=0):
    size = max(n for n in range(1, most + 1) if count % n == 0)

    def run(i, carry):
        start = first + i * size
        return body([start + n for n in range(size)], carry)

    return lax.fori_loop(0, count // size, run, carry)


def flat_part(plan, ext, field, l):
    return flat_flux(plan.sixteen(ext, field, l), plan.sixteen(ext, U, l), 1) + rows_flux(
        plan.rows(ext, field, l), plan.rows(ext, V, l)
    )


def flat_own(plan, ext, fields, flat):
    def some(levels, _):
        results = [(n, l, flat_part(plan, ext, f, l)) for l in levels for n, f in enumerate(fields)]
        for n, l, value in results:
            flat[n, l - REACH] = value
        return 0

    sweep(REACH, LEVELS, 2, some)


def rates(plan, ext, fields, write, around_own, most, flat=None):
    reads = [lambda l, f=f: plan.sixteen(ext, f, l) for f in fields]

    def some(levels, lows, flat=None):
        results = []
        for l in levels:
            w = plan.sixteen(ext, W, l)
            highs = []
            for n, f in enumerate(fields):
                high = level_flux(reads[n], w, l)
                level = flat[n, l - REACH] if flat is not None else flat_part(plan, ext, f, l)
                results.append((n, l, (level + (high - lows[n])) * SIXTIETH))
                highs.append(high)
            lows = tuple(highs)
        for result in results:
            write(*result)
        return lows

    first = REACH - around_own
    w = plan.sixteen(ext, W, first - 1)
    lows = tuple(level_flux(read, w, first - 1) for read in reads)
    if flat is None:
        sweep(first, LEVELS + 2 * around_own, most, some, lows)
        return
    lows = sweep(first, around_own, most, some, lows)
    lows = sweep(REACH, LEVELS, 4, lambda levels, c: some(levels, c, flat), lows)
    sweep(REACH + LEVELS, around_own, most, some, lows)


def first_own(place_ref, own, above, below, from_right, from_left, ext, flat):
    place_own(FIRST, (own, above, below, from_right, from_left), ext)

    @pl.when(place_ref[0] == place_ref[1])
    def _():
        for part in "on":
            ext[FIRST.at[W, part], REACH + LEVELS - 1] = jnp.zeros((ROWS, WIDE), F32)

    flat_own(FIRST, ext, (C, PR), flat)


def first_rates(place_ref, ext_in, flat, from_up, from_down, speed, ext, rate):
    place_halo(FIRST, from_up, from_down, ext, place_ref[0], place_ref[1])

    def write(n, l, value):
        rate[n, l] = value

    rates(FIRST, ext, (C, PR), write, 4, 2, flat)


def acoustic(p, u, v, w, read_c, rate, step, first, count, place, last):
    pull = step * sound_speed

    def level(value):
        return sixteen(value) if value.shape[0] == 24 else value

    def wind_w(l, lift_low, lift_high, p_here, p_above):
        lift = (buoyancy * 0.5) * (lift_low + lift_high)
        return (w[0](l) + step * lift - pull * (p_above - p_here)) * in_domain(l, place, last, True)

    def some(levels, w_low):
        talls = [p[0](l) for l in (*levels, levels[-1] + 1)]
        cells = [level(value) for value in talls]
        warm = [read_c(l) for l in (*levels, levels[-1] + 1)]
        results = []
        for n, l in enumerate(levels):
            p_here = cells[n]
            w_new = wind_w(l, warm[n], warm[n + 1], p_here, cells[n + 1])
            u_new = u[0](l) - pull * (shift(p_here, 1, 1) - p_here)
            v_old = v[0](l)
            if v_old.shape[0] == 24:
                v_tall = v_old - pull * (shift(talls[n], 1, 0) - talls[n])
                v_new, v_flow = sixteen(v_tall), sixteen(v_tall - shift(v_tall, -1, 0))
            else:
                v_new = v_old - pull * (shift(p_here, 1, 0) - p_here)
                v_flow = v_new - shift(v_new, -1, 0)
            divergence = (u_new - shift(u_new, -1, 1)) + v_flow + (w_new - w_low)
            p_new = (p_here + step * rate(l) - pull * divergence) * in_domain(
                l, place, last, False
            )
            results.append((l, p_new, u_new, v_new, w_new))
            w_low = w_new
        for l, *news in results:
            for target, value in zip((p, u, v, w), news):
                target[1](l, value)
        return w_low

    low = first - 1
    w_low = wind_w(low, read_c(low), read_c(first), level(p[0](low)), level(p[0](first)))
    w[1](low, w_low)
    sweep(first, count, 6, some, w_low)


def access(ref, *lead):
    def read(l):
        return ref[(*lead, l)]

    def write(l, value):
        ref[(*lead, l)] = value

    return read, write


def begin(start, field, tall=False):
    return lambda l: (FIRST.rows if tall else FIRST.sixteen)(start, field, l)


def own_write(ref, field):
    def write(l, value):
        if not isinstance(l, int):
            ref[field, l - REACH] = value[0:ROWS, 0:COLS]

    return write


def tracer_flat(tiles, u, v, l):
    rows = flat_flux(tiles(l)[:, 0:COLS], v(l)[:, 0:COLS], 0)[0:ROWS]
    return rows + flat_flux(tiles(l)[0:ROWS], u(l)[0:ROWS], 1)[:, 0:COLS]


def tracer_high(tiles, w, l):
    return level_flux(lambda m: tiles(m)[0:ROWS, 0:COLS], w(l)[0:ROWS, 0:COLS], l)


def two_sections(place_ref, speed, start, rate0, s2, down, up, dt_out, s1, rate1, fast):
    place, last = place_ref[0], place_ref[1]
    dt = courant_goal / (1.0 + jnp.max(speed[...]))
    dt_out[0] = dt
    third = dt * (1.0 / 3.0)

    def tracer(levels, _):
        for l in levels:
            s1[C, l] = (FIRST.sixteen(start, C, l) + third * rate0[0, l]) * in_domain(
                l, place, last, False
            )
        return 0

    sweep(REACH - 4, LEVELS + 8, 4, tracer)
    acoustic(
        (begin(start, PR, True), access(s1, PR)[1]),
        (begin(start, U), access(s1, U)[1]),
        (begin(start, V, True), access(s1, V)[1]),
        (begin(start, W), access(s1, W)[1]),
        begin(start, C),
        access(rate0, 1)[0],
        third,
        REACH - 4,
        LEVELS + 8,
        place,
        last,
    )
    half = dt * 0.5
    tiles = access(s1, C)[0]
    winds = [access(s1, f)[0] for f in (U, V, W)]

    def own_tracer(levels, low):
        results = []
        for l in levels:
            high = tracer_high(tiles, winds[2], l)
            tendency = (tracer_flat(tiles, *winds[:2], l) + (high - low)) * SIXTIETH
            low = high
            results.append(start[FIRST.at[C, "o"], l, :, 0:COLS] + half * tendency)
        for l, value in zip(levels, results):
            s2[C, l - REACH] = value
        return low

    sweep(REACH, LEVELS, 4, own_tracer, tracer_high(tiles, winds[2], REACH - 1))

    def write(n, l, value):
        rate1[l] = value

    rates(SECTION, s1, (PR,), write, 1, 3)
    step = half / (NS // 2)
    acoustic(
        (begin(start, PR), access(fast, 0)[1]),
        (begin(start, U), access(fast, 1)[1]),
        (begin(start, V), access(fast, 2)[1]),
        (begin(start, W), access(fast, 3)[1]),
        access(s1, C)[0],
        access(rate1)[0],
        step,
        REACH - 1,
        LEVELS + 2,
        place,
        last,
    )
    acoustic(
        (access(fast, 0)[0], own_write(s2, PR)),
        (access(fast, 1)[0], own_write(s2, U)),
        (access(fast, 2)[0], own_write(s2, V)),
        (access(fast, 3)[0], own_write(s2, W)),
        access(s1, C)[0],
        access(rate1)[0],
        step,
        REACH,
        LEVELS,
        place,
        last,
    )

    def share(levels, _):
        made = [shared_rows(lambda f, k=k: s2[f, k]) for k in levels]
        for k, (to_down, to_up) in zip(levels, made):
            for n in range(3):
                down[n, k] = to_down[n]
                up[n, k] = to_up[n]
        return 0

    sweep(0, LEVELS, 4, share)


class Whole:
    def rows(self, ref, field, l):
        return ref[field, l]

    sixteen = rows


SECTION = Whole()


def second_own(own, above, below, from_right, from_left, ext, flat, tracer):
    place_own(SECOND, (own, above, below, from_right, from_left), ext)
    flat_own(SECOND, ext, (PR,), flat)
    tiles, u, v = (lambda l, f=f: SECOND.rows(ext, f, l) for f in (C, U, V))

    def some(levels, _):
        results = [tracer_flat(tiles, u, v, l) for l in levels]
        for l, value in zip(levels, results):
            tracer[l - REACH] = value
        return 0

    sweep(REACH, LEVELS, 4, some)


def last_tracer(place_ref, dt_ref, ext_in, flat_tracer, from_up, from_down, initial, *rest):
    *chunks, ext, tracer, landed, fallen, factor, by_depth, sem = rest
    dt = dt_ref[0]
    each = LEVELS // len(chunks)
    copies = [
        pltpu.make_async_copy(chunk, by_depth.at[pl.ds(n * each, each)], sem.at[n])
        for n, chunk in enumerate(chunks)
    ]
    for copy in copies:
        copy.start()
    place_halo(SECOND, from_up, from_down, ext, place_ref[0], place_ref[1])
    tiles = lambda l: SECOND.rows(ext, C, l)
    w = lambda l: SECOND.rows(ext, W, l)

    def some(levels, low):
        results = []
        for l in levels:
            high = tracer_high(tiles, w, l)
            tendency = (flat_tracer[l - REACH] + (high - low)) * SIXTIETH
            low = high
            c = initial[C, l - REACH] + dt * tendency
            grown = jnp.exp(growth * c)
            results.append((c, grown, grown * jnp.exp((0.5 * growth) * c)))
        for l, (c, second, third) in zip(levels, results):
            tracer[l - REACH] = c
            factor[0, l - REACH] = second
            factor[1, l - REACH] = third
        return low

    sweep(REACH, LEVELS, 4, some, tracer_high(tiles, w, REACH - 1))
    for copy in copies:
        copy.wait()
    for target in range(-FMAX, LEVELS):
        for moment in range(3):
            total = None
            for depth in range(FMAX + 1):
                k = target + depth
                if 0 <= k < LEVELS:
                    value = by_depth[k, depth, moment]
                    if moment:
                        value = value * factor[moment - 1, k]
                    total = value if total is None else total + value
            if target < 0:
                fallen[moment, target + FMAX] = total
            else:
                landed[moment, target] = total


def last_section(place_ref, dt_ref, ext, flat, start_far, tracer, out, rate, fast, start, sem):
    place, last = place_ref[0], place_ref[1]
    step = dt_ref[0] / NS
    copy = pltpu.make_async_copy(start_far, start, sem)
    copy.start()

    def write(n, l, value):
        rate[l] = value

    rates(SECOND, ext, (PR,), write, 3, 3, flat)
    out[C] = tracer[...]
    copy.wait()
    names = (PR, U, V, W)
    for repeat in range(NS):
        reads = [
            begin(start, f) if repeat == 0 else access(fast, n)[0] for n, f in enumerate(names)
        ]
        writes = [
            own_write(out, f) if repeat == NS - 1 else access(fast, n)[1]
            for n, f in enumerate(names)
        ]
        acoustic(
            *zip(reads, writes),
            lambda l: SECOND.rows(ext, C, l),
            access(rate)[0],
            step,
            REACH - 3 + repeat,
            LEVELS + 6 - 2 * repeat,
            place,
            last,
        )


def deposit(radius, weight, column, counts, fall_depth, out):
    slots, levels = radius.shape[0], radius.shape[1]
    target = lax.broadcasted_iota(jnp.int32, (COLS, COLS), 0)
    row = lax.broadcasted_iota(jnp.int32, (ROWS, COLS), 0)
    per_step = 4

    for k in range(levels):
        out[k] = jnp.zeros(out.shape[1:], F32)
        live = counts[k]

        def some(step, _, k=k, live=live):
            sums = [[None] * 3 for _ in range(FMAX + 1)]
            for part in range(per_step):
                s = step * per_step + part
                r = radius[s, k]
                number = jnp.where(s < live, weight[s, k], 0.0)
                area = number * r * r
                terms = []
                for t in (number, area, area * r):
                    high = t.astype(jnp.bfloat16).astype(F32)
                    terms += [high, t - high]
                cols = column[s, k]
                left, right = [], []
                for j in range(ROWS):
                    left.append(
                        jnp.concatenate([jnp.where(row == j, t, 0.0) for t in terms], axis=0)
                    )
                    right.append(jnp.where(cols[j : j + 1] == target, 1.0, 0.0).astype(F32))
                sent = lax.dot_general(
                    jnp.concatenate(left, axis=1),
                    jnp.concatenate(right, axis=1),
                    (((1,), (1,)), ((), ())),
                    preferred_element_type=F32,
                )
                depth = jnp.broadcast_to(fall_depth[s, k], (ROWS, COLS))
                for d in range(FMAX + 1):
                    falls = depth == d
                    for m in range(3):
                        both = sent[16 * m : 16 * m + 8] + sent[16 * m + 8 : 16 * m + 16]
                        value = jnp.where(falls, both, 0.0)
                        sums[d][m] = value if sums[d][m] is None else sums[d][m] + value
            for d in range(FMAX + 1):
                for m in range(3):
                    out[k, d, m] += sums[d][m]
            return 0

        lax.fori_loop(0, slots // per_step, some, 0)


def vmem(n):
    return [pl.BlockSpec(memory_space=pltpu.VMEM)] * n


def smem(n):
    return [pl.BlockSpec(memory_space=pltpu.SMEM)] * n


def anywhere(n):
    return [pl.BlockSpec(memory_space=pl.ANY)] * n


def shaped(*dims):
    return jax.ShapeDtypeStruct(dims, F32)


def held(*dims):
    return pltpu.VMEM(dims, F32)


def call(kernel, name, ins, outs, scratch=(), out_specs=None, flops=None, grant=4, alias=None):
    made = pl.pallas_call(
        kernel,
        name=name,
        in_specs=ins,
        out_specs=tuple(out_specs or vmem(len(outs))),
        out_shape=tuple(outs),
        scratch_shapes=list(scratch),
        input_output_aliases=alias or {},
        compiler_params=pltpu.CompilerParams(vmem_limit_bytes=grant << 20),
        cost_estimate=(
            pl.CostEstimate(flops=flops, bytes_accessed=0, transcendentals=0) if flops else None
        ),
    )

    def run(*operands):
        return made(
            *(
                pltpu.with_memory_space_constraint(value, pltpu.VMEM)
                if spec.memory_space == pltpu.VMEM
                else value
                for spec, value in zip(ins, operands)
            )
        )

    return run


def both_ways(down, axis, up):
    count = lax.axis_size(axis)
    return (
        lax.ppermute(down, axis, [((i + 1) % count, i) for i in range(count)]),
        lax.ppermute(up, axis, [(i, (i + 1) % count) for i in range(count)]),
    )


def exchange(plan, own, down, up, tokens=()):
    above, below = both_ways(down, "gy", up)
    to_left, to_right = call(
        pack_columns(plan),
        "pack_columns",
        vmem(3) + anywhere(len(tokens)),
        [held(LEVELS, ROWS, COLS)] * 2,
    )(own, above, below, *tokens)
    from_right, from_left = both_ways(to_left, "gx", to_right)
    tiles = len(plan.carried)
    to_down, to_up = call(
        pack_levels(plan), "pack_levels", vmem(5), [held(tiles, ROWS, COLS)] * 2
    )(own, above, below, from_right, from_left)
    from_up, from_down = both_ways(to_down, "gz", to_up)
    return above, below, from_right, from_left, from_up, from_down


def prepare(place_ref, fields, own, speed):
    own[...] = fields[...]
    keep = jnp.where(place_ref[0] == place_ref[1], 0.0, 1.0).astype(F32)
    most = jnp.zeros((ROWS, COLS), F32)
    for k in range(LEVELS):
        w = jnp.abs(fields[W, k])
        if k == LEVELS - 1:
            w = w * keep
        most = jnp.maximum(most, jnp.abs(fields[U, k]) + jnp.abs(fields[V, k]) + w)
    speed[...] = jnp.broadcast_to(jnp.max(most), speed.shape)


def droplets(radius, weight, column, counts, fall_depth, chunk):
    slots = radius.shape[0]
    made = []
    for n in range(LEVELS // chunk):
        whole = pl.BlockSpec((slots, chunk, ROWS, COLS), lambda i, n=n: (0, n, 0, 0))
        made.append(
            pl.pallas_call(
                deposit,
                name="deposit",
                grid=(1,),
                in_specs=[
                    whole,
                    whole,
                    whole,
                    pl.BlockSpec((chunk, ROWS, COLS), lambda i, n=n: (n, 0, 0)),
                    pl.BlockSpec((slots, chunk, ROWS, 1), lambda i, n=n: (0, n, 0, 0)),
                ],
                out_specs=pl.BlockSpec(
                    (chunk, FMAX + 1, 3, ROWS, COLS), lambda i: (0, 0, 0, 0, 0)
                ),
                out_shape=shaped(chunk, FMAX + 1, 3, ROWS, COLS),
                compiler_params=pltpu.CompilerParams(vmem_limit_bytes=12 << 20),
                cost_estimate=pl.CostEstimate(
                    flops=200_000_000, bytes_accessed=0, transcendentals=0
                ),
            )(radius, weight, column, counts, fall_depth)
        )
    return made


def per_device(fields, radius, weight, column, counts, fall_depth):
    place = lax.axis_index("gz")
    last = lax.axis_size("gz") - 1
    where = jnp.stack([place, jnp.int32(last)]).astype(jnp.int32)
    by_depth = droplets(radius, weight, column, counts, fall_depth, 2)
    devices = lax.axis_size(GRID_AXES)
    own, speed = pl.pallas_call(
        prepare,
        name="prepare",
        in_specs=smem(1) + vmem(1),
        out_specs=tuple(vmem(2)),
        out_shape=(held(5, LEVELS, ROWS, COLS), shaped(devices, 1, COLS)),
        compiler_params=pltpu.CompilerParams(vmem_limit_bytes=4 << 20),
    )(where, fields)
    *near, from_up, from_down = exchange(FIRST, own, fields, fields, by_depth[:EARLY])
    ext = held(len(FIRST.tiles), DEPTH, ROWS, WIDE)
    start, flat = call(
        first_own,
        "first_own",
        smem(1) + vmem(5),
        [ext, held(2, LEVELS, 2 * ROWS, WIDE)],
    )(where, own, *near)
    speed, flat = lax.optimization_barrier((speed, flat))
    speed = lax.all_to_all(speed, GRID_AXES, 0, 0)
    start, rate0 = call(
        first_rates,
        "first_rates",
        smem(1) + vmem(4) + anywhere(1),
        [ext, held(2, DEPTH, 2 * ROWS, WIDE)],
        alias={1: 0},
    )(where, start, flat, from_up, from_down, speed)
    s2, down, up, dt = call(
        two_sections,
        "two_sections",
        smem(1) + vmem(3),
        [held(5, LEVELS, ROWS, COLS)] + [held(3, LEVELS, ROWS, COLS)] * 2 + [shaped(1)],
        scratch=[
            pltpu.VMEM((5, DEPTH, 2 * ROWS, WIDE), F32),
            pltpu.VMEM((DEPTH, 2 * ROWS, WIDE), F32),
            pltpu.VMEM((4, DEPTH, 2 * ROWS, WIDE), F32),
        ],
        out_specs=vmem(3) + smem(1),
        grant=10,
    )(where, speed, start, rate0)
    *near, from_up, from_down = exchange(SECOND, s2, down, up, by_depth[EARLY:LATE])
    ext = held(len(SECOND.tiles), DEPTH, ROWS, WIDE)
    around_s2, flat, flat_tracer = call(
        second_own,
        "second_own",
        vmem(5),
        [ext, held(1, LEVELS, 2 * ROWS, WIDE), held(LEVELS, ROWS, COLS)],
        flops=1_000_000_000,
    )(s2, *near)
    around_s2, tracer, landed, fallen = call(
        last_tracer,
        "last_tracer",
        smem(2) + vmem(5) + anywhere(len(by_depth)),
        [
            ext,
            held(LEVELS, ROWS, COLS),
            held(3, LEVELS, ROWS, COLS),
            held(3, FMAX, ROWS, COLS),
        ],
        scratch=[
            pltpu.VMEM((2, LEVELS, ROWS, COLS), F32),
            pltpu.VMEM((LEVELS, FMAX + 1, 3, ROWS, COLS), F32),
            pltpu.SemaphoreType.DMA((len(by_depth),)),
        ],
        alias={2: 0},
    )(where, dt, around_s2, flat_tracer, from_up, from_down, own, *by_depth)
    count = lax.axis_size("gz")
    arrived = lax.ppermute(fallen, "gz", [((i + 1) % count, i) for i in range(count)])
    (new_fields,) = call(
        last_section,
        "last_section",
        smem(2) + vmem(2) + anywhere(1) + vmem(1),
        [shaped(5, LEVELS, ROWS, COLS)],
        scratch=[
            pltpu.VMEM((DEPTH, 2 * ROWS, WIDE), F32),
            pltpu.VMEM((4, DEPTH, 2 * ROWS, WIDE), F32),
            pltpu.VMEM((len(FIRST.tiles), DEPTH, ROWS, WIDE), F32),
            pltpu.SemaphoreType.DMA,
        ],
        flops=1_000_000_000,
        grant=12,
    )(where, dt, around_s2, flat, start, tracer)
    arrived = jnp.where(place == last, 0.0, arrived)
    moments = landed.at[:, LEVELS - FMAX :].add(arrived)
    return (new_fields, moments)


def solution(mesh):
    spread = P(None, "gz", "gy", "gx")
    return jax.shard_map(
        per_device,
        mesh=mesh,
        in_specs=(spread, spread, spread, spread, P("gz", "gy", "gx"), spread),
        out_specs=(spread, spread),
        check_vma=False,
    )
```

```python
import jax
import jax.numpy as jnp
from jax import lax
from jax.experimental import pallas as pl
from jax.experimental.pallas import tpu as pltpu
from jax.sharding import PartitionSpec as P

NS = 4
FMAX = 8
GRID_AXES = ("gx", "gy", "gz")

sound_speed = 10.0
buoyancy = 0.5
courant_goal = 0.6
growth = 0.3

LEVELS, ROWS, COLS = 16, 8, 128
WIDE = 2 * COLS
REACH = 7
DEPTH = LEVELS + 2 * REACH
EDGE = 8
F32 = jnp.float32
C, PR, U, V, W = range(5)


class Plan:
    def __init__(self, tall, reach, sent):
        self.tall, self.reach = tall, reach
        self.tiles = [
            (field, part)
            for field in range(5)
            for part in ("oab" if field in tall else "on")
        ]
        self.at = {tile: n for n, tile in enumerate(self.tiles)}
        self.carried = []
        for a in range(reach):
            for field in range(5):
                for part in sent[field][a] if a < len(sent[field]) else "":
                    self.carried.append((a, (field, part), 0))
            if a < reach - 1:
                self.carried += [(a, None, 0), (a, None, 1)]

    def rows(self, ref, field, l):
        return jnp.concatenate(
            [
                ref[self.at[field, part], l]
                for part in ("oab" if field in self.tall else "on")
            ],
            axis=0,
        )

    def sixteen(self, ref, field, l):
        value = self.rows(ref, field, l)
        return sixteen(value) if field in self.tall else value


def lanes(shape):
    return lax.broadcasted_iota(jnp.int32, shape, len(shape) - 1)


def lower_rows(shape):
    return lax.broadcasted_iota(jnp.int32, shape, 0) < ROWS // 2


def around(above, below):
    return jnp.where(lower_rows(above.shape), above, below)


def sixteen(value):
    return jnp.concatenate(
        [value[0:ROWS], around(value[ROWS : 2 * ROWS], value[2 * ROWS :])], axis=0
    )


def raw_tile(refs, field, part, k):
    own, above, below = refs
    if part == "o":
        return own[field, k]
    if part == "n":
        return around(above[field, k], below[field, k])
    return (above if part == "a" else below)[field, k]


SHARED = {C: (1, 0), U: (1, 1), V: (2, 0), W: (2, 1)}


def shared_rows(read):
    down, up = [read(PR)], [read(PR)]
    for first, second in ((C, U), (V, W)):
        one, other = read(first), pltpu.roll(read(second), ROWS // 2, 0)
        down.append(around(one, other))
        up.append(around(other, one))
    return down, up


def shared_tile(refs, field, part, k):
    own, above, below = refs
    if part == "o":
        return own[field, k]
    if part == "n" and field == PR:
        return around(above[0, k], below[0, k])
    if part == "n":
        index, half = SHARED[field]
        if half == 0:
            return around(above[index, k], below[index, k])
        return pltpu.roll(around(below[index, k], above[index, k]), ROWS // 2, 0)
    return (above if part == "a" else below)[0, k]


THREE, TWO, ONE = "oab", "on", "o"
FIRST = Plan(
    (C, PR, V),
    7,
    {
        C: [THREE] + [TWO] * 4 + [ONE],
        PR: [THREE] * 2 + [TWO] * 4 + [ONE],
        U: [TWO] * 4,
        V: [TWO] * 4,
        W: [TWO] * 4 + [ONE],
    },
)
SECOND = Plan(
    (PR,),
    6,
    {
        C: [TWO] * 3 + [ONE],
        PR: [THREE] + [TWO] * 4 + [ONE],
        U: [TWO] * 3,
        V: [TWO] * 3,
        W: [TWO] * 3 + [ONE],
    },
)
TILE_OF = {FIRST: raw_tile, SECOND: shared_tile}


def pack_columns(plan):
    def kernel(own, above, below, *rest):
        to_left, to_right = rest[-2:]
        lane = lanes((ROWS, COLS))

        def one(k, _):
            left = jnp.zeros((ROWS, COLS), F32)
            right = jnp.zeros((ROWS, COLS), F32)
            for n, (field, part) in enumerate(plan.tiles):
                start = n * EDGE
                here = (lane >= start) & (lane < start + EDGE)
                value = TILE_OF[plan]((own, above, below), field, part, k)
                first = pltpu.roll(value, start, 1) if start else value
                last = pltpu.roll(value, (start + EDGE) % COLS, 1)
                left = jnp.where(here, first, left)
                right = jnp.where(here, last, right)
            to_left[k] = left
            to_right[k] = right
            return 0

        def pair(i, _):
            one(2 * i, 0)
            return one(2 * i + 1, 0)

        lax.fori_loop(0, LEVELS // 2, pair, 0)

    return kernel


def halo_columns(from_right, from_left, n):
    start = n * EDGE
    right = pltpu.roll(from_right, COLS - start, 1) if start else from_right
    left = pltpu.roll(from_left, (COLS - EDGE - start) % COLS, 1)
    return jnp.where(lanes((ROWS, COLS)) < COLS // 2, right, left)


def pack_levels(plan):
    def kernel(own, above, below, from_right, from_left, to_down, to_up):
        for index, (a, tile, side) in enumerate(plan.carried):
            for out, k in ((to_down, a), (to_up, LEVELS - 1 - a)):
                if tile:
                    out[index] = TILE_OF[plan]((own, above, below), *tile, k)
                else:
                    out[index] = (from_left if side else from_right)[k]

    return kernel


def place_own(plan, refs, ext):
    own, above, below, from_right, from_left = refs

    def middle(levels, _):
        for k in levels:
            right, left = from_right[k], from_left[k]
            for n, (field, part) in enumerate(plan.tiles):
                ext[n, REACH + k, :, 0:COLS] = TILE_OF[plan]((own, above, below), field, part, k)
                ext[n, REACH + k, :, COLS:WIDE] = halo_columns(right, left, n)
        return 0

    sweep(0, LEVELS, 4, middle)


def place_halo(plan, from_up, from_down, ext, place, last):
    columns = {(a, side): i for i, (a, tile, side) in enumerate(plan.carried) if not tile}
    for message, level, there in (
        (from_down, lambda a: REACH - 1 - a, place > 0),
        (from_up, lambda a: REACH + LEVELS + a, place < last),
    ):
        keep = jnp.where(there, 1.0, 0.0).astype(F32)
        for index, (a, tile, _) in enumerate(plan.carried):
            if not tile:
                continue
            field, part = tile
            value = message[index] * keep
            for kept in "ab" if part == "n" and field in plan.tall else part:
                n = plan.at[field, kept]
                ext[n, level(a), :, 0:COLS] = value
                if (a, 0) in columns:
                    ext[n, level(a), :, COLS:WIDE] = (
                        halo_columns(message[columns[a, 0]], message[columns[a, 1]], n) * keep
                    )


def shift(value, by, axis):
    return pltpu.roll(value, (-by) % value.shape[axis], axis)


def face_flux(q, wind):
    central = 37.0 * (q[2] + q[3]) - 8.0 * (q[1] + q[4]) + (q[0] + q[5])
    upwind = 10.0 * (q[3] - q[2]) - 5.0 * (q[4] - q[1]) + (q[5] - q[0])
    return wind * central - jnp.abs(wind) * upwind


def flat_flux(q, wind, axis):
    flux = face_flux([shift(q, by, axis) if by else q for by in range(-2, 4)], wind)
    return flux - shift(flux, -1, axis)


def rows_flux(q, wind):
    if wind.shape[0] == 24:
        return sixteen(flat_flux(q, wind, 0))
    if q.shape[0] == 24:
        flux = face_flux([sixteen(shift(q, by, 0) if by else q) for by in range(-2, 4)], wind)
        return flux - shift(flux, -1, 0)
    return flat_flux(q, wind, 0)


def level_flux(read, wind, l):
    return face_flux([read(l + by) for by in range(-2, 4)], wind)


def in_domain(l, place, last, lid):
    g = place * LEVELS + l - REACH
    top = (last + 1) * LEVELS - (1 if lid else 0)
    return jnp.where((g >= 0) & (g < top), 1.0, 0.0).astype(F32)


SIXTIETH = -1.0 / 60.0


def sweep(first, count, most, body, carry=0):
    size = max(n for n in range(1, most + 1) if count % n == 0)

    def run(i, carry):
        start = first + i * size
        return body([start + n for n in range(size)], carry)

    return lax.fori_loop(0, count // size, run, carry)


def flat_part(plan, ext, field, l):
    return flat_flux(plan.sixteen(ext, field, l), plan.sixteen(ext, U, l), 1) + rows_flux(
        plan.rows(ext, field, l), plan.rows(ext, V, l)
    )


def flat_own(plan, ext, fields, flat):
    def some(levels, _):
        results = [(n, l, flat_part(plan, ext, f, l)) for l in levels for n, f in enumerate(fields)]
        for n, l, value in results:
            flat[n, l - REACH] = value
        return 0

    sweep(REACH, LEVELS, 2, some)


def rates(plan, ext, fields, write, around_own, most, flat=None):
    reads = [lambda l, f=f: plan.sixteen(ext, f, l) for f in fields]

    def some(levels, lows, flat=None):
        results = []
        for l in levels:
            w = plan.sixteen(ext, W, l)
            highs = []
            for n, f in enumerate(fields):
                high = level_flux(reads[n], w, l)
                level = flat[n, l - REACH] if flat is not None else flat_part(plan, ext, f, l)
                results.append((n, l, (level + (high - lows[n])) * SIXTIETH))
                highs.append(high)
            lows = tuple(highs)
        for result in results:
            write(*result)
        return lows

    first = REACH - around_own
    w = plan.sixteen(ext, W, first - 1)
    lows = tuple(level_flux(read, w, first - 1) for read in reads)
    if flat is None:
        sweep(first, LEVELS + 2 * around_own, most, some, lows)
        return
    lows = sweep(first, around_own, most, some, lows)
    lows = sweep(REACH, LEVELS, 4, lambda levels, c: some(levels, c, flat), lows)
    sweep(REACH + LEVELS, around_own, most, some, lows)


def first_own(place_ref, own, above, below, from_right, from_left, ext, flat):
    place_own(FIRST, (own, above, below, from_right, from_left), ext)

    @pl.when(place_ref[0] == place_ref[1])
    def _():
        for part in "on":
            ext[FIRST.at[W, part], REACH + LEVELS - 1] = jnp.zeros((ROWS, WIDE), F32)

    flat_own(FIRST, ext, (C, PR), flat)


def first_rates(place_ref, ext_in, flat, from_up, from_down, *rest):
    ext, rate = rest[-2:]
    place_halo(FIRST, from_up, from_down, ext, place_ref[0], place_ref[1])

    def write(n, l, value):
        rate[n, l] = value

    rates(FIRST, ext, (C, PR), write, 4, 2, flat)


def acoustic(p, u, v, w, read_c, rate, step, first, count, place, last):
    pull = step * sound_speed

    def level(value):
        return sixteen(value) if value.shape[0] == 24 else value

    def wind_w(l, lift_low, lift_high, p_here, p_above):
        lift = (buoyancy * 0.5) * (lift_low + lift_high)
        return (w[0](l) + step * lift - pull * (p_above - p_here)) * in_domain(l, place, last, True)

    def some(levels, w_low):
        talls = [p[0](l) for l in (*levels, levels[-1] + 1)]
        cells = [level(value) for value in talls]
        warm = [read_c(l) for l in (*levels, levels[-1] + 1)]
        results = []
        for n, l in enumerate(levels):
            p_here = cells[n]
            w_new = wind_w(l, warm[n], warm[n + 1], p_here, cells[n + 1])
            u_new = u[0](l) - pull * (shift(p_here, 1, 1) - p_here)
            v_old = v[0](l)
            if v_old.shape[0] == 24:
                v_tall = v_old - pull * (shift(talls[n], 1, 0) - talls[n])
                v_new, v_flow = sixteen(v_tall), sixteen(v_tall - shift(v_tall, -1, 0))
            else:
                v_new = v_old - pull * (shift(p_here, 1, 0) - p_here)
                v_flow = v_new - shift(v_new, -1, 0)
            divergence = (u_new - shift(u_new, -1, 1)) + v_flow + (w_new - w_low)
            p_new = (p_here + step * rate(l) - pull * divergence) * in_domain(
                l, place, last, False
            )
            results.append((l, p_new, u_new, v_new, w_new))
            w_low = w_new
        for l, *news in results:
            for target, value in zip((p, u, v, w), news):
                target[1](l, value)
        return w_low

    low = first - 1
    w_low = wind_w(low, read_c(low), read_c(first), level(p[0](low)), level(p[0](first)))
    w[1](low, w_low)
    sweep(first, count, 6, some, w_low)


def access(ref, *lead):
    def read(l):
        return ref[(*lead, l)]

    def write(l, value):
        ref[(*lead, l)] = value

    return read, write


def begin(start, field, tall=False):
    return lambda l: (FIRST.rows if tall else FIRST.sixteen)(start, field, l)


def own_write(ref, field):
    def write(l, value):
        if not isinstance(l, int):
            ref[field, l - REACH] = value[0:ROWS, 0:COLS]

    return write


def tracer_flat(tiles, u, v, l):
    rows = flat_flux(tiles(l)[:, 0:COLS], v(l)[:, 0:COLS], 0)[0:ROWS]
    return rows + flat_flux(tiles(l)[0:ROWS], u(l)[0:ROWS], 1)[:, 0:COLS]


def tracer_high(tiles, w, l):
    return level_flux(lambda m: tiles(m)[0:ROWS, 0:COLS], w(l)[0:ROWS, 0:COLS], l)


def two_sections(place_ref, speed, start, rate0, s2, down, up, dt_out, s1, rate1, fast):
    place, last = place_ref[0], place_ref[1]
    dt = courant_goal / (1.0 + jnp.max(speed[...]))
    dt_out[0] = dt
    third = dt * (1.0 / 3.0)

    def tracer(levels, _):
        for l in levels:
            s1[C, l] = (FIRST.sixteen(start, C, l) + third * rate0[0, l]) * in_domain(
                l, place, last, False
            )
        return 0

    sweep(REACH - 4, LEVELS + 8, 4, tracer)
    acoustic(
        (begin(start, PR, True), access(s1, PR)[1]),
        (begin(start, U), access(s1, U)[1]),
        (begin(start, V, True), access(s1, V)[1]),
        (begin(start, W), access(s1, W)[1]),
        begin(start, C),
        access(rate0, 1)[0],
        third,
        REACH - 4,
        LEVELS + 8,
        place,
        last,
    )
    half = dt * 0.5
    tiles = access(s1, C)[0]
    winds = [access(s1, f)[0] for f in (U, V, W)]

    def own_tracer(levels, low):
        results = []
        for l in levels:
            high = tracer_high(tiles, winds[2], l)
            tendency = (tracer_flat(tiles, *winds[:2], l) + (high - low)) * SIXTIETH
            low = high
            results.append(start[FIRST.at[C, "o"], l, :, 0:COLS] + half * tendency)
        for l, value in zip(levels, results):
            s2[C, l - REACH] = value
        return low

    sweep(REACH, LEVELS, 4, own_tracer, tracer_high(tiles, winds[2], REACH - 1))

    def write(n, l, value):
        rate1[l] = value

    rates(SECTION, s1, (PR,), write, 1, 3)
    step = half / (NS // 2)
    acoustic(
        (begin(start, PR), access(fast, 0)[1]),
        (begin(start, U), access(fast, 1)[1]),
        (begin(start, V), access(fast, 2)[1]),
        (begin(start, W), access(fast, 3)[1]),
        access(s1, C)[0],
        access(rate1)[0],
        step,
        REACH - 1,
        LEVELS + 2,
        place,
        last,
    )
    acoustic(
        (access(fast, 0)[0], own_write(s2, PR)),
        (access(fast, 1)[0], own_write(s2, U)),
        (access(fast, 2)[0], own_write(s2, V)),
        (access(fast, 3)[0], own_write(s2, W)),
        access(s1, C)[0],
        access(rate1)[0],
        step,
        REACH,
        LEVELS,
        place,
        last,
    )

    def share(levels, _):
        made = [shared_rows(lambda f, k=k: s2[f, k]) for k in levels]
        for k, (to_down, to_up) in zip(levels, made):
            for n in range(3):
                down[n, k] = to_down[n]
                up[n, k] = to_up[n]
        return 0

    sweep(0, LEVELS, 4, share)


class Whole:
    def rows(self, ref, field, l):
        return ref[field, l]

    sixteen = rows


SECTION = Whole()


def second_own(own, above, below, from_right, from_left, ext, flat, tracer):
    place_own(SECOND, (own, above, below, from_right, from_left), ext)
    flat_own(SECOND, ext, (PR,), flat)
    tiles, u, v = (lambda l, f=f: SECOND.rows(ext, f, l) for f in (C, U, V))

    def some(levels, _):
        results = [tracer_flat(tiles, u, v, l) for l in levels]
        for l, value in zip(levels, results):
            tracer[l - REACH] = value
        return 0

    sweep(REACH, LEVELS, 4, some)


def last_tracer(
    place_ref, dt_ref, ext_in, flat, flat_tracer, from_up, from_down, initial, *rest
):
    *chunks, ext, tracer, landed, fallen, rate, warm, factor, by_depth, sem = rest
    dt = dt_ref[0]
    each = LEVELS // len(chunks)
    copies = [
        pltpu.make_async_copy(chunk, by_depth.at[pl.ds(n * each, each)], sem.at[n])
        for n, chunk in enumerate(chunks)
    ]
    for copy in copies:
        copy.start()
    place_halo(SECOND, from_up, from_down, ext, place_ref[0], place_ref[1])

    def write(n, l, value):
        rate[l] = value

    rates(SECOND, ext, (PR,), write, 3, 3, flat)

    def keep(levels, _):
        for l in levels:
            warm[l] = SECOND.rows(ext, C, l)
        return 0

    sweep(REACH - 4, LEVELS + 8, 4, keep)
    tiles = lambda l: SECOND.rows(ext, C, l)
    w = lambda l: SECOND.rows(ext, W, l)

    def some(levels, low):
        results = []
        for l in levels:
            high = tracer_high(tiles, w, l)
            tendency = (flat_tracer[l - REACH] + (high - low)) * SIXTIETH
            low = high
            c = initial[C, l - REACH] + dt * tendency
            grown = jnp.exp(growth * c)
            results.append((c, grown, grown * jnp.exp((0.5 * growth) * c)))
        for l, (c, second, third) in zip(levels, results):
            tracer[l - REACH] = c
            factor[0, l - REACH] = second
            factor[1, l - REACH] = third
        return low

    sweep(REACH, LEVELS, 4, some, tracer_high(tiles, w, REACH - 1))
    for copy in copies:
        copy.wait()
    for target in range(-FMAX, LEVELS):
        for moment in range(3):
            total = None
            for depth in range(FMAX + 1):
                k = target + depth
                if 0 <= k < LEVELS:
                    value = by_depth[k, depth, moment]
                    if moment:
                        value = value * factor[moment - 1, k]
                    total = value if total is None else total + value
            if target < 0:
                fallen[moment, target + FMAX] = total
            else:
                landed[moment, target] = total


def last_section(place_ref, dt_ref, rate, warm, start, tracer, out, fast):
    place, last = place_ref[0], place_ref[1]
    step = dt_ref[0] / NS
    out[C] = tracer[...]
    names = (PR, U, V, W)
    for repeat in range(NS):
        reads = [
            begin(start, f) if repeat == 0 else access(fast, n)[0] for n, f in enumerate(names)
        ]
        writes = [
            own_write(out, f) if repeat == NS - 1 else access(fast, n)[1]
            for n, f in enumerate(names)
        ]
        acoustic(
            *zip(reads, writes),
            access(warm)[0],
            access(rate)[0],
            step,
            REACH - 3 + repeat,
            LEVELS + 6 - 2 * repeat,
            place,
            last,
        )


def land(place_ref, landed, arrived, out):
    keep = jnp.where(place_ref[0] < place_ref[1], 1.0, 0.0).astype(F32)
    out[:, 0 : LEVELS - FMAX] = landed[:, 0 : LEVELS - FMAX]
    out[:, LEVELS - FMAX :] = landed[:, LEVELS - FMAX :] + keep * arrived[...]


def deposit(radius, weight, column, counts, fall_depth, out):
    slots, levels = radius.shape[0], radius.shape[1]
    target = lax.broadcasted_iota(jnp.int32, (COLS, COLS), 0)
    row = lax.broadcasted_iota(jnp.int32, (ROWS, COLS), 0)
    per_step = 4

    for k in range(levels):
        out[k] = jnp.zeros(out.shape[1:], F32)
        live = counts[k]

        def some(step, _, k=k, live=live):
            sums = [[None] * 3 for _ in range(FMAX + 1)]
            for part in range(per_step):
                s = step * per_step + part
                r = radius[s, k]
                number = jnp.where(s < live, weight[s, k], 0.0)
                area = number * r * r
                terms = []
                for t in (number, area, area * r):
                    high = t.astype(jnp.bfloat16).astype(F32)
                    terms += [high, t - high]
                cols = column[s, k]
                left, right = [], []
                for j in range(ROWS):
                    left.append(
                        jnp.concatenate([jnp.where(row == j, t, 0.0) for t in terms], axis=0)
                    )
                    right.append(jnp.where(cols[j : j + 1] == target, 1.0, 0.0).astype(F32))
                sent = lax.dot_general(
                    jnp.concatenate(left, axis=1),
                    jnp.concatenate(right, axis=1),
                    (((1,), (1,)), ((), ())),
                    preferred_element_type=F32,
                )
                depth = jnp.broadcast_to(fall_depth[s, k], (ROWS, COLS))
                for d in range(FMAX + 1):
                    falls = depth == d
                    for m in range(3):
                        both = sent[16 * m : 16 * m + 8] + sent[16 * m + 8 : 16 * m + 16]
                        value = jnp.where(falls, both, 0.0)
                        sums[d][m] = value if sums[d][m] is None else sums[d][m] + value
            for d in range(FMAX + 1):
                for m in range(3):
                    out[k, d, m] += sums[d][m]
            return 0

        lax.fori_loop(0, slots // per_step, some, 0)


def vmem(n):
    return [pl.BlockSpec(memory_space=pltpu.VMEM)] * n


def smem(n):
    return [pl.BlockSpec(memory_space=pltpu.SMEM)] * n


def anywhere(n):
    return [pl.BlockSpec(memory_space=pl.ANY)] * n


def shaped(*dims):
    return jax.ShapeDtypeStruct(dims, F32)


def held(*dims):
    return pltpu.VMEM(dims, F32)


def call(kernel, name, ins, outs, scratch=(), out_specs=None, flops=None, grant=4, alias=None):
    made = pl.pallas_call(
        kernel,
        name=name,
        in_specs=ins,
        out_specs=tuple(out_specs or vmem(len(outs))),
        out_shape=tuple(outs),
        scratch_shapes=list(scratch),
        input_output_aliases=alias or {},
        compiler_params=pltpu.CompilerParams(vmem_limit_bytes=grant << 20),
        cost_estimate=(
            pl.CostEstimate(flops=flops, bytes_accessed=0, transcendentals=0) if flops else None
        ),
    )

    def run(*operands):
        return made(
            *(
                pltpu.with_memory_space_constraint(value, pltpu.VMEM)
                if spec.memory_space == pltpu.VMEM
                else value
                for spec, value in zip(ins, operands)
            )
        )

    return run


def both_ways(down, axis, up):
    count = lax.axis_size(axis)
    return (
        lax.ppermute(down, axis, [((i + 1) % count, i) for i in range(count)]),
        lax.ppermute(up, axis, [(i, (i + 1) % count) for i in range(count)]),
    )


def exchange(plan, own, down, up, tokens=()):
    above, below = both_ways(down, "gy", up)
    to_left, to_right = call(
        pack_columns(plan),
        "pack_columns",
        vmem(3) + anywhere(len(tokens)),
        [held(LEVELS, ROWS, COLS)] * 2,
    )(own, above, below, *tokens)
    from_right, from_left = both_ways(to_left, "gx", to_right)
    tiles = len(plan.carried)
    to_down, to_up = call(
        pack_levels(plan), "pack_levels", vmem(5), [held(tiles, ROWS, COLS)] * 2
    )(own, above, below, from_right, from_left)
    from_up, from_down = both_ways(to_down, "gz", to_up)
    return above, below, from_right, from_left, from_up, from_down, to_down


def prepare(place_ref, fields, own, speed):
    own[...] = fields[...]
    keep = jnp.where(place_ref[0] == place_ref[1], 0.0, 1.0).astype(F32)
    most = jnp.zeros((ROWS, COLS), F32)
    for k in range(LEVELS):
        w = jnp.abs(fields[W, k])
        if k == LEVELS - 1:
            w = w * keep
        most = jnp.maximum(most, jnp.abs(fields[U, k]) + jnp.abs(fields[V, k]) + w)
    speed[...] = jnp.broadcast_to(jnp.max(most), speed.shape)


def droplets(radius, weight, column, counts, fall_depth, chunk, numbers, after=None):
    slots = radius.shape[0]
    if after is not None:
        counts, _ = lax.optimization_barrier((counts, after))
    made = []
    for n in numbers:
        whole = pl.BlockSpec((slots, chunk, ROWS, COLS), lambda i, n=n: (0, n, 0, 0))
        made.append(
            pl.pallas_call(
                deposit,
                name="deposit",
                grid=(1,),
                in_specs=[
                    whole,
                    whole,
                    whole,
                    pl.BlockSpec((chunk, ROWS, COLS), lambda i, n=n: (n, 0, 0)),
                    pl.BlockSpec((slots, chunk, ROWS, 1), lambda i, n=n: (0, n, 0, 0)),
                ],
                out_specs=pl.BlockSpec(
                    (chunk, FMAX + 1, 3, ROWS, COLS), lambda i: (0, 0, 0, 0, 0)
                ),
                out_shape=shaped(chunk, FMAX + 1, 3, ROWS, COLS),
                compiler_params=pltpu.CompilerParams(vmem_limit_bytes=12 << 20),
                cost_estimate=pl.CostEstimate(
                    flops=200_000_000, bytes_accessed=0, transcendentals=0
                ),
            )(radius, weight, column, counts, fall_depth)
        )
    return made


def per_device(fields, radius, weight, column, counts, fall_depth):
    place = lax.axis_index("gz")
    last = lax.axis_size("gz") - 1
    where = jnp.stack([place, jnp.int32(last)]).astype(jnp.int32)
    def drops(numbers, after=None):
        return droplets(radius, weight, column, counts, fall_depth, 2, numbers, after)

    devices = lax.axis_size(GRID_AXES)
    own, speed = pl.pallas_call(
        prepare,
        name="prepare",
        in_specs=smem(1) + vmem(1),
        out_specs=tuple(vmem(2)),
        out_shape=(held(5, LEVELS, ROWS, COLS), shaped(devices, 1, COLS)),
        compiler_params=pltpu.CompilerParams(vmem_limit_bytes=4 << 20),
    )(where, fields)
    early = drops(range(0, 2), speed)
    speed = lax.all_to_all(speed, GRID_AXES, 0, 0)
    *near, from_up, from_down, sent = exchange(FIRST, own, fields, fields, [speed, *early])
    by_depth = drops(range(2, 3), sent)
    ext = held(len(FIRST.tiles), DEPTH, ROWS, WIDE)
    start, flat = call(
        first_own,
        "first_own",
        smem(1) + vmem(5),
        [ext, held(2, LEVELS, 2 * ROWS, WIDE)],
    )(where, own, *near)
    start, rate0 = call(
        first_rates,
        "first_rates",
        smem(1) + vmem(4) + anywhere(len(by_depth)),
        [ext, held(2, DEPTH, 2 * ROWS, WIDE)],
        alias={1: 0},
    )(where, start, flat, from_up, from_down, *by_depth)
    s2, down, up, dt = call(
        two_sections,
        "two_sections",
        smem(1) + vmem(3),
        [held(5, LEVELS, ROWS, COLS)] + [held(3, LEVELS, ROWS, COLS)] * 2 + [shaped(1)],
        scratch=[
            pltpu.VMEM((5, DEPTH, 2 * ROWS, WIDE), F32),
            pltpu.VMEM((DEPTH, 2 * ROWS, WIDE), F32),
            pltpu.VMEM((4, DEPTH, 2 * ROWS, WIDE), F32),
        ],
        out_specs=vmem(3) + smem(1),
        grant=10,
    )(where, speed, start, rate0)
    middle = drops(range(3, 7), s2)
    *near, from_up, from_down, sent = exchange(SECOND, s2, down, up, middle)
    by_depth = early + by_depth + middle + drops(range(7, 8), sent)
    ext = held(len(SECOND.tiles), DEPTH, ROWS, WIDE)
    around_s2, flat, flat_tracer = call(
        second_own,
        "second_own",
        vmem(5),
        [ext, held(1, LEVELS, 2 * ROWS, WIDE), held(LEVELS, ROWS, COLS)],
        flops=1_000_000_000,
    )(s2, *near)
    rows = held(DEPTH, 2 * ROWS, WIDE)
    _, tracer, landed, fallen, rate, warm = call(
        last_tracer,
        "last_tracer",
        smem(2) + vmem(6) + anywhere(len(by_depth)),
        [
            ext,
            held(LEVELS, ROWS, COLS),
            held(3, LEVELS, ROWS, COLS),
            held(3, FMAX, ROWS, COLS),
            rows,
            rows,
        ],
        scratch=[
            pltpu.VMEM((2, LEVELS, ROWS, COLS), F32),
            pltpu.VMEM((LEVELS, FMAX + 1, 3, ROWS, COLS), F32),
            pltpu.SemaphoreType.DMA((len(by_depth),)),
        ],
        alias={2: 0},
    )(where, dt, around_s2, flat, flat_tracer, from_up, from_down, own, *by_depth)
    count = lax.axis_size("gz")
    arrived = lax.ppermute(fallen, "gz", [((i + 1) % count, i) for i in range(count)])
    (new_fields,) = call(
        last_section,
        "last_section",
        smem(2) + vmem(4),
        [shaped(5, LEVELS, ROWS, COLS)],
        scratch=[pltpu.VMEM((4, DEPTH, 2 * ROWS, WIDE), F32)],
        flops=1_000_000_000,
    )(where, dt, rate, warm, start, tracer)
    (moments,) = call(
        land, "land", smem(1) + vmem(2), [shaped(3, LEVELS, ROWS, COLS)]
    )(where, landed, arrived)
    return (new_fields, moments)


def solution(mesh):
    spread = P(None, "gz", "gy", "gx")
    return jax.shard_map(
        per_device,
        mesh=mesh,
        in_specs=(spread, spread, spread, spread, P("gz", "gy", "gx"), spread),
        out_specs=(spread, spread),
        check_vma=False,
    )
```

```python
import jax
import jax.numpy as jnp
from jax import lax
from jax.experimental import pallas as pl
from jax.experimental.pallas import tpu as pltpu
from jax.sharding import PartitionSpec as P

NS = 4
FMAX = 8
GRID_AXES = ("gx", "gy", "gz")

sound_speed = 10.0
buoyancy = 0.5
courant_goal = 0.6
growth = 0.3

LEVELS, ROWS, COLS = 16, 8, 128
WIDE = 2 * COLS
REACH = 7
DEPTH = LEVELS + 2 * REACH
EDGE = 8
F32 = jnp.float32
C, PR, U, V, W = range(5)


class Plan:
    def __init__(self, tall, reach, sent):
        self.tall, self.reach = tall, reach
        self.tiles = [
            (field, part)
            for field in range(5)
            for part in ("oab" if field in tall else "on")
        ]
        self.at = {tile: n for n, tile in enumerate(self.tiles)}
        self.carried = []
        for a in range(reach):
            for field in range(5):
                for part in sent[field][a] if a < len(sent[field]) else "":
                    self.carried.append((a, (field, part), 0))
            if a < reach - 1:
                self.carried += [(a, None, 0), (a, None, 1)]

    def rows(self, ref, field, l):
        return jnp.concatenate(
            [
                ref[self.at[field, part], l]
                for part in ("oab" if field in self.tall else "on")
            ],
            axis=0,
        )

    def sixteen(self, ref, field, l):
        value = self.rows(ref, field, l)
        return sixteen(value) if field in self.tall else value


def lanes(shape):
    return lax.broadcasted_iota(jnp.int32, shape, len(shape) - 1)


def lower_rows(shape):
    return lax.broadcasted_iota(jnp.int32, shape, 0) < ROWS // 2


def around(above, below):
    return jnp.where(lower_rows(above.shape), above, below)


def sixteen(value):
    return jnp.concatenate(
        [value[0:ROWS], around(value[ROWS : 2 * ROWS], value[2 * ROWS :])], axis=0
    )


def raw_tile(refs, field, part, k):
    own, above, below = refs
    if part == "o":
        return own[field, k]
    if part == "n":
        return around(above[field, k], below[field, k])
    return (above if part == "a" else below)[field, k]


SHARED = {C: (1, 0), U: (1, 1), V: (2, 0), W: (2, 1)}


def shared_rows(read):
    down, up = [read(PR)], [read(PR)]
    for first, second in ((C, U), (V, W)):
        one, other = read(first), pltpu.roll(read(second), ROWS // 2, 0)
        down.append(around(one, other))
        up.append(around(other, one))
    return down, up


def shared_tile(refs, field, part, k):
    own, above, below = refs
    if part == "o":
        return own[field, k]
    if part == "n" and field == PR:
        return around(above[0, k], below[0, k])
    if part == "n":
        index, half = SHARED[field]
        if half == 0:
            return around(above[index, k], below[index, k])
        return pltpu.roll(around(below[index, k], above[index, k]), ROWS // 2, 0)
    return (above if part == "a" else below)[0, k]


THREE, TWO, ONE = "oab", "on", "o"
FIRST = Plan(
    (C, PR, V),
    7,
    {
        C: [THREE] + [TWO] * 4 + [ONE],
        PR: [THREE] * 2 + [TWO] * 4 + [ONE],
        U: [TWO] * 4,
        V: [TWO] * 4,
        W: [TWO] * 4 + [ONE],
    },
)
SECOND = Plan(
    (PR,),
    6,
    {
        C: [TWO] * 3 + [ONE],
        PR: [THREE] + [TWO] * 4 + [ONE],
        U: [TWO] * 3,
        V: [TWO] * 3,
        W: [TWO] * 3 + [ONE],
    },
)
TILE_OF = {FIRST: raw_tile, SECOND: shared_tile}


SPARE = 104


def pack_columns(plan, with_speed):
    def kernel(own, above, below, *rest):
        to_left, to_right = rest[-2:]
        lane = lanes((ROWS, COLS))
        filler = jnp.zeros((ROWS, COLS), F32)
        if with_speed:
            filler = filler + jnp.max(rest[0][...])

        def one(k, _):
            left = filler
            right = filler
            for n, (field, part) in enumerate(plan.tiles):
                start = n * EDGE
                here = (lane >= start) & (lane < start + EDGE)
                value = TILE_OF[plan]((own, above, below), field, part, k)
                first = pltpu.roll(value, start, 1) if start else value
                last = pltpu.roll(value, (start + EDGE) % COLS, 1)
                left = jnp.where(here, first, left)
                right = jnp.where(here, last, right)
            to_left[k] = left
            to_right[k] = right
            return 0

        def pair(i, _):
            one(2 * i, 0)
            return one(2 * i + 1, 0)

        lax.fori_loop(0, LEVELS // 2, pair, 0)

    return kernel


def halo_columns(from_right, from_left, n):
    start = n * EDGE
    right = pltpu.roll(from_right, COLS - start, 1) if start else from_right
    left = pltpu.roll(from_left, (COLS - EDGE - start) % COLS, 1)
    return jnp.where(lanes((ROWS, COLS)) < COLS // 2, right, left)


def pack_levels(plan, with_speed):
    def kernel(own, above, below, from_right, from_left, *rest):
        if with_speed:
            speed, to_down, to_up, speeds = rest
            near = jnp.maximum(from_right[0], from_left[0])
            near = jnp.where(lanes((ROWS, COLS)) < SPARE, 0.0, near)
            top = jnp.maximum(jnp.max(near), jnp.max(speed[...]))
            speeds[...] = jnp.broadcast_to(top, speeds.shape)
        else:
            to_down, to_up = rest
        for index, (a, tile, side) in enumerate(plan.carried):
            for out, k in ((to_down, a), (to_up, LEVELS - 1 - a)):
                if tile:
                    out[index] = TILE_OF[plan]((own, above, below), *tile, k)
                else:
                    out[index] = (from_left if side else from_right)[k]

    return kernel


def place_own(plan, refs, ext):
    own, above, below, from_right, from_left = refs

    def middle(levels, _):
        for k in levels:
            right, left = from_right[k], from_left[k]
            for n, (field, part) in enumerate(plan.tiles):
                ext[n, REACH + k, :, 0:COLS] = TILE_OF[plan]((own, above, below), field, part, k)
                ext[n, REACH + k, :, COLS:WIDE] = halo_columns(right, left, n)
        return 0

    sweep(0, LEVELS, 4, middle)


def place_halo(plan, from_up, from_down, ext, place, last):
    columns = {(a, side): i for i, (a, tile, side) in enumerate(plan.carried) if not tile}
    for message, level, there in (
        (from_down, lambda a: REACH - 1 - a, place > 0),
        (from_up, lambda a: REACH + LEVELS + a, place < last),
    ):
        keep = jnp.where(there, 1.0, 0.0).astype(F32)
        for index, (a, tile, _) in enumerate(plan.carried):
            if not tile:
                continue
            field, part = tile
            value = message[index] * keep
            for kept in "ab" if part == "n" and field in plan.tall else part:
                n = plan.at[field, kept]
                ext[n, level(a), :, 0:COLS] = value
                if (a, 0) in columns:
                    ext[n, level(a), :, COLS:WIDE] = (
                        halo_columns(message[columns[a, 0]], message[columns[a, 1]], n) * keep
                    )


def shift(value, by, axis):
    return pltpu.roll(value, (-by) % value.shape[axis], axis)


def face_flux(q, wind):
    central = 37.0 * (q[2] + q[3]) - 8.0 * (q[1] + q[4]) + (q[0] + q[5])
    upwind = 10.0 * (q[3] - q[2]) - 5.0 * (q[4] - q[1]) + (q[5] - q[0])
    return wind * central - jnp.abs(wind) * upwind


def flat_flux(q, wind, axis):
    flux = face_flux([shift(q, by, axis) if by else q for by in range(-2, 4)], wind)
    return flux - shift(flux, -1, axis)


def rows_flux(q, wind):
    if wind.shape[0] == 24:
        return sixteen(flat_flux(q, wind, 0))
    if q.shape[0] == 24:
        flux = face_flux([sixteen(shift(q, by, 0) if by else q) for by in range(-2, 4)], wind)
        return flux - shift(flux, -1, 0)
    return flat_flux(q, wind, 0)


def level_flux(read, wind, l):
    return face_flux([read(l + by) for by in range(-2, 4)], wind)


def in_domain(l, place, last, lid):
    g = place * LEVELS + l - REACH
    top = (last + 1) * LEVELS - (1 if lid else 0)
    return jnp.where((g >= 0) & (g < top), 1.0, 0.0).astype(F32)


SIXTIETH = -1.0 / 60.0


def sweep(first, count, most, body, carry=0):
    size = max(n for n in range(1, most + 1) if count % n == 0)

    def run(i, carry):
        start = first + i * size
        return body([start + n for n in range(size)], carry)

    return lax.fori_loop(0, count // size, run, carry)


def flat_part(plan, ext, field, l):
    return flat_flux(plan.sixteen(ext, field, l), plan.sixteen(ext, U, l), 1) + rows_flux(
        plan.rows(ext, field, l), plan.rows(ext, V, l)
    )


def flat_own(plan, ext, fields, flat):
    def some(levels, _):
        results = [(n, l, flat_part(plan, ext, f, l)) for l in levels for n, f in enumerate(fields)]
        for n, l, value in results:
            flat[n, l - REACH] = value
        return 0

    sweep(REACH, LEVELS, 2, some)


def rates(plan, ext, fields, write, around_own, most, flat=None):
    reads = [lambda l, f=f: plan.sixteen(ext, f, l) for f in fields]

    def some(levels, lows, flat=None):
        results = []
        for l in levels:
            w = plan.sixteen(ext, W, l)
            highs = []
            for n, f in enumerate(fields):
                high = level_flux(reads[n], w, l)
                level = flat[n, l - REACH] if flat is not None else flat_part(plan, ext, f, l)
                results.append((n, l, (level + (high - lows[n])) * SIXTIETH))
                highs.append(high)
            lows = tuple(highs)
        for result in results:
            write(*result)
        return lows

    first = REACH - around_own
    w = plan.sixteen(ext, W, first - 1)
    lows = tuple(level_flux(read, w, first - 1) for read in reads)
    if flat is None:
        sweep(first, LEVELS + 2 * around_own, most, some, lows)
        return
    lows = sweep(first, around_own, most, some, lows)
    lows = sweep(REACH, LEVELS, 4, lambda levels, c: some(levels, c, flat), lows)
    sweep(REACH + LEVELS, around_own, most, some, lows)


def first_own(place_ref, own, above, below, from_right, from_left, *rest):
    ext, flat = rest[-2:]
    place_own(FIRST, (own, above, below, from_right, from_left), ext)

    @pl.when(place_ref[0] == place_ref[1])
    def _():
        for part in "on":
            ext[FIRST.at[W, part], REACH + LEVELS - 1] = jnp.zeros((ROWS, WIDE), F32)

    flat_own(FIRST, ext, (C, PR), flat)


def first_rates(place_ref, ext_in, flat, from_up, from_down, ext, rate):
    place_halo(FIRST, from_up, from_down, ext, place_ref[0], place_ref[1])

    def write(n, l, value):
        rate[n, l] = value

    rates(FIRST, ext, (C, PR), write, 4, 2, flat)


def acoustic(p, u, v, w, read_c, rate, step, first, count, place, last):
    pull = step * sound_speed

    def level(value):
        return sixteen(value) if value.shape[0] == 24 else value

    def wind_w(l, lift_low, lift_high, p_here, p_above):
        lift = (buoyancy * 0.5) * (lift_low + lift_high)
        return (w[0](l) + step * lift - pull * (p_above - p_here)) * in_domain(l, place, last, True)

    def some(levels, w_low):
        talls = [p[0](l) for l in (*levels, levels[-1] + 1)]
        cells = [level(value) for value in talls]
        warm = [read_c(l) for l in (*levels, levels[-1] + 1)]
        results = []
        for n, l in enumerate(levels):
            p_here = cells[n]
            w_new = wind_w(l, warm[n], warm[n + 1], p_here, cells[n + 1])
            u_new = u[0](l) - pull * (shift(p_here, 1, 1) - p_here)
            v_old = v[0](l)
            if v_old.shape[0] == 24:
                v_tall = v_old - pull * (shift(talls[n], 1, 0) - talls[n])
                v_new, v_flow = sixteen(v_tall), sixteen(v_tall - shift(v_tall, -1, 0))
            else:
                v_new = v_old - pull * (shift(p_here, 1, 0) - p_here)
                v_flow = v_new - shift(v_new, -1, 0)
            divergence = (u_new - shift(u_new, -1, 1)) + v_flow + (w_new - w_low)
            p_new = (p_here + step * rate(l) - pull * divergence) * in_domain(
                l, place, last, False
            )
            results.append((l, p_new, u_new, v_new, w_new))
            w_low = w_new
        for l, *news in results:
            for target, value in zip((p, u, v, w), news):
                target[1](l, value)
        return w_low

    low = first - 1
    w_low = wind_w(low, read_c(low), read_c(first), level(p[0](low)), level(p[0](first)))
    w[1](low, w_low)
    sweep(first, count, 6, some, w_low)


def access(ref, *lead):
    def read(l):
        return ref[(*lead, l)]

    def write(l, value):
        ref[(*lead, l)] = value

    return read, write


def begin(start, field, tall=False):
    return lambda l: (FIRST.rows if tall else FIRST.sixteen)(start, field, l)


def own_write(ref, field):
    def write(l, value):
        if not isinstance(l, int):
            ref[field, l - REACH] = value[0:ROWS, 0:COLS]

    return write


def tracer_flat(tiles, u, v, l):
    rows = flat_flux(tiles(l)[:, 0:COLS], v(l)[:, 0:COLS], 0)[0:ROWS]
    return rows + flat_flux(tiles(l)[0:ROWS], u(l)[0:ROWS], 1)[:, 0:COLS]


def tracer_high(tiles, w, l):
    return level_flux(lambda m: tiles(m)[0:ROWS, 0:COLS], w(l)[0:ROWS, 0:COLS], l)


def two_sections(place_ref, speed, start, rate0, s2, down, up, dt_out, s1, rate1, fast):
    place, last = place_ref[0], place_ref[1]
    dt = courant_goal / (1.0 + jnp.max(speed[...]))
    dt_out[0] = dt
    third = dt * (1.0 / 3.0)

    def tracer(levels, _):
        for l in levels:
            s1[C, l] = (FIRST.sixteen(start, C, l) + third * rate0[0, l]) * in_domain(
                l, place, last, False
            )
        return 0

    sweep(REACH - 4, LEVELS + 8, 4, tracer)
    acoustic(
        (begin(start, PR, True), access(s1, PR)[1]),
        (begin(start, U), access(s1, U)[1]),
        (begin(start, V, True), access(s1, V)[1]),
        (begin(start, W), access(s1, W)[1]),
        begin(start, C),
        access(rate0, 1)[0],
        third,
        REACH - 4,
        LEVELS + 8,
        place,
        last,
    )
    half = dt * 0.5
    tiles = access(s1, C)[0]
    winds = [access(s1, f)[0] for f in (U, V, W)]

    def own_tracer(levels, low):
        results = []
        for l in levels:
            high = tracer_high(tiles, winds[2], l)
            tendency = (tracer_flat(tiles, *winds[:2], l) + (high - low)) * SIXTIETH
            low = high
            results.append(start[FIRST.at[C, "o"], l, :, 0:COLS] + half * tendency)
        for l, value in zip(levels, results):
            s2[C, l - REACH] = value
        return low

    sweep(REACH, LEVELS, 4, own_tracer, tracer_high(tiles, winds[2], REACH - 1))

    def write(n, l, value):
        rate1[l] = value

    rates(SECTION, s1, (PR,), write, 1, 3)
    step = half / (NS // 2)
    acoustic(
        (begin(start, PR), access(fast, 0)[1]),
        (begin(start, U), access(fast, 1)[1]),
        (begin(start, V), access(fast, 2)[1]),
        (begin(start, W), access(fast, 3)[1]),
        access(s1, C)[0],
        access(rate1)[0],
        step,
        REACH - 1,
        LEVELS + 2,
        place,
        last,
    )
    acoustic(
        (access(fast, 0)[0], own_write(s2, PR)),
        (access(fast, 1)[0], own_write(s2, U)),
        (access(fast, 2)[0], own_write(s2, V)),
        (access(fast, 3)[0], own_write(s2, W)),
        access(s1, C)[0],
        access(rate1)[0],
        step,
        REACH,
        LEVELS,
        place,
        last,
    )

    def share(levels, _):
        made = [shared_rows(lambda f, k=k: s2[f, k]) for k in levels]
        for k, (to_down, to_up) in zip(levels, made):
            for n in range(3):
                down[n, k] = to_down[n]
                up[n, k] = to_up[n]
        return 0

    sweep(0, LEVELS, 4, share)


class Whole:
    def rows(self, ref, field, l):
        return ref[field, l]

    sixteen = rows


SECTION = Whole()


def second_own(own, above, below, from_right, from_left, ext, flat, tracer):
    place_own(SECOND, (own, above, below, from_right, from_left), ext)
    flat_own(SECOND, ext, (PR,), flat)
    tiles, u, v = (lambda l, f=f: SECOND.rows(ext, f, l) for f in (C, U, V))

    def some(levels, _):
        results = [tracer_flat(tiles, u, v, l) for l in levels]
        for l, value in zip(levels, results):
            tracer[l - REACH] = value
        return 0

    sweep(REACH, LEVELS, 4, some)


def last_tracer(
    place_ref, dt_ref, ext_in, flat, flat_tracer, from_up, from_down, initial, *rest
):
    *chunks, ext, tracer, landed, fallen, rate, warm, factor, by_depth, sem = rest
    dt = dt_ref[0]
    each = LEVELS // len(chunks)
    copies = [
        pltpu.make_async_copy(chunk, by_depth.at[pl.ds(n * each, each)], sem.at[n])
        for n, chunk in enumerate(chunks)
    ]
    for copy in copies:
        copy.start()
    place_halo(SECOND, from_up, from_down, ext, place_ref[0], place_ref[1])

    def write(n, l, value):
        rate[l] = value

    rates(SECOND, ext, (PR,), write, 3, 3, flat)

    def keep(levels, _):
        for l in levels:
            warm[l] = SECOND.rows(ext, C, l)
        return 0

    sweep(REACH - 4, LEVELS + 8, 4, keep)
    tiles = lambda l: SECOND.rows(ext, C, l)
    w = lambda l: SECOND.rows(ext, W, l)

    def some(levels, low):
        results = []
        for l in levels:
            high = tracer_high(tiles, w, l)
            tendency = (flat_tracer[l - REACH] + (high - low)) * SIXTIETH
            low = high
            c = initial[C, l - REACH] + dt * tendency
            grown = jnp.exp(growth * c)
            results.append((c, grown, grown * jnp.exp((0.5 * growth) * c)))
        for l, (c, second, third) in zip(levels, results):
            tracer[l - REACH] = c
            factor[0, l - REACH] = second
            factor[1, l - REACH] = third
        return low

    sweep(REACH, LEVELS, 4, some, tracer_high(tiles, w, REACH - 1))
    for copy in copies:
        copy.wait()
    for target in range(-FMAX, LEVELS):
        for moment in range(3):
            total = None
            for depth in range(FMAX + 1):
                k = target + depth
                if 0 <= k < LEVELS:
                    value = by_depth[k, depth, moment]
                    if moment:
                        value = value * factor[moment - 1, k]
                    total = value if total is None else total + value
            if target < 0:
                fallen[moment, target + FMAX] = total
            else:
                landed[moment, target] = total


def last_section(place_ref, dt_ref, rate, warm, start, tracer, out, fast):
    place, last = place_ref[0], place_ref[1]
    step = dt_ref[0] / NS
    out[C] = tracer[...]
    names = (PR, U, V, W)
    for repeat in range(NS):
        reads = [
            begin(start, f) if repeat == 0 else access(fast, n)[0] for n, f in enumerate(names)
        ]
        writes = [
            own_write(out, f) if repeat == NS - 1 else access(fast, n)[1]
            for n, f in enumerate(names)
        ]
        acoustic(
            *zip(reads, writes),
            access(warm)[0],
            access(rate)[0],
            step,
            REACH - 3 + repeat,
            LEVELS + 6 - 2 * repeat,
            place,
            last,
        )


def land(place_ref, landed, arrived, out):
    keep = jnp.where(place_ref[0] < place_ref[1], 1.0, 0.0).astype(F32)
    out[:, 0 : LEVELS - FMAX] = landed[:, 0 : LEVELS - FMAX]
    out[:, LEVELS - FMAX :] = landed[:, LEVELS - FMAX :] + keep * arrived[...]


def deposit(radius, weight, column, counts, fall_depth, out):
    slots, levels = radius.shape[0], radius.shape[1]
    target = lax.broadcasted_iota(jnp.int32, (COLS, COLS), 0)
    row = lax.broadcasted_iota(jnp.int32, (ROWS, COLS), 0)
    per_step = 4

    for k in range(levels):
        out[k] = jnp.zeros(out.shape[1:], F32)
        live = counts[k]

        def some(step, _, k=k, live=live):
            sums = [[None] * 3 for _ in range(FMAX + 1)]
            for part in range(per_step):
                s = step * per_step + part
                r = radius[s, k]
                number = jnp.where(s < live, weight[s, k], 0.0)
                area = number * r * r
                terms = []
                for t in (number, area, area * r):
                    high = t.astype(jnp.bfloat16).astype(F32)
                    terms += [high, t - high]
                cols = column[s, k]
                left, right = [], []
                for j in range(ROWS):
                    left.append(
                        jnp.concatenate([jnp.where(row == j, t, 0.0) for t in terms], axis=0)
                    )
                    right.append(jnp.where(cols[j : j + 1] == target, 1.0, 0.0).astype(F32))
                sent = lax.dot_general(
                    jnp.concatenate(left, axis=1),
                    jnp.concatenate(right, axis=1),
                    (((1,), (1,)), ((), ())),
                    preferred_element_type=F32,
                )
                depth = jnp.broadcast_to(fall_depth[s, k], (ROWS, COLS))
                for d in range(FMAX + 1):
                    falls = depth == d
                    for m in range(3):
                        both = sent[16 * m : 16 * m + 8] + sent[16 * m + 8 : 16 * m + 16]
                        value = jnp.where(falls, both, 0.0)
                        sums[d][m] = value if sums[d][m] is None else sums[d][m] + value
            for d in range(FMAX + 1):
                for m in range(3):
                    out[k, d, m] += sums[d][m]
            return 0

        lax.fori_loop(0, slots // per_step, some, 0)


def vmem(n):
    return [pl.BlockSpec(memory_space=pltpu.VMEM)] * n


def smem(n):
    return [pl.BlockSpec(memory_space=pltpu.SMEM)] * n


def anywhere(n):
    return [pl.BlockSpec(memory_space=pl.ANY)] * n


def shaped(*dims):
    return jax.ShapeDtypeStruct(dims, F32)


def held(*dims):
    return pltpu.VMEM(dims, F32)


def call(kernel, name, ins, outs, scratch=(), out_specs=None, flops=None, grant=4, alias=None):
    made = pl.pallas_call(
        kernel,
        name=name,
        in_specs=ins,
        out_specs=tuple(out_specs or vmem(len(outs))),
        out_shape=tuple(outs),
        scratch_shapes=list(scratch),
        input_output_aliases=alias or {},
        compiler_params=pltpu.CompilerParams(vmem_limit_bytes=grant << 20),
        cost_estimate=(
            pl.CostEstimate(flops=flops, bytes_accessed=0, transcendentals=0) if flops else None
        ),
    )

    def run(*operands):
        return made(
            *(
                pltpu.with_memory_space_constraint(value, pltpu.VMEM)
                if spec.memory_space == pltpu.VMEM
                else value
                for spec, value in zip(ins, operands)
            )
        )

    return run


def both_ways(down, axis, up):
    count = lax.axis_size(axis)
    return (
        lax.ppermute(down, axis, [((i + 1) % count, i) for i in range(count)]),
        lax.ppermute(up, axis, [(i, (i + 1) % count) for i in range(count)]),
    )


def exchange(plan, own, down, up, tokens=(), speed=None):
    above, below = both_ways(down, "gy", up)
    extra = [] if speed is None else [speed]
    to_left, to_right = call(
        pack_columns(plan, bool(extra)),
        "pack_columns",
        vmem(3 + len(extra)) + anywhere(len(tokens)),
        [held(LEVELS, ROWS, COLS)] * 2,
    )(own, above, below, *extra, *tokens)
    from_right, from_left = both_ways(to_left, "gx", to_right)
    tiles = len(plan.carried)
    to_down, to_up, *speeds = call(
        pack_levels(plan, bool(extra)),
        "pack_levels",
        vmem(5 + len(extra)),
        [held(tiles, ROWS, COLS)] * 2 + [shaped(lax.axis_size("gy"), 1, COLS)] * len(extra),
    )(own, above, below, from_right, from_left, *extra)
    from_up, from_down = both_ways(to_down, "gz", to_up)
    return above, below, from_right, from_left, from_up, from_down, to_down, *speeds


def prepare(place_ref, fields, own, speed):
    own[...] = fields[...]
    keep = jnp.where(place_ref[0] == place_ref[1], 0.0, 1.0).astype(F32)
    most = jnp.zeros((ROWS, COLS), F32)
    for k in range(LEVELS):
        w = jnp.abs(fields[W, k])
        if k == LEVELS - 1:
            w = w * keep
        most = jnp.maximum(most, jnp.abs(fields[U, k]) + jnp.abs(fields[V, k]) + w)
    speed[...] = jnp.broadcast_to(jnp.max(most), speed.shape)


def droplets(radius, weight, column, counts, fall_depth, chunk, numbers, after=None):
    slots = radius.shape[0]
    if after is not None:
        counts, _ = lax.optimization_barrier((counts, after))
    made = []
    for n in numbers:
        whole = pl.BlockSpec((slots, chunk, ROWS, COLS), lambda i, n=n: (0, n, 0, 0))
        made.append(
            pl.pallas_call(
                deposit,
                name="deposit",
                grid=(1,),
                in_specs=[
                    whole,
                    whole,
                    whole,
                    pl.BlockSpec((chunk, ROWS, COLS), lambda i, n=n: (n, 0, 0)),
                    pl.BlockSpec((slots, chunk, ROWS, 1), lambda i, n=n: (0, n, 0, 0)),
                ],
                out_specs=pl.BlockSpec(
                    (chunk, FMAX + 1, 3, ROWS, COLS), lambda i: (0, 0, 0, 0, 0)
                ),
                out_shape=shaped(chunk, FMAX + 1, 3, ROWS, COLS),
                compiler_params=pltpu.CompilerParams(vmem_limit_bytes=12 << 20),
                cost_estimate=pl.CostEstimate(
                    flops=200_000_000, bytes_accessed=0, transcendentals=0
                ),
            )(radius, weight, column, counts, fall_depth)
        )
    return made


def per_device(fields, radius, weight, column, counts, fall_depth):
    place = lax.axis_index("gz")
    last = lax.axis_size("gz") - 1
    where = jnp.stack([place, jnp.int32(last)]).astype(jnp.int32)
    def drops(numbers, after=None):
        return droplets(radius, weight, column, counts, fall_depth, 2, numbers, after)

    own, speed = pl.pallas_call(
        prepare,
        name="prepare",
        in_specs=smem(1) + vmem(1),
        out_specs=tuple(vmem(2)),
        out_shape=(held(5, LEVELS, ROWS, COLS), shaped(ROWS, COLS)),
        compiler_params=pltpu.CompilerParams(vmem_limit_bytes=4 << 20),
    )(where, fields)
    pair = [(i, i ^ 1) for i in range(lax.axis_size("gx"))]
    speed = jnp.maximum(speed, lax.ppermute(speed, "gx", pair))
    speed = jnp.broadcast_to(speed[0:1], (lax.axis_size("gz"), 1, COLS))
    speed = jnp.max(lax.all_to_all(speed, "gz", 0, 0), axis=0)
    *near, from_up, from_down, sent, speed = exchange(FIRST, own, fields, fields, (), speed)
    early = drops(range(0, 2), sent)
    speed = lax.all_to_all(speed, "gy", 0, 0)
    ext = held(len(FIRST.tiles), DEPTH, ROWS, WIDE)
    start, flat = call(
        first_own,
        "first_own",
        smem(1) + vmem(5) + anywhere(1 + len(early)),
        [ext, held(2, LEVELS, 2 * ROWS, WIDE)],
    )(where, own, *near, speed, *early)
    start, rate0 = call(
        first_rates,
        "first_rates",
        smem(1) + vmem(4),
        [ext, held(2, DEPTH, 2 * ROWS, WIDE)],
        alias={1: 0},
    )(where, start, flat, from_up, from_down)
    s2, down, up, dt = call(
        two_sections,
        "two_sections",
        smem(1) + vmem(3),
        [held(5, LEVELS, ROWS, COLS)] + [held(3, LEVELS, ROWS, COLS)] * 2 + [shaped(1)],
        scratch=[
            pltpu.VMEM((5, DEPTH, 2 * ROWS, WIDE), F32),
            pltpu.VMEM((DEPTH, 2 * ROWS, WIDE), F32),
            pltpu.VMEM((4, DEPTH, 2 * ROWS, WIDE), F32),
        ],
        out_specs=vmem(3) + smem(1),
        grant=10,
    )(where, speed, start, rate0)
    middle = drops(range(2, 6), s2)
    *near, from_up, from_down, sent = exchange(SECOND, s2, down, up, middle)
    by_depth = early + middle + drops(range(6, 8), sent)
    ext = held(len(SECOND.tiles), DEPTH, ROWS, WIDE)
    around_s2, flat, flat_tracer = call(
        second_own,
        "second_own",
        vmem(5),
        [ext, held(1, LEVELS, 2 * ROWS, WIDE), held(LEVELS, ROWS, COLS)],
        flops=1_000_000_000,
    )(s2, *near)
    rows = held(DEPTH, 2 * ROWS, WIDE)
    _, tracer, landed, fallen, rate, warm = call(
        last_tracer,
        "last_tracer",
        smem(2) + vmem(6) + anywhere(len(by_depth)),
        [
            ext,
            held(LEVELS, ROWS, COLS),
            held(3, LEVELS, ROWS, COLS),
            held(3, FMAX, ROWS, COLS),
            rows,
            rows,
        ],
        scratch=[
            pltpu.VMEM((2, LEVELS, ROWS, COLS), F32),
            pltpu.VMEM((LEVELS, FMAX + 1, 3, ROWS, COLS), F32),
            pltpu.SemaphoreType.DMA((len(by_depth),)),
        ],
        alias={2: 0},
    )(where, dt, around_s2, flat, flat_tracer, from_up, from_down, own, *by_depth)
    count = lax.axis_size("gz")
    arrived = lax.ppermute(fallen, "gz", [((i + 1) % count, i) for i in range(count)])
    (new_fields,) = call(
        last_section,
        "last_section",
        smem(2) + vmem(4),
        [shaped(5, LEVELS, ROWS, COLS)],
        scratch=[pltpu.VMEM((4, DEPTH, 2 * ROWS, WIDE), F32)],
        flops=1_000_000_000,
    )(where, dt, rate, warm, start, tracer)
    (moments,) = call(
        land, "land", smem(1) + vmem(2), [shaped(3, LEVELS, ROWS, COLS)]
    )(where, landed, arrived)
    return (new_fields, moments)


def solution(mesh):
    spread = P(None, "gz", "gy", "gx")
    return jax.shard_map(
        per_device,
        mesh=mesh,
        in_specs=(spread, spread, spread, spread, P("gz", "gy", "gx"), spread),
        out_specs=(spread, spread),
        check_vma=False,
    )
```

```python
import jax
import jax.numpy as jnp
from jax import lax
from jax.experimental import pallas as pl
from jax.experimental.pallas import tpu as pltpu
from jax.sharding import Mesh
from jax.sharding import PartitionSpec as P

NS = 4
FMAX = 8
GY = ("gy_hi", "gy_lo")

sound_speed = 10.0
buoyancy = 0.5
courant_goal = 0.6
growth = 0.3

LEVELS, ROWS, COLS = 16, 8, 128
WIDE = 2 * COLS
REACH = 7
DEPTH = LEVELS + 2 * REACH
EDGE = 8
F32 = jnp.float32
C, PR, U, V, W = range(5)


class Plan:
    def __init__(self, tall, reach, sent):
        self.tall, self.reach = tall, reach
        self.tiles = [
            (field, part)
            for field in range(5)
            for part in ("oab" if field in tall else "on")
        ]
        self.at = {tile: n for n, tile in enumerate(self.tiles)}
        self.carried = []
        for a in range(reach):
            for field in range(5):
                for part in sent[field][a] if a < len(sent[field]) else "":
                    self.carried.append((a, (field, part), 0))
            if a < reach - 1:
                self.carried += [(a, None, 0), (a, None, 1)]

    def rows(self, ref, field, l):
        return jnp.concatenate(
            [
                ref[self.at[field, part], l]
                for part in ("oab" if field in self.tall else "on")
            ],
            axis=0,
        )

    def sixteen(self, ref, field, l):
        value = self.rows(ref, field, l)
        return sixteen(value) if field in self.tall else value


def lanes(shape):
    return lax.broadcasted_iota(jnp.int32, shape, len(shape) - 1)


def lower_rows(shape):
    return lax.broadcasted_iota(jnp.int32, shape, 0) < ROWS // 2


def around(above, below):
    return jnp.where(lower_rows(above.shape), above, below)


def sixteen(value):
    return jnp.concatenate(
        [value[0:ROWS], around(value[ROWS : 2 * ROWS], value[2 * ROWS :])], axis=0
    )


def raw_tile(refs, field, part, k):
    own, above, below = refs
    if part == "o":
        return own[field, k]
    if part == "n":
        return around(above[field, k], below[field, k])
    return (above if part == "a" else below)[field, k]


SHARED = {C: (1, 0), U: (1, 1), V: (2, 0), W: (2, 1)}


def shared_rows(read):
    down, up = [read(PR)], [read(PR)]
    for first, second in ((C, U), (V, W)):
        one, other = read(first), pltpu.roll(read(second), ROWS // 2, 0)
        down.append(around(one, other))
        up.append(around(other, one))
    return down, up


def shared_tile(refs, field, part, k):
    own, above, below = refs
    if part == "o":
        return own[field, k]
    if part == "n" and field == PR:
        return around(above[0, k], below[0, k])
    if part == "n":
        index, half = SHARED[field]
        if half == 0:
            return around(above[index, k], below[index, k])
        return pltpu.roll(around(below[index, k], above[index, k]), ROWS // 2, 0)
    return (above if part == "a" else below)[0, k]


THREE, TWO, ONE = "oab", "on", "o"
FIRST = Plan(
    (C, PR, V),
    7,
    {
        C: [THREE] + [TWO] * 4 + [ONE],
        PR: [THREE] * 2 + [TWO] * 4 + [ONE],
        U: [TWO] * 4,
        V: [TWO] * 4,
        W: [TWO] * 4 + [ONE],
    },
)
SECOND = Plan(
    (PR,),
    6,
    {
        C: [TWO] * 3 + [ONE],
        PR: [THREE] + [TWO] * 4 + [ONE],
        U: [TWO] * 3,
        V: [TWO] * 3,
        W: [TWO] * 3 + [ONE],
    },
)
TILE_OF = {FIRST: raw_tile, SECOND: shared_tile}


SPARE = 104


def pack_columns(plan, with_speed):
    def kernel(own, above, below, *rest):
        to_left, to_right = rest[-2:]
        lane = lanes((ROWS, COLS))
        filler = jnp.zeros((ROWS, COLS), F32)
        if with_speed:
            filler = filler + jnp.max(rest[0][...])

        def one(k, _):
            left = filler
            right = filler
            for n, (field, part) in enumerate(plan.tiles):
                start = n * EDGE
                here = (lane >= start) & (lane < start + EDGE)
                value = TILE_OF[plan]((own, above, below), field, part, k)
                first = pltpu.roll(value, start, 1) if start else value
                last = pltpu.roll(value, (start + EDGE) % COLS, 1)
                left = jnp.where(here, first, left)
                right = jnp.where(here, last, right)
            to_left[k] = left
            to_right[k] = right
            return 0

        def some(levels, _):
            for k in levels:
                one(k, 0)
            return 0

        sweep(0, LEVELS, 8, some)

    return kernel


def halo_columns(from_right, from_left, n):
    start = n * EDGE
    right = pltpu.roll(from_right, COLS - start, 1) if start else from_right
    left = pltpu.roll(from_left, (COLS - EDGE - start) % COLS, 1)
    return jnp.where(lanes((ROWS, COLS)) < COLS // 2, right, left)


def pack_levels(plan, with_speed):
    def kernel(own, above, below, from_right, from_left, *rest):
        if with_speed:
            speed, to_down, to_up, speeds = rest
            near = jnp.maximum(from_right[0], from_left[0])
            near = jnp.where(lanes((ROWS, COLS)) < SPARE, 0.0, near)
            top = jnp.maximum(jnp.max(near), jnp.max(speed[...]))
            speeds[...] = jnp.broadcast_to(top, speeds.shape)
        else:
            to_down, to_up = rest
        for index, (a, tile, side) in enumerate(plan.carried):
            for out, k in ((to_down, a), (to_up, LEVELS - 1 - a)):
                if tile:
                    out[index] = TILE_OF[plan]((own, above, below), *tile, k)
                else:
                    out[index] = (from_left if side else from_right)[k]

    return kernel


def place_own(plan, refs, ext):
    own, above, below, from_right, from_left = refs

    def middle(levels, _):
        for k in levels:
            right, left = from_right[k], from_left[k]
            for n, (field, part) in enumerate(plan.tiles):
                ext[n, REACH + k, :, 0:COLS] = TILE_OF[plan]((own, above, below), field, part, k)
                ext[n, REACH + k, :, COLS:WIDE] = halo_columns(right, left, n)
        return 0

    sweep(0, LEVELS, 4, middle)


def place_halo(plan, from_up, from_down, ext, place, last):
    columns = {(a, side): i for i, (a, tile, side) in enumerate(plan.carried) if not tile}
    for message, level, there in (
        (from_down, lambda a: REACH - 1 - a, place > 0),
        (from_up, lambda a: REACH + LEVELS + a, place < last),
    ):
        keep = jnp.where(there, 1.0, 0.0).astype(F32)
        for index, (a, tile, _) in enumerate(plan.carried):
            if not tile:
                continue
            field, part = tile
            value = message[index] * keep
            for kept in "ab" if part == "n" and field in plan.tall else part:
                n = plan.at[field, kept]
                ext[n, level(a), :, 0:COLS] = value
                if (a, 0) in columns:
                    ext[n, level(a), :, COLS:WIDE] = (
                        halo_columns(message[columns[a, 0]], message[columns[a, 1]], n) * keep
                    )


def shift(value, by, axis):
    return pltpu.roll(value, (-by) % value.shape[axis], axis)


def face_flux(q, wind):
    central = 37.0 * (q[2] + q[3]) - 8.0 * (q[1] + q[4]) + (q[0] + q[5])
    upwind = 10.0 * (q[3] - q[2]) - 5.0 * (q[4] - q[1]) + (q[5] - q[0])
    return wind * central - jnp.abs(wind) * upwind


def flat_flux(q, wind, axis):
    flux = face_flux([shift(q, by, axis) if by else q for by in range(-2, 4)], wind)
    return flux - shift(flux, -1, axis)


def rows_flux(q, wind):
    if wind.shape[0] == 24:
        return sixteen(flat_flux(q, wind, 0))
    if q.shape[0] == 24:
        flux = face_flux([sixteen(shift(q, by, 0) if by else q) for by in range(-2, 4)], wind)
        return flux - shift(flux, -1, 0)
    return flat_flux(q, wind, 0)


def level_flux(read, wind, l):
    return face_flux([read(l + by) for by in range(-2, 4)], wind)


def in_domain(l, place, last, lid):
    g = place * LEVELS + l - REACH
    top = (last + 1) * LEVELS - (1 if lid else 0)
    return jnp.where((g >= 0) & (g < top), 1.0, 0.0).astype(F32)


SIXTIETH = -1.0 / 60.0


def sweep(first, count, most, body, carry=0):
    size = max(n for n in range(1, most + 1) if count % n == 0)

    def run(i, carry):
        start = first + i * size
        return body([start + n for n in range(size)], carry)

    return lax.fori_loop(0, count // size, run, carry)


def flat_part(plan, ext, field, l):
    return flat_flux(plan.sixteen(ext, field, l), plan.sixteen(ext, U, l), 1) + rows_flux(
        plan.rows(ext, field, l), plan.rows(ext, V, l)
    )


def flat_own(plan, ext, fields, flat):
    def some(levels, _):
        results = [(n, l, flat_part(plan, ext, f, l)) for l in levels for n, f in enumerate(fields)]
        for n, l, value in results:
            flat[n, l - REACH] = value
        return 0

    sweep(REACH, LEVELS, 4, some)


def rates(plan, ext, fields, write, around_own, most, flat=None):
    reads = [lambda l, f=f: plan.sixteen(ext, f, l) for f in fields]

    def some(levels, lows, flat=None):
        results = []
        for l in levels:
            w = plan.sixteen(ext, W, l)
            highs = []
            for n, f in enumerate(fields):
                high = level_flux(reads[n], w, l)
                level = flat[n, l - REACH] if flat is not None else flat_part(plan, ext, f, l)
                results.append((n, l, (level + (high - lows[n])) * SIXTIETH))
                highs.append(high)
            lows = tuple(highs)
        for result in results:
            write(*result)
        return lows

    first = REACH - around_own
    w = plan.sixteen(ext, W, first - 1)
    lows = tuple(level_flux(read, w, first - 1) for read in reads)
    if flat is None:
        sweep(first, LEVELS + 2 * around_own, most, some, lows)
        return
    lows = sweep(first, around_own, most, some, lows)
    lows = sweep(REACH, LEVELS, 4, lambda levels, c: some(levels, c, flat), lows)
    sweep(REACH + LEVELS, around_own, most, some, lows)


def first_own(place_ref, own, above, below, from_right, from_left, ext, flat):
    place_own(FIRST, (own, above, below, from_right, from_left), ext)

    @pl.when(place_ref[0] == place_ref[1])
    def _():
        for part in "on":
            ext[FIRST.at[W, part], REACH + LEVELS - 1] = jnp.zeros((ROWS, WIDE), F32)

    flat_own(FIRST, ext, (C, PR), flat)


def first_rates(place_ref, ext_in, flat, from_up, from_down, *rest):
    ext, rate = rest[-2:]
    place_halo(FIRST, from_up, from_down, ext, place_ref[0], place_ref[1])

    def write(n, l, value):
        rate[n, l] = value

    rates(FIRST, ext, (C, PR), write, 4, 4, flat)


def acoustic(p, u, v, w, read_c, rate, step, first, count, place, last):
    pull = step * sound_speed

    def level(value):
        return sixteen(value) if value.shape[0] == 24 else value

    def wind_w(l, lift_low, lift_high, p_here, p_above):
        lift = (buoyancy * 0.5) * (lift_low + lift_high)
        return (w[0](l) + step * lift - pull * (p_above - p_here)) * in_domain(l, place, last, True)

    def some(levels, w_low):
        talls = [p[0](l) for l in (*levels, levels[-1] + 1)]
        cells = [level(value) for value in talls]
        warm = [read_c(l) for l in (*levels, levels[-1] + 1)]
        results = []
        for n, l in enumerate(levels):
            p_here = cells[n]
            w_new = wind_w(l, warm[n], warm[n + 1], p_here, cells[n + 1])
            u_new = u[0](l) - pull * (shift(p_here, 1, 1) - p_here)
            v_old = v[0](l)
            if v_old.shape[0] == 24:
                v_tall = v_old - pull * (shift(talls[n], 1, 0) - talls[n])
                v_new, v_flow = sixteen(v_tall), sixteen(v_tall - shift(v_tall, -1, 0))
            else:
                v_new = v_old - pull * (shift(p_here, 1, 0) - p_here)
                v_flow = v_new - shift(v_new, -1, 0)
            divergence = (u_new - shift(u_new, -1, 1)) + v_flow + (w_new - w_low)
            p_new = (p_here + step * rate(l) - pull * divergence) * in_domain(
                l, place, last, False
            )
            results.append((l, p_new, u_new, v_new, w_new))
            w_low = w_new
        for l, *news in results:
            for target, value in zip((p, u, v, w), news):
                target[1](l, value)
        return w_low

    low = first - 1
    w_low = wind_w(low, read_c(low), read_c(first), level(p[0](low)), level(p[0](first)))
    w[1](low, w_low)
    sweep(first, count, 12, some, w_low)


def access(ref, *lead):
    def read(l):
        return ref[(*lead, l)]

    def write(l, value):
        ref[(*lead, l)] = value

    return read, write


def begin(start, field, tall=False):
    return lambda l: (FIRST.rows if tall else FIRST.sixteen)(start, field, l)


def own_write(ref, field):
    def write(l, value):
        if not isinstance(l, int):
            ref[field, l - REACH] = value[0:ROWS, 0:COLS]

    return write


def tracer_flat(tiles, u, v, l):
    rows = flat_flux(tiles(l)[:, 0:COLS], v(l)[:, 0:COLS], 0)[0:ROWS]
    return rows + flat_flux(tiles(l)[0:ROWS], u(l)[0:ROWS], 1)[:, 0:COLS]


def tracer_high(tiles, w, l):
    return level_flux(lambda m: tiles(m)[0:ROWS, 0:COLS], w(l)[0:ROWS, 0:COLS], l)


def two_sections(place_ref, speed, other_speed, start, rate0, s2, down, up, dt_out, s1, rate1, fast):
    place, last = place_ref[0], place_ref[1]
    dt = courant_goal / (1.0 + jnp.max(jnp.maximum(speed[...], other_speed[...])))
    dt_out[0] = dt
    third = dt * (1.0 / 3.0)

    def tracer(levels, _):
        for l in levels:
            s1[C, l] = (FIRST.sixteen(start, C, l) + third * rate0[0, l]) * in_domain(
                l, place, last, False
            )
        return 0

    sweep(REACH - 4, LEVELS + 8, 4, tracer)
    acoustic(
        (begin(start, PR, True), access(s1, PR)[1]),
        (begin(start, U), access(s1, U)[1]),
        (begin(start, V, True), access(s1, V)[1]),
        (begin(start, W), access(s1, W)[1]),
        begin(start, C),
        access(rate0, 1)[0],
        third,
        REACH - 4,
        LEVELS + 8,
        place,
        last,
    )
    half = dt * 0.5
    tiles = access(s1, C)[0]
    winds = [access(s1, f)[0] for f in (U, V, W)]

    def own_tracer(levels, low):
        results = []
        for l in levels:
            high = tracer_high(tiles, winds[2], l)
            tendency = (tracer_flat(tiles, *winds[:2], l) + (high - low)) * SIXTIETH
            low = high
            results.append(start[FIRST.at[C, "o"], l, :, 0:COLS] + half * tendency)
        for l, value in zip(levels, results):
            s2[C, l - REACH] = value
        return low

    sweep(REACH, LEVELS, 8, own_tracer, tracer_high(tiles, winds[2], REACH - 1))

    def write(n, l, value):
        rate1[l] = value

    rates(SECTION, s1, (PR,), write, 1, 6)
    step = half / (NS // 2)
    acoustic(
        (begin(start, PR), access(fast, 0)[1]),
        (begin(start, U), access(fast, 1)[1]),
        (begin(start, V), access(fast, 2)[1]),
        (begin(start, W), access(fast, 3)[1]),
        access(s1, C)[0],
        access(rate1)[0],
        step,
        REACH - 1,
        LEVELS + 2,
        place,
        last,
    )
    acoustic(
        (access(fast, 0)[0], own_write(s2, PR)),
        (access(fast, 1)[0], own_write(s2, U)),
        (access(fast, 2)[0], own_write(s2, V)),
        (access(fast, 3)[0], own_write(s2, W)),
        access(s1, C)[0],
        access(rate1)[0],
        step,
        REACH,
        LEVELS,
        place,
        last,
    )

    def share(levels, _):
        made = [shared_rows(lambda f, k=k: s2[f, k]) for k in levels]
        for k, (to_down, to_up) in zip(levels, made):
            for n in range(3):
                down[n, k] = to_down[n]
                up[n, k] = to_up[n]
        return 0

    sweep(0, LEVELS, 4, share)


class Whole:
    def rows(self, ref, field, l):
        return ref[field, l]

    sixteen = rows


SECTION = Whole()


def second_own(own, above, below, from_right, from_left, ext, flat, tracer):
    place_own(SECOND, (own, above, below, from_right, from_left), ext)
    flat_own(SECOND, ext, (PR,), flat)
    tiles, u, v = (lambda l, f=f: SECOND.rows(ext, f, l) for f in (C, U, V))

    def some(levels, _):
        results = [tracer_flat(tiles, u, v, l) for l in levels]
        for l, value in zip(levels, results):
            tracer[l - REACH] = value
        return 0

    sweep(REACH, LEVELS, 4, some)


def last_tracer(
    place_ref, dt_ref, ext_in, flat, flat_tracer, from_up, from_down, initial, *rest
):
    *chunks, ext, tracer, landed, fallen, rate, warm, factor, by_depth, sem = rest
    dt = dt_ref[0]
    each = LEVELS // len(chunks)
    copies = [
        pltpu.make_async_copy(chunk, by_depth.at[pl.ds(n * each, each)], sem.at[n])
        for n, chunk in enumerate(chunks)
    ]
    for copy in copies:
        copy.start()
    place_halo(SECOND, from_up, from_down, ext, place_ref[0], place_ref[1])

    def write(n, l, value):
        rate[l] = value

    rates(SECOND, ext, (PR,), write, 3, 3, flat)

    def keep(levels, _):
        for l in levels:
            warm[l] = SECOND.rows(ext, C, l)
        return 0

    sweep(REACH - 4, LEVELS + 8, 4, keep)
    tiles = lambda l: SECOND.rows(ext, C, l)
    w = lambda l: SECOND.rows(ext, W, l)

    def some(levels, low):
        results = []
        for l in levels:
            high = tracer_high(tiles, w, l)
            tendency = (flat_tracer[l - REACH] + (high - low)) * SIXTIETH
            low = high
            c = initial[C, l - REACH] + dt * tendency
            grown = jnp.exp(growth * c)
            results.append((c, grown, grown * jnp.exp((0.5 * growth) * c)))
        for l, (c, second, third) in zip(levels, results):
            tracer[l - REACH] = c
            factor[0, l - REACH] = second
            factor[1, l - REACH] = third
        return low

    sweep(REACH, LEVELS, 4, some, tracer_high(tiles, w, REACH - 1))
    for copy in copies:
        copy.wait()
    for target in range(-FMAX, LEVELS):
        for moment in range(3):
            total = None
            for depth in range(FMAX + 1):
                k = target + depth
                if 0 <= k < LEVELS:
                    value = by_depth[k, depth, moment]
                    if moment:
                        value = value * factor[moment - 1, k]
                    total = value if total is None else total + value
            if target < 0:
                fallen[moment, target + FMAX] = total
            else:
                landed[moment, target] = total


def last_section(place_ref, dt_ref, rate, warm, start, tracer, out, fast):
    place, last = place_ref[0], place_ref[1]
    step = dt_ref[0] / NS
    out[C] = tracer[...]
    names = (PR, U, V, W)
    for repeat in range(NS):
        reads = [
            begin(start, f) if repeat == 0 else access(fast, n)[0] for n, f in enumerate(names)
        ]
        writes = [
            own_write(out, f) if repeat == NS - 1 else access(fast, n)[1]
            for n, f in enumerate(names)
        ]
        acoustic(
            *zip(reads, writes),
            access(warm)[0],
            access(rate)[0],
            step,
            REACH - 3 + repeat,
            LEVELS + 6 - 2 * repeat,
            place,
            last,
        )


def land(place_ref, landed, arrived, out):
    keep = jnp.where(place_ref[0] < place_ref[1], 1.0, 0.0).astype(F32)
    out[:, 0 : LEVELS - FMAX] = landed[:, 0 : LEVELS - FMAX]
    out[:, LEVELS - FMAX :] = landed[:, LEVELS - FMAX :] + keep * arrived[...]


def deposit(radius, weight, column, counts, fall_depth, out):
    slots, levels = radius.shape[0], radius.shape[1]
    target = lax.broadcasted_iota(jnp.int32, (COLS, COLS), 0)
    row = lax.broadcasted_iota(jnp.int32, (ROWS, COLS), 0)
    per_step = 4

    for k in range(levels):
        out[k] = jnp.zeros(out.shape[1:], F32)
        live = counts[k]

        def some(step, _, k=k, live=live):
            sums = [[None] * 3 for _ in range(FMAX + 1)]
            for part in range(per_step):
                s = step * per_step + part
                r = radius[s, k]
                number = jnp.where(s < live, weight[s, k], 0.0)
                area = number * r * r
                terms = []
                for t in (number, area, area * r):
                    high = t.astype(jnp.bfloat16).astype(F32)
                    terms += [high, t - high]
                cols = column[s, k]
                left, right = [], []
                for j in range(ROWS):
                    left.append(
                        jnp.concatenate([jnp.where(row == j, t, 0.0) for t in terms], axis=0)
                    )
                    right.append(jnp.where(cols[j : j + 1] == target, 1.0, 0.0).astype(F32))
                sent = lax.dot_general(
                    jnp.concatenate(left, axis=1),
                    jnp.concatenate(right, axis=1),
                    (((1,), (1,)), ((), ())),
                    preferred_element_type=F32,
                )
                depth = jnp.broadcast_to(fall_depth[s, k], (ROWS, COLS))
                for d in range(FMAX + 1):
                    falls = depth == d
                    for m in range(3):
                        both = sent[16 * m : 16 * m + 8] + sent[16 * m + 8 : 16 * m + 16]
                        value = jnp.where(falls, both, 0.0)
                        sums[d][m] = value if sums[d][m] is None else sums[d][m] + value
            for d in range(FMAX + 1):
                for m in range(3):
                    out[k, d, m] += sums[d][m]
            return 0

        lax.fori_loop(0, slots // per_step, some, 0)


def vmem(n):
    return [pl.BlockSpec(memory_space=pltpu.VMEM)] * n


def smem(n):
    return [pl.BlockSpec(memory_space=pltpu.SMEM)] * n


def far(n):
    return [pl.BlockSpec(memory_space=pltpu.HBM)] * n


def shaped(*dims):
    return jax.ShapeDtypeStruct(dims, F32)


def held(*dims):
    return pltpu.VMEM(dims, F32)


def call(kernel, name, ins, outs, scratch=(), out_specs=None, flops=None, grant=4, alias=None):
    made = pl.pallas_call(
        kernel,
        name=name,
        in_specs=ins,
        out_specs=tuple(out_specs or vmem(len(outs))),
        out_shape=tuple(outs),
        scratch_shapes=list(scratch),
        input_output_aliases=alias or {},
        compiler_params=pltpu.CompilerParams(vmem_limit_bytes=grant << 20),
        cost_estimate=(
            pl.CostEstimate(flops=flops, bytes_accessed=0, transcendentals=0) if flops else None
        ),
    )

    def run(*operands):
        return made(
            *(
                pltpu.with_memory_space_constraint(value, spec.memory_space)
                if spec.memory_space != pltpu.SMEM
                else value
                for spec, value in zip(ins, operands)
            )
        )

    return run


def both_ways(down, axis, up):
    count = lax.axis_size(axis)
    return (
        lax.ppermute(down, axis, [((i + 1) % count, i) for i in range(count)]),
        lax.ppermute(up, axis, [(i, (i + 1) % count) for i in range(count)]),
    )


def exchange(plan, own, down, up, tokens=(), speed=None):
    above, below = both_ways(down, GY, up)
    extra = [] if speed is None else [speed]
    to_left, to_right = call(
        pack_columns(plan, bool(extra)),
        "pack_columns",
        vmem(3 + len(extra)) + far(len(tokens)),
        [held(LEVELS, ROWS, COLS)] * 2,
    )(own, above, below, *extra, *tokens)
    from_right, from_left = both_ways(to_left, "gx", to_right)
    tiles = len(plan.carried)
    to_down, to_up, *speeds = call(
        pack_levels(plan, bool(extra)),
        "pack_levels",
        vmem(5 + len(extra)),
        [held(tiles, ROWS, COLS)] * 2 + [shaped(ROWS, COLS)] * len(extra),
    )(own, above, below, from_right, from_left, *extra)
    from_up, from_down = both_ways(to_down, "gz", to_up)
    return above, below, from_right, from_left, from_up, from_down, to_down, *speeds


def prepare(place_ref, fields, own, speed):
    own[...] = fields[...]
    keep = jnp.where(place_ref[0] == place_ref[1], 0.0, 1.0).astype(F32)
    most = jnp.zeros((ROWS, COLS), F32)
    for k in range(LEVELS):
        w = jnp.abs(fields[W, k])
        if k == LEVELS - 1:
            w = w * keep
        most = jnp.maximum(most, jnp.abs(fields[U, k]) + jnp.abs(fields[V, k]) + w)
    speed[...] = jnp.broadcast_to(jnp.max(most), speed.shape)


def droplets(radius, weight, column, counts, fall_depth, chunk, numbers, after=None):
    slots = radius.shape[0]
    if after is not None:
        counts, _ = lax.optimization_barrier((counts, after))
    made = []
    for n in numbers:
        whole = pl.BlockSpec((slots, chunk, ROWS, COLS), lambda i, n=n: (0, n, 0, 0))
        made.append(
            pl.pallas_call(
                deposit,
                name="deposit",
                grid=(1,),
                in_specs=[
                    whole,
                    whole,
                    whole,
                    pl.BlockSpec((chunk, ROWS, COLS), lambda i, n=n: (n, 0, 0)),
                    pl.BlockSpec((slots, chunk, ROWS, 1), lambda i, n=n: (0, n, 0, 0)),
                ],
                out_specs=pl.BlockSpec(
                    (chunk, FMAX + 1, 3, ROWS, COLS), lambda i: (0, 0, 0, 0, 0)
                ),
                out_shape=pltpu.HBM((chunk, FMAX + 1, 3, ROWS, COLS), F32),
                compiler_params=pltpu.CompilerParams(vmem_limit_bytes=12 << 20),
                cost_estimate=pl.CostEstimate(
                    flops=200_000_000, bytes_accessed=0, transcendentals=0
                ),
            )(radius, weight, column, counts, fall_depth)
        )
    return made


def per_device(fields, radius, weight, column, counts, fall_depth):
    place = lax.axis_index("gz")
    last = lax.axis_size("gz") - 1
    where = jnp.stack([place, jnp.int32(last)]).astype(jnp.int32)
    def drops(numbers, after=None):
        return droplets(radius, weight, column, counts, fall_depth, 2, numbers, after)

    own, speed = pl.pallas_call(
        prepare,
        name="prepare",
        in_specs=smem(1) + vmem(1),
        out_specs=tuple(vmem(2)),
        out_shape=(held(5, LEVELS, ROWS, COLS), shaped(ROWS, COLS)),
        compiler_params=pltpu.CompilerParams(vmem_limit_bytes=4 << 20),
    )(where, fields)
    pair = [(i, i ^ 1) for i in range(lax.axis_size("gx"))]
    speed = jnp.maximum(speed, lax.ppermute(speed, "gx", pair))
    plane = ("gy_hi", "gz")
    speed = jnp.broadcast_to(speed[0:1], (lax.axis_size(plane), 1, COLS))
    speed = jnp.max(lax.all_to_all(speed, plane, 0, 0), axis=0)
    *near, from_up, from_down, sent, speed = exchange(FIRST, own, fields, fields, (), speed)
    other_speed = lax.ppermute(speed, "gy_lo", [(0, 1), (1, 0)])
    by_depth = drops(range(0, 2), sent)
    ext = held(len(FIRST.tiles), DEPTH, ROWS, WIDE)
    start, flat = call(
        first_own,
        "first_own",
        smem(1) + vmem(5),
        [ext, held(2, LEVELS, 2 * ROWS, WIDE)],
    )(where, own, *near)
    start, rate0 = call(
        first_rates,
        "first_rates",
        smem(1) + vmem(4) + far(len(by_depth)),
        [ext, held(2, DEPTH, 2 * ROWS, WIDE)],
        alias={1: 0},
    )(where, start, flat, from_up, from_down, *by_depth)
    s2, down, up, dt = call(
        two_sections,
        "two_sections",
        smem(1) + vmem(4),
        [held(5, LEVELS, ROWS, COLS)] + [held(3, LEVELS, ROWS, COLS)] * 2 + [shaped(1)],
        scratch=[
            pltpu.VMEM((5, DEPTH, 2 * ROWS, WIDE), F32),
            pltpu.VMEM((DEPTH, 2 * ROWS, WIDE), F32),
            pltpu.VMEM((4, DEPTH, 2 * ROWS, WIDE), F32),
        ],
        out_specs=vmem(3) + smem(1),
        grant=10,
    )(where, speed, other_speed, start, rate0)
    middle = drops(range(2, 7), s2)
    *near, from_up, from_down, sent = exchange(SECOND, s2, down, up, middle)
    by_depth = by_depth + middle + drops(range(7, 8), sent)
    ext = held(len(SECOND.tiles), DEPTH, ROWS, WIDE)
    around_s2, flat, flat_tracer = call(
        second_own,
        "second_own",
        vmem(5),
        [ext, held(1, LEVELS, 2 * ROWS, WIDE), held(LEVELS, ROWS, COLS)],
        flops=1_000_000_000,
    )(s2, *near)
    rows = held(DEPTH, 2 * ROWS, WIDE)
    _, tracer, landed, fallen, rate, warm = call(
        last_tracer,
        "last_tracer",
        smem(2) + vmem(6) + far(len(by_depth)),
        [
            ext,
            held(LEVELS, ROWS, COLS),
            held(3, LEVELS, ROWS, COLS),
            held(3, FMAX, ROWS, COLS),
            rows,
            rows,
        ],
        scratch=[
            pltpu.VMEM((2, LEVELS, ROWS, COLS), F32),
            pltpu.VMEM((LEVELS, FMAX + 1, 3, ROWS, COLS), F32),
            pltpu.SemaphoreType.DMA((len(by_depth),)),
        ],
        alias={2: 0},
    )(where, dt, around_s2, flat, flat_tracer, from_up, from_down, own, *by_depth)
    count = lax.axis_size("gz")
    arrived = lax.ppermute(fallen, "gz", [((i + 1) % count, i) for i in range(count)])
    (new_fields,) = call(
        last_section,
        "last_section",
        smem(2) + vmem(4),
        [shaped(5, LEVELS, ROWS, COLS)],
        scratch=[pltpu.VMEM((4, DEPTH, 2 * ROWS, WIDE), F32)],
        flops=1_000_000_000,
    )(where, dt, rate, warm, start, tracer)
    (moments,) = call(
        land, "land", smem(1) + vmem(2), [shaped(3, LEVELS, ROWS, COLS)]
    )(where, landed, arrived)
    return (new_fields, moments)


def solution(mesh):
    count = mesh.shape["gy"]
    split = Mesh(
        mesh.devices.reshape(mesh.shape["gx"], count // 2, 2, mesh.shape["gz"]),
        ("gx", *GY, "gz"),
    )
    spread = P(None, "gz", GY, "gx")
    return jax.shard_map(
        per_device,
        mesh=split,
        in_specs=(spread, spread, spread, spread, P("gz", GY, "gx"), spread),
        out_specs=(spread, spread),
        check_vma=False,
    )
```

```python
import jax
import jax.numpy as jnp
from jax import lax
from jax.experimental import pallas as pl
from jax.experimental.pallas import tpu as pltpu
from jax.sharding import Mesh
from jax.sharding import PartitionSpec as P

NS = 4
FMAX = 8
GY = ("gy_hi", "gy_lo")

sound_speed = 10.0
buoyancy = 0.5
courant_goal = 0.6
growth = 0.3

LEVELS, ROWS, COLS = 16, 8, 128
WIDE = 2 * COLS
REACH = 7
DEPTH = LEVELS + 2 * REACH
EDGE = 8
F32 = jnp.float32
C, PR, U, V, W = range(5)


class Plan:
    def __init__(self, tall, reach, sent):
        self.tall, self.reach = tall, reach
        self.tiles = [
            (field, part)
            for field in range(5)
            for part in ("oab" if field in tall else "on")
        ]
        self.at = {tile: n for n, tile in enumerate(self.tiles)}
        self.carried = []
        for a in range(reach):
            for field in range(5):
                for part in sent[field][a] if a < len(sent[field]) else "":
                    self.carried.append((a, (field, part), 0))
            if a < reach - 1:
                self.carried += [(a, None, 0), (a, None, 1)]

    def rows(self, ref, field, l):
        return jnp.concatenate(
            [
                ref[self.at[field, part], l]
                for part in ("oab" if field in self.tall else "on")
            ],
            axis=0,
        )

    def sixteen(self, ref, field, l):
        value = self.rows(ref, field, l)
        return sixteen(value) if field in self.tall else value


def lanes(shape):
    return lax.broadcasted_iota(jnp.int32, shape, len(shape) - 1)


def lower_rows(shape):
    return lax.broadcasted_iota(jnp.int32, shape, 0) < ROWS // 2


def around(above, below):
    return jnp.where(lower_rows(above.shape), above, below)


def sixteen(value):
    return jnp.concatenate(
        [value[0:ROWS], around(value[ROWS : 2 * ROWS], value[2 * ROWS :])], axis=0
    )


def raw_tile(refs, field, part, k):
    own, above, below = refs
    if part == "o":
        return own[field, k]
    if part == "n":
        return around(above[field, k], below[field, k])
    return (above if part == "a" else below)[field, k]


SHARED = {C: (1, 0), U: (1, 1), V: (2, 0), W: (2, 1)}


def shared_rows(read):
    down, up = [read(PR)], [read(PR)]
    for first, second in ((C, U), (V, W)):
        one, other = read(first), pltpu.roll(read(second), ROWS // 2, 0)
        down.append(around(one, other))
        up.append(around(other, one))
    return down, up


def shared_tile(refs, field, part, k):
    own, above, below = refs
    if part == "o":
        return own[field, k]
    if part == "n" and field == PR:
        return around(above[0, k], below[0, k])
    if part == "n":
        index, half = SHARED[field]
        if half == 0:
            return around(above[index, k], below[index, k])
        return pltpu.roll(around(below[index, k], above[index, k]), ROWS // 2, 0)
    return (above if part == "a" else below)[0, k]


THREE, TWO, ONE = "oab", "on", "o"
FIRST = Plan(
    (C, PR, V),
    7,
    {
        C: [THREE] + [TWO] * 4 + [ONE],
        PR: [THREE] * 2 + [TWO] * 4 + [ONE],
        U: [TWO] * 4,
        V: [TWO] * 4,
        W: [TWO] * 4 + [ONE],
    },
)
SECOND = Plan(
    (PR,),
    6,
    {
        C: [TWO] * 3 + [ONE],
        PR: [THREE] + [TWO] * 4 + [ONE],
        U: [TWO] * 3,
        V: [TWO] * 3,
        W: [TWO] * 3 + [ONE],
    },
)
TILE_OF = {FIRST: raw_tile, SECOND: shared_tile}


SPARE = 104


def pack_columns(plan, with_speed):
    def kernel(own, above, below, *rest):
        to_left, to_right = rest[-2:]
        lane = lanes((ROWS, COLS))
        filler = jnp.zeros((ROWS, COLS), F32)
        if with_speed:
            filler = filler + jnp.max(rest[0][...])

        def one(k, _):
            left = filler
            right = filler
            for n, (field, part) in enumerate(plan.tiles):
                start = n * EDGE
                here = (lane >= start) & (lane < start + EDGE)
                value = TILE_OF[plan]((own, above, below), field, part, k)
                first = pltpu.roll(value, start, 1) if start else value
                last = pltpu.roll(value, (start + EDGE) % COLS, 1)
                left = jnp.where(here, first, left)
                right = jnp.where(here, last, right)
            to_left[k] = left
            to_right[k] = right
            return 0

        def some(levels, _):
            for k in levels:
                one(k, 0)
            return 0

        sweep(0, LEVELS, 8, some)

    return kernel


def halo_columns(from_right, from_left, n):
    start = n * EDGE
    right = pltpu.roll(from_right, COLS - start, 1) if start else from_right
    left = pltpu.roll(from_left, (COLS - EDGE - start) % COLS, 1)
    return jnp.where(lanes((ROWS, COLS)) < COLS // 2, right, left)


def pack_levels(plan, with_speed):
    def kernel(own, above, below, from_right, from_left, *rest):
        if with_speed:
            speed, to_down, to_up, speeds = rest
            near = jnp.maximum(from_right[0], from_left[0])
            near = jnp.where(lanes((ROWS, COLS)) < SPARE, 0.0, near)
            top = jnp.maximum(jnp.max(near), jnp.max(speed[...]))
            speeds[...] = jnp.broadcast_to(top, speeds.shape)
        else:
            to_down, to_up = rest
        for index, (a, tile, side) in enumerate(plan.carried):
            for out, k in ((to_down, a), (to_up, LEVELS - 1 - a)):
                if tile:
                    out[index] = TILE_OF[plan]((own, above, below), *tile, k)
                else:
                    out[index] = (from_left if side else from_right)[k]

    return kernel


def place_own(plan, refs, ext):
    own, above, below, from_right, from_left = refs

    def middle(levels, _):
        for k in levels:
            right, left = from_right[k], from_left[k]
            for n, (field, part) in enumerate(plan.tiles):
                ext[n, REACH + k, :, 0:COLS] = TILE_OF[plan]((own, above, below), field, part, k)
                ext[n, REACH + k, :, COLS:WIDE] = halo_columns(right, left, n)
        return 0

    sweep(0, LEVELS, 4, middle)


def place_halo(plan, from_up, from_down, ext, place, last):
    columns = {(a, side): i for i, (a, tile, side) in enumerate(plan.carried) if not tile}
    for message, level, there in (
        (from_down, lambda a: REACH - 1 - a, place > 0),
        (from_up, lambda a: REACH + LEVELS + a, place < last),
    ):
        keep = jnp.where(there, 1.0, 0.0).astype(F32)
        for index, (a, tile, _) in enumerate(plan.carried):
            if not tile:
                continue
            field, part = tile
            value = message[index] * keep
            for kept in "ab" if part == "n" and field in plan.tall else part:
                n = plan.at[field, kept]
                ext[n, level(a), :, 0:COLS] = value
                if (a, 0) in columns:
                    ext[n, level(a), :, COLS:WIDE] = (
                        halo_columns(message[columns[a, 0]], message[columns[a, 1]], n) * keep
                    )


def shift(value, by, axis):
    return pltpu.roll(value, (-by) % value.shape[axis], axis)


def face_flux(q, wind):
    central = 37.0 * (q[2] + q[3]) - 8.0 * (q[1] + q[4]) + (q[0] + q[5])
    upwind = 10.0 * (q[3] - q[2]) - 5.0 * (q[4] - q[1]) + (q[5] - q[0])
    return wind * central - jnp.abs(wind) * upwind


def flat_flux(q, wind, axis):
    flux = face_flux([shift(q, by, axis) if by else q for by in range(-2, 4)], wind)
    return flux - shift(flux, -1, axis)


def rows_flux(q, wind):
    if wind.shape[0] == 24:
        return sixteen(flat_flux(q, wind, 0))
    if q.shape[0] == 24:
        flux = face_flux([sixteen(shift(q, by, 0) if by else q) for by in range(-2, 4)], wind)
        return flux - shift(flux, -1, 0)
    return flat_flux(q, wind, 0)


def level_flux(read, wind, l):
    return face_flux([read(l + by) for by in range(-2, 4)], wind)


def in_domain(l, place, last, lid):
    g = place * LEVELS + l - REACH
    top = (last + 1) * LEVELS - (1 if lid else 0)
    return jnp.where((g >= 0) & (g < top), 1.0, 0.0).astype(F32)


SIXTIETH = -1.0 / 60.0


def sweep(first, count, most, body, carry=0):
    size = max(n for n in range(1, most + 1) if count % n == 0)

    def run(i, carry):
        start = first + i * size
        return body([start + n for n in range(size)], carry)

    return lax.fori_loop(0, count // size, run, carry)


def flat_part(plan, ext, field, l):
    return flat_flux(plan.sixteen(ext, field, l), plan.sixteen(ext, U, l), 1) + rows_flux(
        plan.rows(ext, field, l), plan.rows(ext, V, l)
    )


def flat_own(plan, ext, fields, flat):
    def some(levels, _):
        results = [(n, l, flat_part(plan, ext, f, l)) for l in levels for n, f in enumerate(fields)]
        for n, l, value in results:
            flat[n, l - REACH] = value
        return 0

    sweep(REACH, LEVELS, 4, some)


def rates(plan, ext, fields, write, around_own, most, flat=None):
    reads = [lambda l, f=f: plan.sixteen(ext, f, l) for f in fields]

    def some(levels, lows, flat=None):
        results = []
        for l in levels:
            w = plan.sixteen(ext, W, l)
            highs = []
            for n, f in enumerate(fields):
                high = level_flux(reads[n], w, l)
                level = flat[n, l - REACH] if flat is not None else flat_part(plan, ext, f, l)
                results.append((n, l, (level + (high - lows[n])) * SIXTIETH))
                highs.append(high)
            lows = tuple(highs)
        for result in results:
            write(*result)
        return lows

    first = REACH - around_own
    w = plan.sixteen(ext, W, first - 1)
    lows = tuple(level_flux(read, w, first - 1) for read in reads)
    if flat is None:
        sweep(first, LEVELS + 2 * around_own, most, some, lows)
        return
    lows = sweep(first, around_own, most, some, lows)
    lows = sweep(REACH, LEVELS, 4, lambda levels, c: some(levels, c, flat), lows)
    sweep(REACH + LEVELS, around_own, most, some, lows)


def first_own(place_ref, own, above, below, from_right, from_left, ext, flat):
    place_own(FIRST, (own, above, below, from_right, from_left), ext)

    @pl.when(place_ref[0] == place_ref[1])
    def _():
        for part in "on":
            ext[FIRST.at[W, part], REACH + LEVELS - 1] = jnp.zeros((ROWS, WIDE), F32)

    flat_own(FIRST, ext, (C, PR), flat)


def first_rates(place_ref, ext_in, flat, from_up, from_down, ext, rate):
    place_halo(FIRST, from_up, from_down, ext, place_ref[0], place_ref[1])

    def write(n, l, value):
        rate[n, l] = value

    rates(FIRST, ext, (C, PR), write, 4, 4, flat)


def acoustic(p, u, v, w, read_c, rate, step, first, count, place, last):
    pull = step * sound_speed

    def level(value):
        return sixteen(value) if value.shape[0] == 24 else value

    def wind_w(l, lift_low, lift_high, p_here, p_above):
        lift = (buoyancy * 0.5) * (lift_low + lift_high)
        return (w[0](l) + step * lift - pull * (p_above - p_here)) * in_domain(l, place, last, True)

    def some(levels, w_low):
        talls = [p[0](l) for l in (*levels, levels[-1] + 1)]
        cells = [level(value) for value in talls]
        warm = [read_c(l) for l in (*levels, levels[-1] + 1)]
        results = []
        for n, l in enumerate(levels):
            p_here = cells[n]
            w_new = wind_w(l, warm[n], warm[n + 1], p_here, cells[n + 1])
            u_new = u[0](l) - pull * (shift(p_here, 1, 1) - p_here)
            v_old = v[0](l)
            if v_old.shape[0] == 24:
                v_tall = v_old - pull * (shift(talls[n], 1, 0) - talls[n])
                v_new, v_flow = sixteen(v_tall), sixteen(v_tall - shift(v_tall, -1, 0))
            else:
                v_new = v_old - pull * (shift(p_here, 1, 0) - p_here)
                v_flow = v_new - shift(v_new, -1, 0)
            divergence = (u_new - shift(u_new, -1, 1)) + v_flow + (w_new - w_low)
            p_new = (p_here + step * rate(l) - pull * divergence) * in_domain(
                l, place, last, False
            )
            results.append((l, p_new, u_new, v_new, w_new))
            w_low = w_new
        for l, *news in results:
            for target, value in zip((p, u, v, w), news):
                target[1](l, value)
        return w_low

    low = first - 1
    w_low = wind_w(low, read_c(low), read_c(first), level(p[0](low)), level(p[0](first)))
    w[1](low, w_low)
    sweep(first, count, 12, some, w_low)


def access(ref, *lead):
    def read(l):
        return ref[(*lead, l)]

    def write(l, value):
        ref[(*lead, l)] = value

    return read, write


def begin(start, field, tall=False):
    return lambda l: (FIRST.rows if tall else FIRST.sixteen)(start, field, l)


def own_write(ref, field):
    def write(l, value):
        if not isinstance(l, int):
            ref[field, l - REACH] = value[0:ROWS, 0:COLS]

    return write


def tracer_flat(tiles, u, v, l):
    rows = flat_flux(tiles(l)[:, 0:COLS], v(l)[:, 0:COLS], 0)[0:ROWS]
    return rows + flat_flux(tiles(l)[0:ROWS], u(l)[0:ROWS], 1)[:, 0:COLS]


def tracer_high(tiles, w, l):
    return level_flux(lambda m: tiles(m)[0:ROWS, 0:COLS], w(l)[0:ROWS, 0:COLS], l)


def two_sections(place_ref, speed, other_speed, start, rate0, s2, down, up, dt_out, s1, rate1, fast):
    place, last = place_ref[0], place_ref[1]
    dt = courant_goal / (1.0 + jnp.max(jnp.maximum(speed[...], other_speed[...])))
    dt_out[0] = dt
    third = dt * (1.0 / 3.0)

    def tracer(levels, _):
        for l in levels:
            s1[C, l] = (FIRST.sixteen(start, C, l) + third * rate0[0, l]) * in_domain(
                l, place, last, False
            )
        return 0

    sweep(REACH - 4, LEVELS + 8, 4, tracer)
    acoustic(
        (begin(start, PR, True), access(s1, PR)[1]),
        (begin(start, U), access(s1, U)[1]),
        (begin(start, V, True), access(s1, V)[1]),
        (begin(start, W), access(s1, W)[1]),
        begin(start, C),
        access(rate0, 1)[0],
        third,
        REACH - 4,
        LEVELS + 8,
        place,
        last,
    )
    half = dt * 0.5
    tiles = access(s1, C)[0]
    winds = [access(s1, f)[0] for f in (U, V, W)]

    def own_tracer(levels, low):
        results = []
        for l in levels:
            high = tracer_high(tiles, winds[2], l)
            tendency = (tracer_flat(tiles, *winds[:2], l) + (high - low)) * SIXTIETH
            low = high
            results.append(start[FIRST.at[C, "o"], l, :, 0:COLS] + half * tendency)
        for l, value in zip(levels, results):
            s2[C, l - REACH] = value
        return low

    sweep(REACH, LEVELS, 8, own_tracer, tracer_high(tiles, winds[2], REACH - 1))

    def write(n, l, value):
        rate1[l] = value

    rates(SECTION, s1, (PR,), write, 1, 6)
    step = half / (NS // 2)
    acoustic(
        (begin(start, PR), access(fast, 0)[1]),
        (begin(start, U), access(fast, 1)[1]),
        (begin(start, V), access(fast, 2)[1]),
        (begin(start, W), access(fast, 3)[1]),
        access(s1, C)[0],
        access(rate1)[0],
        step,
        REACH - 1,
        LEVELS + 2,
        place,
        last,
    )
    acoustic(
        (access(fast, 0)[0], own_write(s2, PR)),
        (access(fast, 1)[0], own_write(s2, U)),
        (access(fast, 2)[0], own_write(s2, V)),
        (access(fast, 3)[0], own_write(s2, W)),
        access(s1, C)[0],
        access(rate1)[0],
        step,
        REACH,
        LEVELS,
        place,
        last,
    )

    def share(levels, _):
        made = [shared_rows(lambda f, k=k: s2[f, k]) for k in levels]
        for k, (to_down, to_up) in zip(levels, made):
            for n in range(3):
                down[n, k] = to_down[n]
                up[n, k] = to_up[n]
        return 0

    sweep(0, LEVELS, 4, share)


class Whole:
    def rows(self, ref, field, l):
        return ref[field, l]

    sixteen = rows


SECTION = Whole()


def second_own(own, above, below, from_right, from_left, ext, flat, tracer):
    place_own(SECOND, (own, above, below, from_right, from_left), ext)
    flat_own(SECOND, ext, (PR,), flat)
    tiles, u, v = (lambda l, f=f: SECOND.rows(ext, f, l) for f in (C, U, V))

    def some(levels, _):
        results = [tracer_flat(tiles, u, v, l) for l in levels]
        for l, value in zip(levels, results):
            tracer[l - REACH] = value
        return 0

    sweep(REACH, LEVELS, 4, some)


def last_tracer(
    place_ref, dt_ref, ext_in, flat, flat_tracer, from_up, from_down, initial, *rest
):
    *chunks, ext, tracer, landed, fallen, rate, warm, factor, by_depth, sem = rest
    dt = dt_ref[0]
    copies, first = [], 0
    for n, chunk in enumerate(chunks):
        there = by_depth.at[pl.ds(first, chunk.shape[0])]
        copies.append(pltpu.make_async_copy(chunk, there, sem.at[n]))
        first += chunk.shape[0]
    for copy in copies:
        copy.start()
    place_halo(SECOND, from_up, from_down, ext, place_ref[0], place_ref[1])

    def write(n, l, value):
        rate[l] = value

    rates(SECOND, ext, (PR,), write, 3, 3, flat)

    def keep(levels, _):
        for l in levels:
            warm[l] = SECOND.rows(ext, C, l)
        return 0

    sweep(REACH - 4, LEVELS + 8, 4, keep)
    tiles = lambda l: SECOND.rows(ext, C, l)
    w = lambda l: SECOND.rows(ext, W, l)

    def some(levels, low):
        results = []
        for l in levels:
            high = tracer_high(tiles, w, l)
            tendency = (flat_tracer[l - REACH] + (high - low)) * SIXTIETH
            low = high
            c = initial[C, l - REACH] + dt * tendency
            grown = jnp.exp(growth * c)
            results.append((c, grown, grown * jnp.exp((0.5 * growth) * c)))
        for l, (c, second, third) in zip(levels, results):
            tracer[l - REACH] = c
            factor[0, l - REACH] = second
            factor[1, l - REACH] = third
        return low

    sweep(REACH, LEVELS, 4, some, tracer_high(tiles, w, REACH - 1))
    for copy in copies:
        copy.wait()
    for target in range(-FMAX, LEVELS):
        for moment in range(3):
            total = None
            for depth in range(FMAX + 1):
                k = target + depth
                if 0 <= k < LEVELS:
                    value = by_depth[k, depth, moment]
                    if moment:
                        value = value * factor[moment - 1, k]
                    total = value if total is None else total + value
            if target < 0:
                fallen[moment, target + FMAX] = total
            else:
                landed[moment, target] = total


def last_section(place_ref, dt_ref, rate, warm, start, tracer, out, fast):
    place, last = place_ref[0], place_ref[1]
    step = dt_ref[0] / NS
    out[C] = tracer[...]
    names = (PR, U, V, W)
    for repeat in range(NS):
        reads = [
            begin(start, f) if repeat == 0 else access(fast, n)[0] for n, f in enumerate(names)
        ]
        writes = [
            own_write(out, f) if repeat == NS - 1 else access(fast, n)[1]
            for n, f in enumerate(names)
        ]
        acoustic(
            *zip(reads, writes),
            access(warm)[0],
            access(rate)[0],
            step,
            REACH - 3 + repeat,
            LEVELS + 6 - 2 * repeat,
            place,
            last,
        )


def land(place_ref, landed, arrived, out):
    keep = jnp.where(place_ref[0] < place_ref[1], 1.0, 0.0).astype(F32)
    out[:, 0 : LEVELS - FMAX] = landed[:, 0 : LEVELS - FMAX]
    out[:, LEVELS - FMAX :] = landed[:, LEVELS - FMAX :] + keep * arrived[...]


def deposit(radius, weight, column, counts, fall_depth, out):
    slots, levels = radius.shape[0], radius.shape[1]
    target = lax.broadcasted_iota(jnp.int32, (COLS, COLS), 0)
    row = lax.broadcasted_iota(jnp.int32, (ROWS, COLS), 0)
    per_step = 4

    for k in range(levels):
        out[k] = jnp.zeros(out.shape[1:], F32)
        live = counts[k]

        def some(step, _, k=k, live=live):
            sums = [[None] * 3 for _ in range(FMAX + 1)]
            for part in range(per_step):
                s = step * per_step + part
                r = radius[s, k]
                number = jnp.where(s < live, weight[s, k], 0.0)
                area = number * r * r
                terms = []
                for t in (number, area, area * r):
                    high = t.astype(jnp.bfloat16).astype(F32)
                    terms += [high, t - high]
                cols = column[s, k]
                left, right = [], []
                for j in range(ROWS):
                    left.append(
                        jnp.concatenate([jnp.where(row == j, t, 0.0) for t in terms], axis=0)
                    )
                    right.append(jnp.where(cols[j : j + 1] == target, 1.0, 0.0).astype(F32))
                sent = lax.dot_general(
                    jnp.concatenate(left, axis=1),
                    jnp.concatenate(right, axis=1),
                    (((1,), (1,)), ((), ())),
                    preferred_element_type=F32,
                )
                depth = jnp.broadcast_to(fall_depth[s, k], (ROWS, COLS))
                for d in range(FMAX + 1):
                    falls = depth == d
                    for m in range(3):
                        both = sent[16 * m : 16 * m + 8] + sent[16 * m + 8 : 16 * m + 16]
                        value = jnp.where(falls, both, 0.0)
                        sums[d][m] = value if sums[d][m] is None else sums[d][m] + value
            for d in range(FMAX + 1):
                for m in range(3):
                    out[k, d, m] += sums[d][m]
            return 0

        lax.fori_loop(0, slots // per_step, some, 0)


def vmem(n):
    return [pl.BlockSpec(memory_space=pltpu.VMEM)] * n


def smem(n):
    return [pl.BlockSpec(memory_space=pltpu.SMEM)] * n


def far(n):
    return [pl.BlockSpec(memory_space=pltpu.HBM)] * n


def shaped(*dims):
    return jax.ShapeDtypeStruct(dims, F32)


def held(*dims):
    return pltpu.VMEM(dims, F32)


def call(kernel, name, ins, outs, scratch=(), out_specs=None, flops=None, grant=4, alias=None):
    made = pl.pallas_call(
        kernel,
        name=name,
        in_specs=ins,
        out_specs=tuple(out_specs or vmem(len(outs))),
        out_shape=tuple(outs),
        scratch_shapes=list(scratch),
        input_output_aliases=alias or {},
        compiler_params=pltpu.CompilerParams(vmem_limit_bytes=grant << 20),
        cost_estimate=(
            pl.CostEstimate(flops=flops, bytes_accessed=0, transcendentals=0) if flops else None
        ),
    )

    def run(*operands):
        return made(
            *(
                pltpu.with_memory_space_constraint(value, spec.memory_space)
                if spec.memory_space != pltpu.SMEM
                else value
                for spec, value in zip(ins, operands)
            )
        )

    return run


def both_ways(down, axis, up):
    count = lax.axis_size(axis)
    return (
        lax.ppermute(down, axis, [((i + 1) % count, i) for i in range(count)]),
        lax.ppermute(up, axis, [(i, (i + 1) % count) for i in range(count)]),
    )


def exchange(plan, own, down, up, tokens=(), speed=None):
    above, below = both_ways(down, GY, up)
    extra = [] if speed is None else [speed]
    to_left, to_right = call(
        pack_columns(plan, bool(extra)),
        "pack_columns",
        vmem(3 + len(extra)) + far(len(tokens)),
        [held(LEVELS, ROWS, COLS)] * 2,
    )(own, above, below, *extra, *tokens)
    from_right, from_left = both_ways(to_left, "gx", to_right)
    tiles = len(plan.carried)
    to_down, to_up, *speeds = call(
        pack_levels(plan, bool(extra)),
        "pack_levels",
        vmem(5 + len(extra)),
        [held(tiles, ROWS, COLS)] * 2 + [held(ROWS, COLS)] * len(extra),
    )(own, above, below, from_right, from_left, *extra)
    from_up, from_down = both_ways(to_down, "gz", to_up)
    return above, below, from_right, from_left, from_up, from_down, to_down, *speeds


def prepare(place_ref, fields, own, speed):
    own[...] = fields[...]
    keep = jnp.where(place_ref[0] == place_ref[1], 0.0, 1.0).astype(F32)
    most = jnp.zeros((ROWS, COLS), F32)
    for k in range(LEVELS):
        w = jnp.abs(fields[W, k])
        if k == LEVELS - 1:
            w = w * keep
        most = jnp.maximum(most, jnp.abs(fields[U, k]) + jnp.abs(fields[V, k]) + w)
    speed[...] = jnp.broadcast_to(jnp.max(most), speed.shape)


def droplets(radius, weight, column, counts, fall_depth, first, count, after):
    slots, step = radius.shape[0], 2
    counts, _ = lax.optimization_barrier((counts, after))
    whole = pl.BlockSpec((slots, step, ROWS, COLS), lambda i: (0, first // step + i, 0, 0))
    return pl.pallas_call(
        deposit,
        name="deposit",
        grid=(count // step,),
        in_specs=[
            whole,
            whole,
            whole,
            pl.BlockSpec((step, ROWS, COLS), lambda i: (first // step + i, 0, 0)),
            pl.BlockSpec((slots, step, ROWS, 1), lambda i: (0, first // step + i, 0, 0)),
        ],
        out_specs=pl.BlockSpec((step, FMAX + 1, 3, ROWS, COLS), lambda i: (i, 0, 0, 0, 0)),
        out_shape=pltpu.HBM((count, FMAX + 1, 3, ROWS, COLS), F32),
        compiler_params=pltpu.CompilerParams(vmem_limit_bytes=12 << 20),
        cost_estimate=pl.CostEstimate(
            flops=100_000_000 * count, bytes_accessed=0, transcendentals=0
        ),
    )(
        *(
            pltpu.with_memory_space_constraint(value, pltpu.HBM)
            for value in (radius, weight, column, counts)
        ),
        fall_depth,
    )


def per_device(fields, radius, weight, column, counts, fall_depth):
    place = lax.axis_index("gz")
    last = lax.axis_size("gz") - 1
    where = jnp.stack([place, jnp.int32(last)]).astype(jnp.int32)
    def drops(first, count, after):
        return droplets(radius, weight, column, counts, fall_depth, first, count, after)

    own, speed = pl.pallas_call(
        prepare,
        name="prepare",
        in_specs=smem(1) + vmem(1),
        out_specs=tuple(vmem(2)),
        out_shape=(held(5, LEVELS, ROWS, COLS), shaped(ROWS, COLS)),
        compiler_params=pltpu.CompilerParams(vmem_limit_bytes=4 << 20),
    )(where, fields)
    pair = [(i, i ^ 1) for i in range(lax.axis_size("gx"))]
    speed = jnp.maximum(speed, lax.ppermute(speed, "gx", pair))
    plane = ("gy_hi", "gz")
    early = drops(0, 6, speed)
    speed = jnp.broadcast_to(speed[0:1], (lax.axis_size(plane), 1, COLS))
    speed = jnp.max(lax.all_to_all(speed, plane, 0, 0), axis=0)
    *near, from_up, from_down, _, speed = exchange(FIRST, own, fields, fields, [early], speed)
    other_speed = lax.ppermute(speed, "gy_lo", [(0, 1), (1, 0)])
    ext = held(len(FIRST.tiles), DEPTH, ROWS, WIDE)
    start, flat = call(
        first_own,
        "first_own",
        smem(1) + vmem(5),
        [ext, held(2, LEVELS, 2 * ROWS, WIDE)],
    )(where, own, *near)
    start, rate0 = call(
        first_rates,
        "first_rates",
        smem(1) + vmem(4),
        [ext, held(2, DEPTH, 2 * ROWS, WIDE)],
        alias={1: 0},
    )(where, start, flat, from_up, from_down)
    s2, down, up, dt = call(
        two_sections,
        "two_sections",
        smem(1) + vmem(4),
        [held(5, LEVELS, ROWS, COLS)] + [held(3, LEVELS, ROWS, COLS)] * 2 + [shaped(1)],
        scratch=[
            pltpu.VMEM((5, DEPTH, 2 * ROWS, WIDE), F32),
            pltpu.VMEM((DEPTH, 2 * ROWS, WIDE), F32),
            pltpu.VMEM((4, DEPTH, 2 * ROWS, WIDE), F32),
        ],
        out_specs=vmem(3) + smem(1),
        grant=10,
    )(where, speed, other_speed, start, rate0)
    middle = drops(6, 8, s2)
    *near, from_up, from_down, sent = exchange(SECOND, s2, down, up, [middle])
    by_depth = [early, middle, drops(14, 2, sent)]
    ext = held(len(SECOND.tiles), DEPTH, ROWS, WIDE)
    around_s2, flat, flat_tracer = call(
        second_own,
        "second_own",
        vmem(5),
        [ext, held(1, LEVELS, 2 * ROWS, WIDE), held(LEVELS, ROWS, COLS)],
        flops=1_000_000_000,
    )(s2, *near)
    rows = held(DEPTH, 2 * ROWS, WIDE)
    _, tracer, landed, fallen, rate, warm = call(
        last_tracer,
        "last_tracer",
        smem(2) + vmem(6) + far(len(by_depth)),
        [
            ext,
            held(LEVELS, ROWS, COLS),
            held(3, LEVELS, ROWS, COLS),
            held(3, FMAX, ROWS, COLS),
            rows,
            rows,
        ],
        scratch=[
            pltpu.VMEM((2, LEVELS, ROWS, COLS), F32),
            pltpu.VMEM((LEVELS, FMAX + 1, 3, ROWS, COLS), F32),
            pltpu.SemaphoreType.DMA((len(by_depth),)),
        ],
        alias={2: 0},
    )(where, dt, around_s2, flat, flat_tracer, from_up, from_down, own, *by_depth)
    count = lax.axis_size("gz")
    arrived = lax.ppermute(fallen, "gz", [((i + 1) % count, i) for i in range(count)])
    (new_fields,) = call(
        last_section,
        "last_section",
        smem(2) + vmem(4),
        [shaped(5, LEVELS, ROWS, COLS)],
        scratch=[pltpu.VMEM((4, DEPTH, 2 * ROWS, WIDE), F32)],
        flops=1_000_000_000,
    )(where, dt, rate, warm, start, tracer)
    (moments,) = call(
        land, "land", smem(1) + vmem(2), [shaped(3, LEVELS, ROWS, COLS)]
    )(where, landed, arrived)
    return (new_fields, moments)


def solution(mesh):
    count = mesh.shape["gy"]
    split = Mesh(
        mesh.devices.reshape(mesh.shape["gx"], count // 2, 2, mesh.shape["gz"]),
        ("gx", *GY, "gz"),
    )
    spread = P(None, "gz", GY, "gx")
    return jax.shard_map(
        per_device,
        mesh=split,
        in_specs=(spread, spread, spread, spread, P("gz", GY, "gx"), spread),
        out_specs=(spread, spread),
        check_vma=False,
    )
```

```python
import jax
import jax.numpy as jnp
from jax import lax
from jax.experimental import pallas as pl
from jax.experimental.pallas import tpu as pltpu
from jax.sharding import Mesh
from jax.sharding import PartitionSpec as P

NS = 4
FMAX = 8
GY = ("gy_hi", "gy_lo")

sound_speed = 10.0
buoyancy = 0.5
courant_goal = 0.6
growth = 0.3

LEVELS, ROWS, COLS = 16, 8, 128
WIDE = 2 * COLS
REACH = 7
DEPTH = LEVELS + 2 * REACH
EDGE = 8
F32 = jnp.float32
C, PR, U, V, W = range(5)


class Plan:
    def __init__(self, tall, reach, sent):
        self.tall, self.reach = tall, reach
        self.tiles = [
            (field, part)
            for field in range(5)
            for part in ("oab" if field in tall else "on")
        ]
        self.at = {tile: n for n, tile in enumerate(self.tiles)}
        self.carried = []
        for a in range(reach):
            for field in range(5):
                for part in sent[field][a] if a < len(sent[field]) else "":
                    self.carried.append((a, (field, part), 0))
            if a < reach - 1:
                self.carried += [(a, None, 0), (a, None, 1)]

    def rows(self, ref, field, l):
        return jnp.concatenate(
            [
                ref[self.at[field, part], l]
                for part in ("oab" if field in self.tall else "on")
            ],
            axis=0,
        )

    def sixteen(self, ref, field, l):
        value = self.rows(ref, field, l)
        return sixteen(value) if field in self.tall else value


def lanes(shape):
    return lax.broadcasted_iota(jnp.int32, shape, len(shape) - 1)


def lower_rows(shape):
    return lax.broadcasted_iota(jnp.int32, shape, 0) < ROWS // 2


def around(above, below):
    return jnp.where(lower_rows(above.shape), above, below)


def sixteen(value):
    return jnp.concatenate(
        [value[0:ROWS], around(value[ROWS : 2 * ROWS], value[2 * ROWS :])], axis=0
    )


def raw_tile(refs, field, part, k):
    own, above, below = refs
    if part == "o":
        return own[field, k]
    if part == "n":
        return around(above[field, k], below[field, k])
    return (above if part == "a" else below)[field, k]


SHARED = {C: (1, 0), U: (1, 1), V: (2, 0), W: (2, 1)}


def shared_rows(read):
    down, up = [read(PR)], [read(PR)]
    for first, second in ((C, U), (V, W)):
        one, other = read(first), pltpu.roll(read(second), ROWS // 2, 0)
        down.append(around(one, other))
        up.append(around(other, one))
    return down, up


def shared_tile(refs, field, part, k):
    own, above, below = refs
    if part == "o":
        return own[field, k]
    if part == "n" and field == PR:
        return around(above[0, k], below[0, k])
    if part == "n":
        index, half = SHARED[field]
        if half == 0:
            return around(above[index, k], below[index, k])
        return pltpu.roll(around(below[index, k], above[index, k]), ROWS // 2, 0)
    return (above if part == "a" else below)[0, k]


THREE, TWO, ONE = "oab", "on", "o"
FIRST = Plan(
    (C, PR, V),
    7,
    {
        C: [THREE] + [TWO] * 4 + [ONE],
        PR: [THREE] * 2 + [TWO] * 4 + [ONE],
        U: [TWO] * 3 + [ONE],
        V: [TWO] * 4,
        W: [TWO] * 3 + [ONE] * 2,
    },
)
SECOND = Plan(
    (PR,),
    6,
    {
        C: [TWO] * 3 + [ONE],
        PR: [THREE] + [TWO] * 4 + [ONE],
        U: [TWO] * 3,
        V: [TWO] * 3,
        W: [TWO] * 3 + [ONE],
    },
)
TILE_OF = {FIRST: raw_tile, SECOND: shared_tile}


SPARE = 104


def pack_columns(plan, with_speed):
    def kernel(own, above, below, *rest):
        to_left, to_right = rest[-2:]
        lane = lanes((ROWS, COLS))
        filler = jnp.zeros((ROWS, COLS), F32)
        if with_speed:
            filler = filler + jnp.max(rest[0][...])

        def one(k, _):
            left = filler
            right = filler
            for n, (field, part) in enumerate(plan.tiles):
                start = n * EDGE
                here = (lane >= start) & (lane < start + EDGE)
                value = TILE_OF[plan]((own, above, below), field, part, k)
                first = pltpu.roll(value, start, 1) if start else value
                last = pltpu.roll(value, (start + EDGE) % COLS, 1)
                left = jnp.where(here, first, left)
                right = jnp.where(here, last, right)
            to_left[k] = left
            to_right[k] = right
            return 0

        def some(levels, _):
            for k in levels:
                one(k, 0)
            return 0

        sweep(0, LEVELS, 8, some)

    return kernel


def halo_columns(from_right, from_left, n):
    start = n * EDGE
    right = pltpu.roll(from_right, COLS - start, 1) if start else from_right
    left = pltpu.roll(from_left, (COLS - EDGE - start) % COLS, 1)
    return jnp.where(lanes((ROWS, COLS)) < COLS // 2, right, left)


def pack_levels(plan, with_speed):
    def kernel(own, above, below, from_right, from_left, *rest):
        if with_speed:
            speed, to_down, to_up, speeds = rest
            near = jnp.maximum(from_right[0], from_left[0])
            near = jnp.where(lanes((ROWS, COLS)) < SPARE, 0.0, near)
            top = jnp.maximum(jnp.max(near), jnp.max(speed[...]))
            speeds[...] = jnp.broadcast_to(top, speeds.shape)
        else:
            to_down, to_up = rest
        for index, (a, tile, side) in enumerate(plan.carried):
            for out, k in ((to_down, a), (to_up, LEVELS - 1 - a)):
                if tile:
                    out[index] = TILE_OF[plan]((own, above, below), *tile, k)
                else:
                    out[index] = (from_left if side else from_right)[k]

    return kernel


def place_own(plan, refs, ext):
    own, above, below, from_right, from_left = refs

    def middle(levels, _):
        for k in levels:
            right, left = from_right[k], from_left[k]
            for n, (field, part) in enumerate(plan.tiles):
                ext[n, REACH + k, :, 0:COLS] = TILE_OF[plan]((own, above, below), field, part, k)
                ext[n, REACH + k, :, COLS:WIDE] = halo_columns(right, left, n)
        return 0

    sweep(0, LEVELS, 4, middle)


def place_halo(plan, from_up, from_down, ext, place, last):
    columns = {(a, side): i for i, (a, tile, side) in enumerate(plan.carried) if not tile}
    for message, level, there in (
        (from_down, lambda a: REACH - 1 - a, place > 0),
        (from_up, lambda a: REACH + LEVELS + a, place < last),
    ):
        keep = jnp.where(there, 1.0, 0.0).astype(F32)
        for index, (a, tile, _) in enumerate(plan.carried):
            if not tile:
                continue
            field, part = tile
            value = message[index] * keep
            for kept in "ab" if part == "n" and field in plan.tall else part:
                n = plan.at[field, kept]
                ext[n, level(a), :, 0:COLS] = value
                if (a, 0) in columns:
                    ext[n, level(a), :, COLS:WIDE] = (
                        halo_columns(message[columns[a, 0]], message[columns[a, 1]], n) * keep
                    )


def shift(value, by, axis):
    return pltpu.roll(value, (-by) % value.shape[axis], axis)


def face_flux(q, wind):
    central = 37.0 * (q[2] + q[3]) - 8.0 * (q[1] + q[4]) + (q[0] + q[5])
    upwind = 10.0 * (q[3] - q[2]) - 5.0 * (q[4] - q[1]) + (q[5] - q[0])
    return wind * central - jnp.abs(wind) * upwind


def flat_flux(q, wind, axis):
    flux = face_flux([shift(q, by, axis) if by else q for by in range(-2, 4)], wind)
    return flux - shift(flux, -1, axis)


def rows_flux(q, wind):
    if wind.shape[0] == 24:
        return sixteen(flat_flux(q, wind, 0))
    if q.shape[0] == 24:
        flux = face_flux([sixteen(shift(q, by, 0) if by else q) for by in range(-2, 4)], wind)
        return flux - shift(flux, -1, 0)
    return flat_flux(q, wind, 0)


def level_flux(read, wind, l):
    return face_flux([read(l + by) for by in range(-2, 4)], wind)


def in_domain(l, place, last, lid):
    g = place * LEVELS + l - REACH
    top = (last + 1) * LEVELS - (1 if lid else 0)
    return jnp.where((g >= 0) & (g < top), 1.0, 0.0).astype(F32)


SIXTIETH = -1.0 / 60.0


def sweep(first, count, most, body, carry=0):
    size = max(n for n in range(1, most + 1) if count % n == 0)

    def run(i, carry):
        start = first + i * size
        return body([start + n for n in range(size)], carry)

    return lax.fori_loop(0, count // size, run, carry)


def flat_part(plan, ext, field, l):
    return flat_flux(plan.sixteen(ext, field, l), plan.sixteen(ext, U, l), 1) + rows_flux(
        plan.rows(ext, field, l), plan.rows(ext, V, l)
    )


def flat_own(plan, ext, fields, flat):
    def some(levels, _):
        results = [(n, l, flat_part(plan, ext, f, l)) for l in levels for n, f in enumerate(fields)]
        for n, l, value in results:
            flat[n, l - REACH] = value
        return 0

    sweep(REACH, LEVELS, 4, some)


def rates(plan, ext, fields, write, around_own, most, flat=None):
    reads = [lambda l, f=f: plan.sixteen(ext, f, l) for f in fields]

    def some(levels, lows, flat=None):
        results = []
        for l in levels:
            w = plan.sixteen(ext, W, l)
            highs = []
            for n, f in enumerate(fields):
                high = level_flux(reads[n], w, l)
                level = flat[n, l - REACH] if flat is not None else flat_part(plan, ext, f, l)
                results.append((n, l, (level + (high - lows[n])) * SIXTIETH))
                highs.append(high)
            lows = tuple(highs)
        for result in results:
            write(*result)
        return lows

    first = REACH - around_own
    w = plan.sixteen(ext, W, first - 1)
    lows = tuple(level_flux(read, w, first - 1) for read in reads)
    if flat is None:
        sweep(first, LEVELS + 2 * around_own, most, some, lows)
        return
    lows = sweep(first, around_own, most, some, lows)
    lows = sweep(REACH, LEVELS, 4, lambda levels, c: some(levels, c, flat), lows)
    sweep(REACH + LEVELS, around_own, most, some, lows)


def first_own(place_ref, own, above, below, from_right, from_left, ext, flat):
    place_own(FIRST, (own, above, below, from_right, from_left), ext)

    @pl.when(place_ref[0] == place_ref[1])
    def _():
        for part in "on":
            ext[FIRST.at[W, part], REACH + LEVELS - 1] = jnp.zeros((ROWS, WIDE), F32)

    flat_own(FIRST, ext, (C, PR), flat)


def acoustic(p, u, v, w, read_c, rate, step, first, count, place, last):
    pull = step * sound_speed

    def level(value):
        return sixteen(value) if value.shape[0] == 24 else value

    def wind_w(l, lift_low, lift_high, p_here, p_above):
        lift = (buoyancy * 0.5) * (lift_low + lift_high)
        return (w[0](l) + step * lift - pull * (p_above - p_here)) * in_domain(l, place, last, True)

    def some(levels, w_low):
        talls = [p[0](l) for l in (*levels, levels[-1] + 1)]
        cells = [level(value) for value in talls]
        warm = [read_c(l) for l in (*levels, levels[-1] + 1)]
        results = []
        for n, l in enumerate(levels):
            p_here = cells[n]
            w_new = wind_w(l, warm[n], warm[n + 1], p_here, cells[n + 1])
            u_new = u[0](l) - pull * (shift(p_here, 1, 1) - p_here)
            v_old = v[0](l)
            if v_old.shape[0] == 24:
                v_tall = v_old - pull * (shift(talls[n], 1, 0) - talls[n])
                v_new, v_flow = sixteen(v_tall), sixteen(v_tall - shift(v_tall, -1, 0))
            else:
                v_new = v_old - pull * (shift(p_here, 1, 0) - p_here)
                v_flow = v_new - shift(v_new, -1, 0)
            divergence = (u_new - shift(u_new, -1, 1)) + v_flow + (w_new - w_low)
            p_new = (p_here + step * rate(l) - pull * divergence) * in_domain(
                l, place, last, False
            )
            results.append((l, p_new, u_new, v_new, w_new))
            w_low = w_new
        for l, *news in results:
            for target, value in zip((p, u, v, w), news):
                target[1](l, value)
        return w_low

    low = first - 1
    w_low = wind_w(low, read_c(low), read_c(first), level(p[0](low)), level(p[0](first)))
    w[1](low, w_low)
    sweep(first, count, 12, some, w_low)


def access(ref, *lead):
    def read(l):
        return ref[(*lead, l)]

    def write(l, value):
        ref[(*lead, l)] = value

    return read, write


def begin(start, field, tall=False):
    return lambda l: (FIRST.rows if tall else FIRST.sixteen)(start, field, l)


def own_write(ref, field):
    def write(l, value):
        if not isinstance(l, int):
            ref[field, l - REACH] = value[0:ROWS, 0:COLS]

    return write


def tracer_flat(tiles, u, v, l):
    rows = flat_flux(tiles(l)[:, 0:COLS], v(l)[:, 0:COLS], 0)[0:ROWS]
    return rows + flat_flux(tiles(l)[0:ROWS], u(l)[0:ROWS], 1)[:, 0:COLS]


def tracer_high(tiles, w, l):
    return level_flux(lambda m: tiles(m)[0:ROWS, 0:COLS], w(l)[0:ROWS, 0:COLS], l)


def two_sections(
    place_ref, speed, other_speed, start_in, flat, from_up, from_down, *rest
):
    start, s2, down, up, dt_out, rate0, s1, rate1, fast = rest[-9:]
    place, last = place_ref[0], place_ref[1]
    place_halo(FIRST, from_up, from_down, start, place, last)

    def write0(n, l, value):
        rate0[n, l] = value

    rates(FIRST, start, (C, PR), write0, 4, 4, flat)
    dt = courant_goal / (1.0 + jnp.max(jnp.maximum(speed[...], other_speed[...])))
    dt_out[0] = dt
    third = dt * (1.0 / 3.0)

    def tracer(levels, _):
        for l in levels:
            s1[C, l] = (FIRST.sixteen(start, C, l) + third * rate0[0, l]) * in_domain(
                l, place, last, False
            )
        return 0

    sweep(REACH - 4, LEVELS + 8, 4, tracer)
    acoustic(
        (begin(start, PR, True), access(s1, PR)[1]),
        (begin(start, U), access(s1, U)[1]),
        (begin(start, V, True), access(s1, V)[1]),
        (begin(start, W), access(s1, W)[1]),
        begin(start, C),
        access(rate0, 1)[0],
        third,
        REACH - 4,
        LEVELS + 8,
        place,
        last,
    )
    half = dt * 0.5
    tiles = access(s1, C)[0]
    winds = [access(s1, f)[0] for f in (U, V, W)]

    def own_tracer(levels, low):
        results = []
        for l in levels:
            high = tracer_high(tiles, winds[2], l)
            tendency = (tracer_flat(tiles, *winds[:2], l) + (high - low)) * SIXTIETH
            low = high
            results.append(start[FIRST.at[C, "o"], l, :, 0:COLS] + half * tendency)
        for l, value in zip(levels, results):
            s2[C, l - REACH] = value
        return low

    sweep(REACH, LEVELS, 8, own_tracer, tracer_high(tiles, winds[2], REACH - 1))

    def write(n, l, value):
        rate1[l] = value

    rates(SECTION, s1, (PR,), write, 1, 6)
    step = half / (NS // 2)
    acoustic(
        (begin(start, PR), access(fast, 0)[1]),
        (begin(start, U), access(fast, 1)[1]),
        (begin(start, V), access(fast, 2)[1]),
        (begin(start, W), access(fast, 3)[1]),
        access(s1, C)[0],
        access(rate1)[0],
        step,
        REACH - 1,
        LEVELS + 2,
        place,
        last,
    )
    acoustic(
        (access(fast, 0)[0], own_write(s2, PR)),
        (access(fast, 1)[0], own_write(s2, U)),
        (access(fast, 2)[0], own_write(s2, V)),
        (access(fast, 3)[0], own_write(s2, W)),
        access(s1, C)[0],
        access(rate1)[0],
        step,
        REACH,
        LEVELS,
        place,
        last,
    )

    def share(levels, _):
        made = [shared_rows(lambda f, k=k: s2[f, k]) for k in levels]
        for k, (to_down, to_up) in zip(levels, made):
            for n in range(3):
                down[n, k] = to_down[n]
                up[n, k] = to_up[n]
        return 0

    sweep(0, LEVELS, 4, share)


class Whole:
    def rows(self, ref, field, l):
        return ref[field, l]

    sixteen = rows


SECTION = Whole()


def second_own(own, above, below, from_right, from_left, ext, flat, tracer):
    place_own(SECOND, (own, above, below, from_right, from_left), ext)
    flat_own(SECOND, ext, (PR,), flat)
    tiles, u, v = (lambda l, f=f: SECOND.rows(ext, f, l) for f in (C, U, V))

    def some(levels, _):
        results = [tracer_flat(tiles, u, v, l) for l in levels]
        for l, value in zip(levels, results):
            tracer[l - REACH] = value
        return 0

    sweep(REACH, LEVELS, 4, some)


def last_tracer(
    place_ref, dt_ref, ext_in, flat, flat_tracer, from_up, from_down, initial, *rest
):
    *chunks, ext, tracer, landed, fallen, rate, warm, factor, by_depth, sem = rest
    dt = dt_ref[0]
    copies, first = [], 0
    for n, chunk in enumerate(chunks):
        there = by_depth.at[pl.ds(first, chunk.shape[0])]
        copies.append(pltpu.make_async_copy(chunk, there, sem.at[n]))
        first += chunk.shape[0]
    for copy in copies:
        copy.start()
    place_halo(SECOND, from_up, from_down, ext, place_ref[0], place_ref[1])

    def write(n, l, value):
        rate[l] = value

    rates(SECOND, ext, (PR,), write, 3, 3, flat)

    def keep(levels, _):
        for l in levels:
            warm[l] = SECOND.rows(ext, C, l)
        return 0

    sweep(REACH - 4, LEVELS + 8, 4, keep)
    tiles = lambda l: SECOND.rows(ext, C, l)
    w = lambda l: SECOND.rows(ext, W, l)

    def some(levels, low):
        results = []
        for l in levels:
            high = tracer_high(tiles, w, l)
            tendency = (flat_tracer[l - REACH] + (high - low)) * SIXTIETH
            low = high
            c = initial[C, l - REACH] + dt * tendency
            grown = jnp.exp(growth * c)
            results.append((c, grown, grown * jnp.exp((0.5 * growth) * c)))
        for l, (c, second, third) in zip(levels, results):
            tracer[l - REACH] = c
            factor[0, l - REACH] = second
            factor[1, l - REACH] = third
        return low

    sweep(REACH, LEVELS, 4, some, tracer_high(tiles, w, REACH - 1))
    for copy in copies:
        copy.wait()
    for target in range(-FMAX, LEVELS):
        for moment in range(3):
            total = None
            for depth in range(FMAX + 1):
                k = target + depth
                if 0 <= k < LEVELS:
                    value = by_depth[k, depth, moment]
                    if moment:
                        value = value * factor[moment - 1, k]
                    total = value if total is None else total + value
            if target < 0:
                fallen[moment, target + FMAX] = total
            else:
                landed[moment, target] = total


def last_section(place_ref, dt_ref, rate, warm, start, tracer, out, fast):
    place, last = place_ref[0], place_ref[1]
    step = dt_ref[0] / NS
    out[C] = tracer[...]
    names = (PR, U, V, W)
    for repeat in range(NS):
        reads = [
            begin(start, f) if repeat == 0 else access(fast, n)[0] for n, f in enumerate(names)
        ]
        writes = [
            own_write(out, f) if repeat == NS - 1 else access(fast, n)[1]
            for n, f in enumerate(names)
        ]
        acoustic(
            *zip(reads, writes),
            access(warm)[0],
            access(rate)[0],
            step,
            REACH - 3 + repeat,
            LEVELS + 6 - 2 * repeat,
            place,
            last,
        )


def land(place_ref, landed, arrived, out):
    keep = jnp.where(place_ref[0] < place_ref[1], 1.0, 0.0).astype(F32)
    out[:, 0 : LEVELS - FMAX] = landed[:, 0 : LEVELS - FMAX]
    out[:, LEVELS - FMAX :] = landed[:, LEVELS - FMAX :] + keep * arrived[...]


def deposit(radius, weight, column, counts, fall_depth, out):
    slots, levels = radius.shape[0], radius.shape[1]
    target = lax.broadcasted_iota(jnp.int32, (COLS, COLS), 0)
    row = lax.broadcasted_iota(jnp.int32, (ROWS, COLS), 0)
    per_step = 4

    for k in range(levels):
        out[k] = jnp.zeros(out.shape[1:], F32)
        live = counts[k]

        def some(step, _, k=k, live=live):
            sums = [[None] * 3 for _ in range(FMAX + 1)]
            for part in range(per_step):
                s = step * per_step + part
                r = radius[s, k]
                number = jnp.where(s < live, weight[s, k], 0.0)
                area = number * r * r
                terms = []
                for t in (number, area, area * r):
                    high = t.astype(jnp.bfloat16).astype(F32)
                    terms += [high, t - high]
                cols = column[s, k]
                left, right = [], []
                for j in range(ROWS):
                    left.append(
                        jnp.concatenate([jnp.where(row == j, t, 0.0) for t in terms], axis=0)
                    )
                    right.append(jnp.where(cols[j : j + 1] == target, 1.0, 0.0).astype(F32))
                sent = lax.dot_general(
                    jnp.concatenate(left, axis=1),
                    jnp.concatenate(right, axis=1),
                    (((1,), (1,)), ((), ())),
                    preferred_element_type=F32,
                )
                depth = jnp.broadcast_to(fall_depth[s, k], (ROWS, COLS))
                for d in range(FMAX + 1):
                    falls = depth == d
                    for m in range(3):
                        both = sent[16 * m : 16 * m + 8] + sent[16 * m + 8 : 16 * m + 16]
                        value = jnp.where(falls, both, 0.0)
                        sums[d][m] = value if sums[d][m] is None else sums[d][m] + value
            for d in range(FMAX + 1):
                for m in range(3):
                    out[k, d, m] += sums[d][m]
            return 0

        lax.fori_loop(0, slots // per_step, some, 0)


def vmem(n):
    return [pl.BlockSpec(memory_space=pltpu.VMEM)] * n


def smem(n):
    return [pl.BlockSpec(memory_space=pltpu.SMEM)] * n


def far(n):
    return [pl.BlockSpec(memory_space=pltpu.HBM)] * n


def shaped(*dims):
    return jax.ShapeDtypeStruct(dims, F32)


def held(*dims):
    return pltpu.VMEM(dims, F32)


def call(kernel, name, ins, outs, scratch=(), out_specs=None, flops=None, grant=4, alias=None):
    made = pl.pallas_call(
        kernel,
        name=name,
        in_specs=ins,
        out_specs=tuple(out_specs or vmem(len(outs))),
        out_shape=tuple(outs),
        scratch_shapes=list(scratch),
        input_output_aliases=alias or {},
        compiler_params=pltpu.CompilerParams(vmem_limit_bytes=grant << 20),
        cost_estimate=(
            pl.CostEstimate(flops=flops, bytes_accessed=0, transcendentals=0) if flops else None
        ),
    )

    def run(*operands):
        return made(
            *(
                pltpu.with_memory_space_constraint(value, spec.memory_space)
                if spec.memory_space != pltpu.SMEM
                else value
                for spec, value in zip(ins, operands)
            )
        )

    return run


def both_ways(down, axis, up):
    count = lax.axis_size(axis)
    return (
        lax.ppermute(down, axis, [((i + 1) % count, i) for i in range(count)]),
        lax.ppermute(up, axis, [(i, (i + 1) % count) for i in range(count)]),
    )


def exchange(plan, own, down, up, tokens=(), speed=None):
    above, below = both_ways(down, GY, up)
    extra = [] if speed is None else [speed]
    to_left, to_right = call(
        pack_columns(plan, bool(extra)),
        "pack_columns",
        vmem(3 + len(extra)) + far(len(tokens)),
        [held(LEVELS, ROWS, COLS)] * 2,
    )(own, above, below, *extra, *tokens)
    from_right, from_left = both_ways(to_left, "gx", to_right)
    tiles = len(plan.carried)
    to_down, to_up, *speeds = call(
        pack_levels(plan, bool(extra)),
        "pack_levels",
        vmem(5 + len(extra)),
        [held(tiles, ROWS, COLS)] * 2 + [held(ROWS, COLS)] * len(extra),
    )(own, above, below, from_right, from_left, *extra)
    from_up, from_down = both_ways(to_down, "gz", to_up)
    return above, below, from_right, from_left, from_up, from_down, to_down, *speeds


def prepare(place_ref, fields, own, speed):
    own[...] = fields[...]
    keep = jnp.where(place_ref[0] == place_ref[1], 0.0, 1.0).astype(F32)
    most = jnp.zeros((ROWS, COLS), F32)
    for k in range(LEVELS):
        w = jnp.abs(fields[W, k])
        if k == LEVELS - 1:
            w = w * keep
        most = jnp.maximum(most, jnp.abs(fields[U, k]) + jnp.abs(fields[V, k]) + w)
    speed[...] = jnp.broadcast_to(jnp.max(most), speed.shape)


def droplets(radius, weight, column, counts, fall_depth, first, count, after):
    slots, step = radius.shape[0], 2
    counts, _ = lax.optimization_barrier((counts, after))
    whole = pl.BlockSpec((slots, step, ROWS, COLS), lambda i: (0, first // step + i, 0, 0))
    return pl.pallas_call(
        deposit,
        name="deposit",
        grid=(count // step,),
        in_specs=[
            whole,
            whole,
            whole,
            pl.BlockSpec((step, ROWS, COLS), lambda i: (first // step + i, 0, 0)),
            pl.BlockSpec((slots, step, ROWS, 1), lambda i: (0, first // step + i, 0, 0)),
        ],
        out_specs=pl.BlockSpec((step, FMAX + 1, 3, ROWS, COLS), lambda i: (i, 0, 0, 0, 0)),
        out_shape=pltpu.HBM((count, FMAX + 1, 3, ROWS, COLS), F32),
        compiler_params=pltpu.CompilerParams(vmem_limit_bytes=12 << 20),
        cost_estimate=pl.CostEstimate(
            flops=100_000_000 * count, bytes_accessed=0, transcendentals=0
        ),
    )(
        *(
            pltpu.with_memory_space_constraint(value, pltpu.HBM)
            for value in (radius, weight, column, counts)
        ),
        fall_depth,
    )


def per_device(fields, radius, weight, column, counts, fall_depth):
    place = lax.axis_index("gz")
    last = lax.axis_size("gz") - 1
    where = jnp.stack([place, jnp.int32(last)]).astype(jnp.int32)
    def drops(first, count, after):
        return droplets(radius, weight, column, counts, fall_depth, first, count, after)

    own, speed = pl.pallas_call(
        prepare,
        name="prepare",
        in_specs=smem(1) + vmem(1),
        out_specs=tuple(vmem(2)),
        out_shape=(held(5, LEVELS, ROWS, COLS), shaped(ROWS, COLS)),
        compiler_params=pltpu.CompilerParams(vmem_limit_bytes=4 << 20),
    )(where, fields)
    pair = [(i, i ^ 1) for i in range(lax.axis_size("gx"))]
    speed = jnp.maximum(speed, lax.ppermute(speed, "gx", pair))
    plane = ("gy_hi", "gz")
    early = drops(0, 6, speed)
    speed = jnp.broadcast_to(speed[0:1], (lax.axis_size(plane), 1, COLS))
    speed = jnp.max(lax.all_to_all(speed, plane, 0, 0), axis=0)
    *near, from_up, from_down, sent, speed = exchange(FIRST, own, fields, fields, [early], speed)
    other_speed = lax.ppermute(speed, "gy_lo", [(0, 1), (1, 0)])
    second = drops(6, 2, sent)
    ext = held(len(FIRST.tiles), DEPTH, ROWS, WIDE)
    start, flat = call(
        first_own,
        "first_own",
        smem(1) + vmem(5),
        [ext, held(2, LEVELS, 2 * ROWS, WIDE)],
    )(where, own, *near)
    start, s2, down, up, dt = call(
        two_sections,
        "two_sections",
        smem(1) + vmem(6) + far(1),
        [ext, held(5, LEVELS, ROWS, COLS)] + [held(3, LEVELS, ROWS, COLS)] * 2 + [shaped(1)],
        scratch=[
            pltpu.VMEM((2, DEPTH, 2 * ROWS, WIDE), F32),
            pltpu.VMEM((5, DEPTH, 2 * ROWS, WIDE), F32),
            pltpu.VMEM((DEPTH, 2 * ROWS, WIDE), F32),
            pltpu.VMEM((4, DEPTH, 2 * ROWS, WIDE), F32),
        ],
        out_specs=vmem(4) + smem(1),
        grant=12,
        alias={3: 0},
    )(where, speed, other_speed, start, flat, from_up, from_down, second)
    middle = drops(8, 8, s2)
    *near, from_up, from_down, _ = exchange(SECOND, s2, down, up, [middle])
    by_depth = [early, second, middle]
    ext = held(len(SECOND.tiles), DEPTH, ROWS, WIDE)
    around_s2, flat, flat_tracer = call(
        second_own,
        "second_own",
        vmem(5),
        [ext, held(1, LEVELS, 2 * ROWS, WIDE), held(LEVELS, ROWS, COLS)],
        flops=1_000_000_000,
    )(s2, *near)
    rows = held(DEPTH, 2 * ROWS, WIDE)
    _, tracer, landed, fallen, rate, warm = call(
        last_tracer,
        "last_tracer",
        smem(2) + vmem(6) + far(len(by_depth)),
        [
            ext,
            held(LEVELS, ROWS, COLS),
            held(3, LEVELS, ROWS, COLS),
            held(3, FMAX, ROWS, COLS),
            rows,
            rows,
        ],
        scratch=[
            pltpu.VMEM((2, LEVELS, ROWS, COLS), F32),
            pltpu.VMEM((LEVELS, FMAX + 1, 3, ROWS, COLS), F32),
            pltpu.SemaphoreType.DMA((len(by_depth),)),
        ],
        alias={2: 0},
    )(where, dt, around_s2, flat, flat_tracer, from_up, from_down, own, *by_depth)
    count = lax.axis_size("gz")
    arrived = lax.ppermute(fallen, "gz", [((i + 1) % count, i) for i in range(count)])
    (new_fields,) = call(
        last_section,
        "last_section",
        smem(2) + vmem(4),
        [shaped(5, LEVELS, ROWS, COLS)],
        scratch=[pltpu.VMEM((4, DEPTH, 2 * ROWS, WIDE), F32)],
        flops=1_000_000_000,
    )(where, dt, rate, warm, start, tracer)
    (moments,) = call(
        land, "land", smem(1) + vmem(2), [shaped(3, LEVELS, ROWS, COLS)]
    )(where, landed, arrived)
    return (new_fields, moments)


def solution(mesh):
    count = mesh.shape["gy"]
    split = Mesh(
        mesh.devices.reshape(mesh.shape["gx"], count // 2, 2, mesh.shape["gz"]),
        ("gx", *GY, "gz"),
    )
    spread = P(None, "gz", GY, "gx")
    return jax.shard_map(
        per_device,
        mesh=split,
        in_specs=(spread, spread, spread, spread, P("gz", GY, "gx"), spread),
        out_specs=(spread, spread),
        check_vma=False,
    )
```

```python
import jax
import jax.numpy as jnp
from jax import lax
from jax.experimental import pallas as pl
from jax.experimental.pallas import tpu as pltpu
from jax.sharding import Mesh
from jax.sharding import PartitionSpec as P

NS = 4
FMAX = 8
GY = ("gy_hi", "gy_lo")

sound_speed = 10.0
buoyancy = 0.5
courant_goal = 0.6
growth = 0.3

LEVELS, ROWS, COLS = 16, 8, 128
WIDE = 2 * COLS
REACH = 7
DEPTH = LEVELS + 2 * REACH
EDGE = 8
F32 = jnp.float32
C, PR, U, V, W = range(5)


class Plan:
    def __init__(self, tall, reach, sent):
        self.tall, self.reach = tall, reach
        self.tiles = [
            (field, part)
            for field in range(5)
            for part in ("oab" if field in tall else "on")
        ]
        self.at = {tile: n for n, tile in enumerate(self.tiles)}
        self.carried = []
        for a in range(reach):
            for field in range(5):
                for part in sent[field][a] if a < len(sent[field]) else "":
                    self.carried.append((a, (field, part), 0))
            if a < reach - 1:
                self.carried += [(a, None, 0), (a, None, 1)]

    def rows(self, ref, field, l):
        return jnp.concatenate(
            [
                ref[self.at[field, part], l]
                for part in ("oab" if field in self.tall else "on")
            ],
            axis=0,
        )

    def sixteen(self, ref, field, l):
        value = self.rows(ref, field, l)
        return sixteen(value) if field in self.tall else value


def lanes(shape):
    return lax.broadcasted_iota(jnp.int32, shape, len(shape) - 1)


def lower_rows(shape):
    return lax.broadcasted_iota(jnp.int32, shape, 0) < ROWS // 2


def around(above, below):
    return jnp.where(lower_rows(above.shape), above, below)


def sixteen(value):
    return jnp.concatenate(
        [value[0:ROWS], around(value[ROWS : 2 * ROWS], value[2 * ROWS :])], axis=0
    )


def raw_tile(refs, field, part, k):
    own, above, below = refs
    if part == "o":
        return own[field, k]
    if part == "n":
        return around(above[field, k], below[field, k])
    return (above if part == "a" else below)[field, k]


SHARED = {C: (1, 0), U: (1, 1), V: (2, 0), W: (2, 1)}


def shared_rows(read):
    down, up = [read(PR)], [read(PR)]
    for first, second in ((C, U), (V, W)):
        one, other = read(first), pltpu.roll(read(second), ROWS // 2, 0)
        down.append(around(one, other))
        up.append(around(other, one))
    return down, up


def shared_tile(refs, field, part, k):
    own, above, below = refs
    if part == "o":
        return own[field, k]
    if part == "n" and field == PR:
        return around(above[0, k], below[0, k])
    if part == "n":
        index, half = SHARED[field]
        if half == 0:
            return around(above[index, k], below[index, k])
        return pltpu.roll(around(below[index, k], above[index, k]), ROWS // 2, 0)
    return (above if part == "a" else below)[0, k]


THREE, TWO, ONE = "oab", "on", "o"
FIRST = Plan(
    (C, PR, V),
    7,
    {
        C: [THREE] + [TWO] * 4 + [ONE],
        PR: [THREE] * 2 + [TWO] * 4 + [ONE],
        U: [TWO] * 3 + [ONE],
        V: [TWO] * 4,
        W: [TWO] * 4 + [ONE],
    },
)
SECOND = Plan(
    (PR,),
    6,
    {
        C: [TWO] * 3 + [ONE],
        PR: [THREE] + [TWO] * 4 + [ONE],
        U: [TWO] * 3,
        V: [TWO] * 3,
        W: [TWO] * 3 + [ONE],
    },
)
TILE_OF = {FIRST: raw_tile, SECOND: shared_tile}


SPARE = 104


def pack_columns(plan, with_speed):
    def kernel(own, above, below, *rest):
        to_left, to_right = rest[-2:]
        lane = lanes((ROWS, COLS))
        filler = jnp.zeros((ROWS, COLS), F32)
        if with_speed:
            filler = filler + jnp.max(rest[0][...])

        def one(k, _):
            left = filler
            right = filler
            for n, (field, part) in enumerate(plan.tiles):
                start = n * EDGE
                here = (lane >= start) & (lane < start + EDGE)
                value = TILE_OF[plan]((own, above, below), field, part, k)
                first = pltpu.roll(value, start, 1) if start else value
                last = pltpu.roll(value, (start + EDGE) % COLS, 1)
                left = jnp.where(here, first, left)
                right = jnp.where(here, last, right)
            to_left[k] = left
            to_right[k] = right
            return 0

        def some(levels, _):
            for k in levels:
                one(k, 0)
            return 0

        sweep(0, LEVELS, 8, some)

    return kernel


def halo_columns(from_right, from_left, n):
    start = n * EDGE
    right = pltpu.roll(from_right, COLS - start, 1) if start else from_right
    left = pltpu.roll(from_left, (COLS - EDGE - start) % COLS, 1)
    return jnp.where(lanes((ROWS, COLS)) < COLS // 2, right, left)


def pack_levels(plan, with_speed):
    def kernel(own, above, below, from_right, from_left, *rest):
        if with_speed:
            speed, to_down, to_up, speeds = rest
            near = jnp.maximum(from_right[0], from_left[0])
            near = jnp.where(lanes((ROWS, COLS)) < SPARE, 0.0, near)
            top = jnp.maximum(jnp.max(near), jnp.max(speed[...]))
            speeds[...] = jnp.broadcast_to(top, speeds.shape)
        else:
            to_down, to_up = rest
        for index, (a, tile, side) in enumerate(plan.carried):
            for out, k in ((to_down, a), (to_up, LEVELS - 1 - a)):
                if tile:
                    out[index] = TILE_OF[plan]((own, above, below), *tile, k)
                else:
                    out[index] = (from_left if side else from_right)[k]

    return kernel


def place_own(plan, refs, ext):
    own, above, below, from_right, from_left = refs

    def middle(levels, _):
        for k in levels:
            right, left = from_right[k], from_left[k]
            for n, (field, part) in enumerate(plan.tiles):
                ext[n, REACH + k, :, 0:COLS] = TILE_OF[plan]((own, above, below), field, part, k)
                ext[n, REACH + k, :, COLS:WIDE] = halo_columns(right, left, n)
        return 0

    sweep(0, LEVELS, 4, middle)


def place_halo(plan, from_up, from_down, ext, place, last):
    columns = {(a, side): i for i, (a, tile, side) in enumerate(plan.carried) if not tile}
    for message, level, there in (
        (from_down, lambda a: REACH - 1 - a, place > 0),
        (from_up, lambda a: REACH + LEVELS + a, place < last),
    ):
        keep = jnp.where(there, 1.0, 0.0).astype(F32)
        for index, (a, tile, _) in enumerate(plan.carried):
            if not tile:
                continue
            field, part = tile
            value = message[index] * keep
            for kept in "ab" if part == "n" and field in plan.tall else part:
                n = plan.at[field, kept]
                ext[n, level(a), :, 0:COLS] = value
                if (a, 0) in columns:
                    ext[n, level(a), :, COLS:WIDE] = (
                        halo_columns(message[columns[a, 0]], message[columns[a, 1]], n) * keep
                    )


def shift(value, by, axis):
    return pltpu.roll(value, (-by) % value.shape[axis], axis)


def face_flux(q, wind):
    central = 37.0 * (q[2] + q[3]) - 8.0 * (q[1] + q[4]) + (q[0] + q[5])
    upwind = 10.0 * (q[3] - q[2]) - 5.0 * (q[4] - q[1]) + (q[5] - q[0])
    return wind * central - jnp.abs(wind) * upwind


def flat_flux(q, wind, axis):
    flux = face_flux([shift(q, by, axis) if by else q for by in range(-2, 4)], wind)
    return flux - shift(flux, -1, axis)


def rows_flux(q, wind):
    if wind.shape[0] == 24:
        return sixteen(flat_flux(q, wind, 0))
    if q.shape[0] == 24:
        flux = face_flux([sixteen(shift(q, by, 0) if by else q) for by in range(-2, 4)], wind)
        return flux - shift(flux, -1, 0)
    return flat_flux(q, wind, 0)


def level_flux(read, wind, l):
    return face_flux([read(l + by) for by in range(-2, 4)], wind)


def in_domain(l, place, last, lid):
    g = place * LEVELS + l - REACH
    top = (last + 1) * LEVELS - (1 if lid else 0)
    return jnp.where((g >= 0) & (g < top), 1.0, 0.0).astype(F32)


SIXTIETH = -1.0 / 60.0


def sweep(first, count, most, body, carry=0):
    size = max(n for n in range(1, most + 1) if count % n == 0)

    def run(i, carry):
        start = first + i * size
        return body([start + n for n in range(size)], carry)

    return lax.fori_loop(0, count // size, run, carry)


def flat_part(plan, ext, field, l):
    return flat_flux(plan.sixteen(ext, field, l), plan.sixteen(ext, U, l), 1) + rows_flux(
        plan.rows(ext, field, l), plan.rows(ext, V, l)
    )


def flat_own(plan, ext, fields, flat):
    def some(levels, _):
        results = [(n, l, flat_part(plan, ext, f, l)) for l in levels for n, f in enumerate(fields)]
        for n, l, value in results:
            flat[n, l - REACH] = value
        return 0

    sweep(REACH, LEVELS, 4, some)


def rates(plan, ext, fields, write, around_own, most, flat=None):
    reads = [lambda l, f=f: plan.sixteen(ext, f, l) for f in fields]

    def some(levels, lows, flat=None):
        results = []
        for l in levels:
            w = plan.sixteen(ext, W, l)
            highs = []
            for n, f in enumerate(fields):
                high = level_flux(reads[n], w, l)
                level = flat[n, l - REACH] if flat is not None else flat_part(plan, ext, f, l)
                results.append((n, l, (level + (high - lows[n])) * SIXTIETH))
                highs.append(high)
            lows = tuple(highs)
        for result in results:
            write(*result)
        return lows

    first = REACH - around_own
    w = plan.sixteen(ext, W, first - 1)
    lows = tuple(level_flux(read, w, first - 1) for read in reads)
    if flat is None:
        sweep(first, LEVELS + 2 * around_own, most, some, lows)
        return
    lows = sweep(first, around_own, most, some, lows)
    lows = sweep(REACH, LEVELS, 4, lambda levels, c: some(levels, c, flat), lows)
    sweep(REACH + LEVELS, around_own, most, some, lows)


def first_own(place_ref, own, above, below, from_right, from_left, ext, flat):
    place_own(FIRST, (own, above, below, from_right, from_left), ext)

    @pl.when(place_ref[0] == place_ref[1])
    def _():
        for part in "on":
            ext[FIRST.at[W, part], REACH + LEVELS - 1] = jnp.zeros((ROWS, WIDE), F32)

    flat_own(FIRST, ext, (C, PR), flat)


def acoustic(p, u, v, w, read_c, rate, step, first, count, place, last):
    pull = step * sound_speed

    def level(value):
        return sixteen(value) if value.shape[0] == 24 else value

    def wind_w(l, lift_low, lift_high, p_here, p_above):
        lift = (buoyancy * 0.5) * (lift_low + lift_high)
        return (w[0](l) + step * lift - pull * (p_above - p_here)) * in_domain(l, place, last, True)

    def some(levels, w_low):
        talls = [p[0](l) for l in (*levels, levels[-1] + 1)]
        cells = [level(value) for value in talls]
        warm = [read_c(l) for l in (*levels, levels[-1] + 1)]
        results = []
        for n, l in enumerate(levels):
            p_here = cells[n]
            w_new = wind_w(l, warm[n], warm[n + 1], p_here, cells[n + 1])
            u_new = u[0](l) - pull * (shift(p_here, 1, 1) - p_here)
            v_old = v[0](l)
            if v_old.shape[0] == 24:
                v_tall = v_old - pull * (shift(talls[n], 1, 0) - talls[n])
                v_new, v_flow = sixteen(v_tall), sixteen(v_tall - shift(v_tall, -1, 0))
            else:
                v_new = v_old - pull * (shift(p_here, 1, 0) - p_here)
                v_flow = v_new - shift(v_new, -1, 0)
            divergence = (u_new - shift(u_new, -1, 1)) + v_flow + (w_new - w_low)
            p_new = (p_here + step * rate(l) - pull * divergence) * in_domain(
                l, place, last, False
            )
            results.append((l, p_new, u_new, v_new, w_new))
            w_low = w_new
        for l, *news in results:
            for target, value in zip((p, u, v, w), news):
                target[1](l, value)
        return w_low

    low = first - 1
    w_low = wind_w(low, read_c(low), read_c(first), level(p[0](low)), level(p[0](first)))
    w[1](low, w_low)
    sweep(first, count, 12, some, w_low)


def access(ref, *lead):
    def read(l):
        return ref[(*lead, l)]

    def write(l, value):
        ref[(*lead, l)] = value

    return read, write


def begin(start, field, tall=False):
    return lambda l: (FIRST.rows if tall else FIRST.sixteen)(start, field, l)


def own_write(ref, field):
    def write(l, value):
        if not isinstance(l, int):
            ref[field, l - REACH] = value[0:ROWS, 0:COLS]

    return write


def tracer_flat(tiles, u, v, l):
    rows = flat_flux(tiles(l)[:, 0:COLS], v(l)[:, 0:COLS], 0)[0:ROWS]
    return rows + flat_flux(tiles(l)[0:ROWS], u(l)[0:ROWS], 1)[:, 0:COLS]


def tracer_high(tiles, w, l):
    return level_flux(lambda m: tiles(m)[0:ROWS, 0:COLS], w(l)[0:ROWS, 0:COLS], l)


def two_sections(
    place_ref,
    speed,
    other_speed,
    start_in,
    flat,
    from_up,
    from_down,
    start,
    s2,
    down,
    up,
    dt_out,
    rate0,
    s1,
    rate1,
    fast,
):
    place, last = place_ref[0], place_ref[1]
    place_halo(FIRST, from_up, from_down, start, place, last)

    def write0(n, l, value):
        rate0[n, l] = value

    rates(FIRST, start, (C, PR), write0, 4, 4, flat)
    dt = courant_goal / (1.0 + jnp.max(jnp.maximum(speed[...], other_speed[...])))
    dt_out[0] = dt
    third = dt * (1.0 / 3.0)

    def tracer(levels, _):
        for l in levels:
            s1[C, l] = (FIRST.sixteen(start, C, l) + third * rate0[0, l]) * in_domain(
                l, place, last, False
            )
        return 0

    sweep(REACH - 4, LEVELS + 8, 4, tracer)
    acoustic(
        (begin(start, PR, True), access(s1, PR)[1]),
        (begin(start, U), access(s1, U)[1]),
        (begin(start, V, True), access(s1, V)[1]),
        (begin(start, W), access(s1, W)[1]),
        begin(start, C),
        access(rate0, 1)[0],
        third,
        REACH - 4,
        LEVELS + 8,
        place,
        last,
    )
    half = dt * 0.5
    tiles = access(s1, C)[0]
    winds = [access(s1, f)[0] for f in (U, V, W)]

    def own_tracer(levels, low):
        results = []
        for l in levels:
            high = tracer_high(tiles, winds[2], l)
            tendency = (tracer_flat(tiles, *winds[:2], l) + (high - low)) * SIXTIETH
            low = high
            results.append(start[FIRST.at[C, "o"], l, :, 0:COLS] + half * tendency)
        for l, value in zip(levels, results):
            s2[C, l - REACH] = value
        return low

    sweep(REACH, LEVELS, 8, own_tracer, tracer_high(tiles, winds[2], REACH - 1))

    def write(n, l, value):
        rate1[l] = value

    rates(SECTION, s1, (PR,), write, 1, 6)
    step = half / (NS // 2)
    acoustic(
        (begin(start, PR), access(fast, 0)[1]),
        (begin(start, U), access(fast, 1)[1]),
        (begin(start, V), access(fast, 2)[1]),
        (begin(start, W), access(fast, 3)[1]),
        access(s1, C)[0],
        access(rate1)[0],
        step,
        REACH - 1,
        LEVELS + 2,
        place,
        last,
    )
    acoustic(
        (access(fast, 0)[0], own_write(s2, PR)),
        (access(fast, 1)[0], own_write(s2, U)),
        (access(fast, 2)[0], own_write(s2, V)),
        (access(fast, 3)[0], own_write(s2, W)),
        access(s1, C)[0],
        access(rate1)[0],
        step,
        REACH,
        LEVELS,
        place,
        last,
    )

    def share(levels, _):
        made = [shared_rows(lambda f, k=k: s2[f, k]) for k in levels]
        for k, (to_down, to_up) in zip(levels, made):
            for n in range(3):
                down[n, k] = to_down[n]
                up[n, k] = to_up[n]
        return 0

    sweep(0, LEVELS, 4, share)


class Whole:
    def rows(self, ref, field, l):
        return ref[field, l]

    sixteen = rows


SECTION = Whole()


def second_own(own, above, below, from_right, from_left, ext, flat, tracer):
    place_own(SECOND, (own, above, below, from_right, from_left), ext)
    flat_own(SECOND, ext, (PR,), flat)
    tiles, u, v = (lambda l, f=f: SECOND.rows(ext, f, l) for f in (C, U, V))

    def some(levels, _):
        results = [tracer_flat(tiles, u, v, l) for l in levels]
        for l, value in zip(levels, results):
            tracer[l - REACH] = value
        return 0

    sweep(REACH, LEVELS, 4, some)


def last_tracer(
    place_ref, dt_ref, ext_in, flat, flat_tracer, from_up, from_down, initial, *rest
):
    *chunks, ext, tracer, landed, fallen, rate, warm, factor, by_depth, sem = rest
    dt = dt_ref[0]
    copies, first = [], 0
    for n, chunk in enumerate(chunks):
        there = by_depth.at[pl.ds(first, chunk.shape[0])]
        copies.append(pltpu.make_async_copy(chunk, there, sem.at[n]))
        first += chunk.shape[0]
    for copy in copies:
        copy.start()
    place_halo(SECOND, from_up, from_down, ext, place_ref[0], place_ref[1])

    def write(n, l, value):
        rate[l] = value

    rates(SECOND, ext, (PR,), write, 3, 3, flat)

    def keep(levels, _):
        for l in levels:
            warm[l] = SECOND.rows(ext, C, l)
        return 0

    sweep(REACH - 4, LEVELS + 8, 4, keep)
    tiles = lambda l: SECOND.rows(ext, C, l)
    w = lambda l: SECOND.rows(ext, W, l)

    def some(levels, low):
        results = []
        for l in levels:
            high = tracer_high(tiles, w, l)
            tendency = (flat_tracer[l - REACH] + (high - low)) * SIXTIETH
            low = high
            c = initial[C, l - REACH] + dt * tendency
            grown = jnp.exp(growth * c)
            results.append((c, grown, grown * jnp.exp((0.5 * growth) * c)))
        for l, (c, second, third) in zip(levels, results):
            tracer[l - REACH] = c
            factor[0, l - REACH] = second
            factor[1, l - REACH] = third
        return low

    sweep(REACH, LEVELS, 4, some, tracer_high(tiles, w, REACH - 1))
    for copy in copies:
        copy.wait()
    for target in range(-FMAX, LEVELS):
        for moment in range(3):
            total = None
            for depth in range(FMAX + 1):
                k = target + depth
                if 0 <= k < LEVELS:
                    value = by_depth[k, depth, moment]
                    if moment:
                        value = value * factor[moment - 1, k]
                    total = value if total is None else total + value
            if target < 0:
                fallen[moment, target + FMAX] = total
            else:
                landed[moment, target] = total


def last_section(place_ref, dt_ref, rate, warm, start, tracer, out, fast):
    place, last = place_ref[0], place_ref[1]
    step = dt_ref[0] / NS
    out[C] = tracer[...]
    names = (PR, U, V, W)
    for repeat in range(NS):
        reads = [
            begin(start, f) if repeat == 0 else access(fast, n)[0] for n, f in enumerate(names)
        ]
        writes = [
            own_write(out, f) if repeat == NS - 1 else access(fast, n)[1]
            for n, f in enumerate(names)
        ]
        acoustic(
            *zip(reads, writes),
            access(warm)[0],
            access(rate)[0],
            step,
            REACH - 3 + repeat,
            LEVELS + 6 - 2 * repeat,
            place,
            last,
        )


def land(place_ref, landed, arrived, out):
    keep = jnp.where(place_ref[0] < place_ref[1], 1.0, 0.0).astype(F32)
    out[:, 0 : LEVELS - FMAX] = landed[:, 0 : LEVELS - FMAX]
    out[:, LEVELS - FMAX :] = landed[:, LEVELS - FMAX :] + keep * arrived[...]


def deposit(radius, weight, column, counts, fall_depth, out):
    slots, levels = radius.shape[0], radius.shape[1]
    target = lax.broadcasted_iota(jnp.int32, (COLS, COLS), 0)
    row = lax.broadcasted_iota(jnp.int32, (ROWS, COLS), 0)
    per_step = 4

    for k in range(levels):
        out[k] = jnp.zeros(out.shape[1:], F32)
        live = counts[k]

        def some(step, _, k=k, live=live):
            sums = [[None] * 3 for _ in range(FMAX + 1)]
            for part in range(per_step):
                s = step * per_step + part
                r = radius[s, k]
                number = jnp.where(s < live, weight[s, k], 0.0)
                area = number * r * r
                terms = []
                for t in (number, area, area * r):
                    high = t.astype(jnp.bfloat16).astype(F32)
                    terms += [high, t - high]
                cols = column[s, k]
                left, right = [], []
                for j in range(ROWS):
                    left.append(
                        jnp.concatenate([jnp.where(row == j, t, 0.0) for t in terms], axis=0)
                    )
                    right.append(jnp.where(cols[j : j + 1] == target, 1.0, 0.0).astype(F32))
                sent = lax.dot_general(
                    jnp.concatenate(left, axis=1),
                    jnp.concatenate(right, axis=1),
                    (((1,), (1,)), ((), ())),
                    preferred_element_type=F32,
                )
                depth = jnp.broadcast_to(fall_depth[s, k], (ROWS, COLS))
                for d in range(FMAX + 1):
                    falls = depth == d
                    for m in range(3):
                        both = sent[16 * m : 16 * m + 8] + sent[16 * m + 8 : 16 * m + 16]
                        value = jnp.where(falls, both, 0.0)
                        sums[d][m] = value if sums[d][m] is None else sums[d][m] + value
            for d in range(FMAX + 1):
                for m in range(3):
                    out[k, d, m] += sums[d][m]
            return 0

        lax.fori_loop(0, slots // per_step, some, 0)


def vmem(n):
    return [pl.BlockSpec(memory_space=pltpu.VMEM)] * n


def smem(n):
    return [pl.BlockSpec(memory_space=pltpu.SMEM)] * n


def far(n):
    return [pl.BlockSpec(memory_space=pltpu.HBM)] * n


def shaped(*dims):
    return jax.ShapeDtypeStruct(dims, F32)


def held(*dims):
    return pltpu.VMEM(dims, F32)


def call(kernel, name, ins, outs, scratch=(), out_specs=None, flops=None, grant=4, alias=None):
    made = pl.pallas_call(
        kernel,
        name=name,
        in_specs=ins,
        out_specs=tuple(out_specs or vmem(len(outs))),
        out_shape=tuple(outs),
        scratch_shapes=list(scratch),
        input_output_aliases=alias or {},
        compiler_params=pltpu.CompilerParams(vmem_limit_bytes=grant << 20),
        cost_estimate=(
            pl.CostEstimate(flops=flops, bytes_accessed=0, transcendentals=0) if flops else None
        ),
    )

    def run(*operands):
        return made(
            *(
                pltpu.with_memory_space_constraint(value, spec.memory_space)
                if spec.memory_space != pltpu.SMEM
                else value
                for spec, value in zip(ins, operands)
            )
        )

    return run


def both_ways(down, axis, up):
    count = lax.axis_size(axis)
    return (
        lax.ppermute(down, axis, [((i + 1) % count, i) for i in range(count)]),
        lax.ppermute(up, axis, [(i, (i + 1) % count) for i in range(count)]),
    )


def exchange(plan, own, down, up, tokens=(), speed=None):
    above, below = both_ways(down, GY, up)
    extra = [] if speed is None else [speed]
    to_left, to_right = call(
        pack_columns(plan, bool(extra)),
        "pack_columns",
        vmem(3 + len(extra)) + far(len(tokens)),
        [held(LEVELS, ROWS, COLS)] * 2,
    )(own, above, below, *extra, *tokens)
    from_right, from_left = both_ways(to_left, "gx", to_right)
    tiles = len(plan.carried)
    to_down, to_up, *speeds = call(
        pack_levels(plan, bool(extra)),
        "pack_levels",
        vmem(5 + len(extra)),
        [held(tiles, ROWS, COLS)] * 2 + [held(ROWS, COLS)] * len(extra),
    )(own, above, below, from_right, from_left, *extra)
    from_up, from_down = both_ways(to_down, "gz", to_up)
    return above, below, from_right, from_left, from_up, from_down, to_down, *speeds


def prepare(place_ref, fields, own, speed):
    own[...] = fields[...]
    keep = jnp.where(place_ref[0] == place_ref[1], 0.0, 1.0).astype(F32)
    most = jnp.zeros((ROWS, COLS), F32)
    for k in range(LEVELS):
        w = jnp.abs(fields[W, k])
        if k == LEVELS - 1:
            w = w * keep
        most = jnp.maximum(most, jnp.abs(fields[U, k]) + jnp.abs(fields[V, k]) + w)
    speed[...] = jnp.broadcast_to(jnp.max(most), speed.shape)


def droplets(radius, weight, column, counts, fall_depth, first, count, after):
    slots, step = radius.shape[0], 2
    counts, _ = lax.optimization_barrier((counts, after))
    whole = pl.BlockSpec((slots, step, ROWS, COLS), lambda i: (0, first // step + i, 0, 0))
    return pl.pallas_call(
        deposit,
        name="deposit",
        grid=(count // step,),
        in_specs=[
            whole,
            whole,
            whole,
            pl.BlockSpec((step, ROWS, COLS), lambda i: (first // step + i, 0, 0)),
            pl.BlockSpec((slots, step, ROWS, 1), lambda i: (0, first // step + i, 0, 0)),
        ],
        out_specs=pl.BlockSpec((step, FMAX + 1, 3, ROWS, COLS), lambda i: (i, 0, 0, 0, 0)),
        out_shape=pltpu.HBM((count, FMAX + 1, 3, ROWS, COLS), F32),
        compiler_params=pltpu.CompilerParams(vmem_limit_bytes=12 << 20),
        cost_estimate=pl.CostEstimate(
            flops=100_000_000 * count, bytes_accessed=0, transcendentals=0
        ),
    )(
        *(
            pltpu.with_memory_space_constraint(value, pltpu.HBM)
            for value in (radius, weight, column, counts)
        ),
        fall_depth,
    )


def per_device(fields, radius, weight, column, counts, fall_depth):
    place = lax.axis_index("gz")
    last = lax.axis_size("gz") - 1
    where = jnp.stack([place, jnp.int32(last)]).astype(jnp.int32)
    def drops(first, count, after):
        return droplets(radius, weight, column, counts, fall_depth, first, count, after)

    own, speed = pl.pallas_call(
        prepare,
        name="prepare",
        in_specs=smem(1) + vmem(1),
        out_specs=tuple(vmem(2)),
        out_shape=(held(5, LEVELS, ROWS, COLS), shaped(ROWS, COLS)),
        compiler_params=pltpu.CompilerParams(vmem_limit_bytes=4 << 20),
    )(where, fields)
    pair = [(i, i ^ 1) for i in range(lax.axis_size("gx"))]
    speed = jnp.maximum(speed, lax.ppermute(speed, "gx", pair))
    plane = ("gy_hi", "gz")
    early = drops(0, 8, speed)
    speed = jnp.broadcast_to(speed[0:1], (lax.axis_size(plane), 1, COLS))
    speed = jnp.max(lax.all_to_all(speed, plane, 0, 0), axis=0)
    *near, from_up, from_down, _, speed = exchange(FIRST, own, fields, fields, [early], speed)
    other_speed = lax.ppermute(speed, "gy_lo", [(0, 1), (1, 0)])
    ext = held(len(FIRST.tiles), DEPTH, ROWS, WIDE)
    start, flat = call(
        first_own,
        "first_own",
        smem(1) + vmem(5),
        [ext, held(2, LEVELS, 2 * ROWS, WIDE)],
    )(where, own, *near)
    start, s2, down, up, dt = call(
        two_sections,
        "two_sections",
        smem(1) + vmem(6),
        [ext, held(5, LEVELS, ROWS, COLS)] + [held(3, LEVELS, ROWS, COLS)] * 2 + [shaped(1)],
        scratch=[
            pltpu.VMEM((2, DEPTH, 2 * ROWS, WIDE), F32),
            pltpu.VMEM((5, DEPTH, 2 * ROWS, WIDE), F32),
            pltpu.VMEM((DEPTH, 2 * ROWS, WIDE), F32),
            pltpu.VMEM((4, DEPTH, 2 * ROWS, WIDE), F32),
        ],
        out_specs=vmem(4) + smem(1),
        grant=12,
        alias={3: 0},
    )(where, speed, other_speed, start, flat, from_up, from_down)
    middle = drops(8, 6, s2)
    *near, from_up, from_down, sent = exchange(SECOND, s2, down, up, [middle])
    by_depth = [early, middle, drops(14, 2, sent)]
    ext = held(len(SECOND.tiles), DEPTH, ROWS, WIDE)
    around_s2, flat, flat_tracer = call(
        second_own,
        "second_own",
        vmem(5),
        [ext, held(1, LEVELS, 2 * ROWS, WIDE), held(LEVELS, ROWS, COLS)],
        flops=1_000_000_000,
    )(s2, *near)
    rows = held(DEPTH, 2 * ROWS, WIDE)
    _, tracer, landed, fallen, rate, warm = call(
        last_tracer,
        "last_tracer",
        smem(2) + vmem(6) + far(len(by_depth)),
        [
            ext,
            held(LEVELS, ROWS, COLS),
            held(3, LEVELS, ROWS, COLS),
            held(3, FMAX, ROWS, COLS),
            rows,
            rows,
        ],
        scratch=[
            pltpu.VMEM((2, LEVELS, ROWS, COLS), F32),
            pltpu.VMEM((LEVELS, FMAX + 1, 3, ROWS, COLS), F32),
            pltpu.SemaphoreType.DMA((len(by_depth),)),
        ],
        alias={2: 0},
    )(where, dt, around_s2, flat, flat_tracer, from_up, from_down, own, *by_depth)
    count = lax.axis_size("gz")
    arrived = lax.ppermute(fallen, "gz", [((i + 1) % count, i) for i in range(count)])
    (new_fields,) = call(
        last_section,
        "last_section",
        smem(2) + vmem(4),
        [shaped(5, LEVELS, ROWS, COLS)],
        scratch=[pltpu.VMEM((4, DEPTH, 2 * ROWS, WIDE), F32)],
        flops=1_000_000_000,
    )(where, dt, rate, warm, start, tracer)
    (moments,) = call(
        land, "land", smem(1) + vmem(2), [shaped(3, LEVELS, ROWS, COLS)]
    )(where, landed, arrived)
    return (new_fields, moments)


def solution(mesh):
    count = mesh.shape["gy"]
    split = Mesh(
        mesh.devices.reshape(mesh.shape["gx"], count // 2, 2, mesh.shape["gz"]),
        ("gx", *GY, "gz"),
    )
    spread = P(None, "gz", GY, "gx")
    return jax.shard_map(
        per_device,
        mesh=split,
        in_specs=(spread, spread, spread, spread, P("gz", GY, "gx"), spread),
        out_specs=(spread, spread),
        check_vma=False,
    )
```

```python
import jax
import jax.numpy as jnp
from jax import lax
from jax.experimental import pallas as pl
from jax.experimental.pallas import tpu as pltpu
from jax.sharding import Mesh
from jax.sharding import PartitionSpec as P

NS = 4
FMAX = 8
GY = ("gy_hi", "gy_lo")

sound_speed = 10.0
buoyancy = 0.5
courant_goal = 0.6
growth = 0.3

LEVELS, ROWS, COLS = 16, 8, 128
WIDE = 2 * COLS
REACH = 7
DEPTH = LEVELS + 2 * REACH
EDGE = 8
F32 = jnp.float32
C, PR, U, V, W = range(5)


class Plan:
    def __init__(self, tall, reach, sent):
        self.tall, self.reach = tall, reach
        self.tiles = [
            (field, part)
            for field in range(5)
            for part in ("oab" if field in tall else "on")
        ]
        self.at = {tile: n for n, tile in enumerate(self.tiles)}
        self.carried = []
        for a in range(reach):
            for field in range(5):
                for part in sent[field][a] if a < len(sent[field]) else "":
                    self.carried.append((a, (field, part), 0))
            if a < reach - 1:
                self.carried += [(a, None, 0), (a, None, 1)]

    def rows(self, ref, field, l):
        return jnp.concatenate(
            [
                ref[self.at[field, part], l]
                for part in ("oab" if field in self.tall else "on")
            ],
            axis=0,
        )

    def sixteen(self, ref, field, l):
        value = self.rows(ref, field, l)
        return sixteen(value) if field in self.tall else value


def lanes(shape):
    return lax.broadcasted_iota(jnp.int32, shape, len(shape) - 1)


def lower_rows(shape):
    return lax.broadcasted_iota(jnp.int32, shape, 0) < ROWS // 2


def around(above, below):
    return jnp.where(lower_rows(above.shape), above, below)


def sixteen(value):
    return jnp.concatenate(
        [value[0:ROWS], around(value[ROWS : 2 * ROWS], value[2 * ROWS :])], axis=0
    )


def raw_tile(refs, field, part, k):
    own, above, below = refs
    if part == "o":
        return own[field, k]
    if part == "n":
        return around(above[field, k], below[field, k])
    return (above if part == "a" else below)[field, k]


SHARED = {C: (1, 0), U: (1, 1), V: (2, 0), W: (2, 1)}


def shared_rows(read):
    down, up = [read(PR)], [read(PR)]
    for first, second in ((C, U), (V, W)):
        one, other = read(first), pltpu.roll(read(second), ROWS // 2, 0)
        down.append(around(one, other))
        up.append(around(other, one))
    return down, up


def shared_tile(refs, field, part, k):
    own, above, below = refs
    if part == "o":
        return own[field, k]
    if part == "n" and field == PR:
        return around(above[0, k], below[0, k])
    if part == "n":
        index, half = SHARED[field]
        if half == 0:
            return around(above[index, k], below[index, k])
        return pltpu.roll(around(below[index, k], above[index, k]), ROWS // 2, 0)
    return (above if part == "a" else below)[0, k]


THREE, TWO, ONE = "oab", "on", "o"
FIRST = Plan(
    (C, PR, V),
    7,
    {
        C: [THREE] + [TWO] * 4 + [ONE],
        PR: [THREE] * 2 + [TWO] * 4 + [ONE],
        U: [TWO] * 3 + [ONE],
        V: [TWO] * 4,
        W: [TWO] * 4 + [ONE],
    },
)
SECOND = Plan(
    (PR,),
    6,
    {
        C: [TWO] * 3 + [ONE],
        PR: [THREE] + [TWO] * 4 + [ONE],
        U: [TWO] * 3,
        V: [TWO] * 3,
        W: [TWO] * 3 + [ONE],
    },
)
TILE_OF = {FIRST: raw_tile, SECOND: shared_tile}


SPARE = 104


def pack_columns(plan, with_speed):
    def kernel(own, above, below, *rest):
        to_left, to_right = rest[-2:]
        lane = lanes((ROWS, COLS))
        filler = jnp.zeros((ROWS, COLS), F32)
        if with_speed:
            filler = filler + jnp.max(rest[0][...])

        def one(k, _):
            left = filler
            right = filler
            for n, (field, part) in enumerate(plan.tiles):
                start = n * EDGE
                here = (lane >= start) & (lane < start + EDGE)
                value = TILE_OF[plan]((own, above, below), field, part, k)
                first = pltpu.roll(value, start, 1) if start else value
                last = pltpu.roll(value, (start + EDGE) % COLS, 1)
                left = jnp.where(here, first, left)
                right = jnp.where(here, last, right)
            to_left[k] = left
            to_right[k] = right
            return 0

        def some(levels, _):
            for k in levels:
                one(k, 0)
            return 0

        sweep(0, LEVELS, 8, some)

    return kernel


def halo_columns(from_right, from_left, n):
    start = n * EDGE
    right = pltpu.roll(from_right, COLS - start, 1) if start else from_right
    left = pltpu.roll(from_left, (COLS - EDGE - start) % COLS, 1)
    return jnp.where(lanes((ROWS, COLS)) < COLS // 2, right, left)


def pack_levels(plan, with_speed):
    def kernel(own, above, below, from_right, from_left, *rest):
        if with_speed:
            speed, to_down, to_up, speeds = rest
            near = jnp.maximum(from_right[0], from_left[0])
            near = jnp.where(lanes((ROWS, COLS)) < SPARE, 0.0, near)
            top = jnp.maximum(jnp.max(near), jnp.max(speed[...]))
            speeds[...] = jnp.broadcast_to(top, speeds.shape)
        else:
            to_down, to_up = rest
        for index, (a, tile, side) in enumerate(plan.carried):
            for out, k in ((to_down, a), (to_up, LEVELS - 1 - a)):
                if tile:
                    out[index] = TILE_OF[plan]((own, above, below), *tile, k)
                else:
                    out[index] = (from_left if side else from_right)[k]

    return kernel


def place_own(plan, refs, ext):
    own, above, below, from_right, from_left = refs

    def middle(levels, _):
        for k in levels:
            right, left = from_right[k], from_left[k]
            for n, (field, part) in enumerate(plan.tiles):
                ext[n, REACH + k, :, 0:COLS] = TILE_OF[plan]((own, above, below), field, part, k)
                ext[n, REACH + k, :, COLS:WIDE] = halo_columns(right, left, n)
        return 0

    sweep(0, LEVELS, 4, middle)


def place_halo(plan, from_up, from_down, ext, place, last):
    columns = {(a, side): i for i, (a, tile, side) in enumerate(plan.carried) if not tile}
    for message, level, there in (
        (from_down, lambda a: REACH - 1 - a, place > 0),
        (from_up, lambda a: REACH + LEVELS + a, place < last),
    ):
        keep = jnp.where(there, 1.0, 0.0).astype(F32)
        for index, (a, tile, _) in enumerate(plan.carried):
            if not tile:
                continue
            field, part = tile
            value = message[index] * keep
            for kept in "ab" if part == "n" and field in plan.tall else part:
                n = plan.at[field, kept]
                ext[n, level(a), :, 0:COLS] = value
                if (a, 0) in columns:
                    ext[n, level(a), :, COLS:WIDE] = (
                        halo_columns(message[columns[a, 0]], message[columns[a, 1]], n) * keep
                    )


def shift(value, by, axis):
    return pltpu.roll(value, (-by) % value.shape[axis], axis)


def face_flux(q, wind):
    central = 37.0 * (q[2] + q[3]) - 8.0 * (q[1] + q[4]) + (q[0] + q[5])
    upwind = 10.0 * (q[3] - q[2]) - 5.0 * (q[4] - q[1]) + (q[5] - q[0])
    return wind * central - jnp.abs(wind) * upwind


def flat_flux(q, wind, axis):
    flux = face_flux([shift(q, by, axis) if by else q for by in range(-2, 4)], wind)
    return flux - shift(flux, -1, axis)


def rows_flux(q, wind):
    if wind.shape[0] == 24:
        return sixteen(flat_flux(q, wind, 0))
    if q.shape[0] == 24:
        flux = face_flux([sixteen(shift(q, by, 0) if by else q) for by in range(-2, 4)], wind)
        return flux - shift(flux, -1, 0)
    return flat_flux(q, wind, 0)


def level_flux(read, wind, l):
    return face_flux([read(l + by) for by in range(-2, 4)], wind)


def in_domain(l, place, last, lid):
    g = place * LEVELS + l - REACH
    top = (last + 1) * LEVELS - (1 if lid else 0)
    return jnp.where((g >= 0) & (g < top), 1.0, 0.0).astype(F32)


SIXTIETH = -1.0 / 60.0


def sweep(first, count, most, body, carry=0):
    size = max(n for n in range(1, most + 1) if count % n == 0)

    def run(i, carry):
        start = first + i * size
        return body([start + n for n in range(size)], carry)

    return lax.fori_loop(0, count // size, run, carry)


def flat_part(plan, ext, field, l):
    return flat_flux(plan.sixteen(ext, field, l), plan.sixteen(ext, U, l), 1) + rows_flux(
        plan.rows(ext, field, l), plan.rows(ext, V, l)
    )


def flat_own(plan, ext, fields, flat):
    def some(levels, _):
        results = [(n, l, flat_part(plan, ext, f, l)) for l in levels for n, f in enumerate(fields)]
        for n, l, value in results:
            flat[n, l - REACH] = value
        return 0

    sweep(REACH, LEVELS, 4, some)


def rates(plan, ext, fields, write, around_own, most, flat=None):
    reads = [lambda l, f=f: plan.sixteen(ext, f, l) for f in fields]

    def some(levels, lows, flat=None):
        results = []
        for l in levels:
            w = plan.sixteen(ext, W, l)
            highs = []
            for n, f in enumerate(fields):
                high = level_flux(reads[n], w, l)
                level = flat[n, l - REACH] if flat is not None else flat_part(plan, ext, f, l)
                results.append((n, l, (level + (high - lows[n])) * SIXTIETH))
                highs.append(high)
            lows = tuple(highs)
        for result in results:
            write(*result)
        return lows

    first = REACH - around_own
    w = plan.sixteen(ext, W, first - 1)
    lows = tuple(level_flux(read, w, first - 1) for read in reads)
    if flat is None:
        sweep(first, LEVELS + 2 * around_own, most, some, lows)
        return
    lows = sweep(first, around_own, most, some, lows)
    lows = sweep(REACH, LEVELS, 4, lambda levels, c: some(levels, c, flat), lows)
    sweep(REACH + LEVELS, around_own, most, some, lows)


def first_own(place_ref, own, above, below, from_right, from_left, ext, flat):
    place_own(FIRST, (own, above, below, from_right, from_left), ext)

    @pl.when(place_ref[0] == place_ref[1])
    def _():
        for part in "on":
            ext[FIRST.at[W, part], REACH + LEVELS - 1] = jnp.zeros((ROWS, WIDE), F32)

    flat_own(FIRST, ext, (C, PR), flat)


def acoustic(p, u, v, w, read_c, rate, step, first, count, place, last):
    pull = step * sound_speed

    def level(value):
        return sixteen(value) if value.shape[0] == 24 else value

    def wind_w(l, lift_low, lift_high, p_here, p_above):
        lift = (buoyancy * 0.5) * (lift_low + lift_high)
        return (w[0](l) + step * lift - pull * (p_above - p_here)) * in_domain(l, place, last, True)

    def some(levels, w_low):
        talls = [p[0](l) for l in (*levels, levels[-1] + 1)]
        cells = [level(value) for value in talls]
        warm = [read_c(l) for l in (*levels, levels[-1] + 1)]
        results = []
        for n, l in enumerate(levels):
            p_here = cells[n]
            w_new = wind_w(l, warm[n], warm[n + 1], p_here, cells[n + 1])
            u_new = u[0](l) - pull * (shift(p_here, 1, 1) - p_here)
            v_old = v[0](l)
            if v_old.shape[0] == 24:
                v_tall = v_old - pull * (shift(talls[n], 1, 0) - talls[n])
                v_new, v_flow = sixteen(v_tall), sixteen(v_tall - shift(v_tall, -1, 0))
            else:
                v_new = v_old - pull * (shift(p_here, 1, 0) - p_here)
                v_flow = v_new - shift(v_new, -1, 0)
            divergence = (u_new - shift(u_new, -1, 1)) + v_flow + (w_new - w_low)
            p_new = (p_here + step * rate(l) - pull * divergence) * in_domain(
                l, place, last, False
            )
            results.append((l, p_new, u_new, v_new, w_new))
            w_low = w_new
        for l, *news in results:
            for target, value in zip((p, u, v, w), news):
                target[1](l, value)
        return w_low

    low = first - 1
    w_low = wind_w(low, read_c(low), read_c(first), level(p[0](low)), level(p[0](first)))
    w[1](low, w_low)
    sweep(first, count, 12, some, w_low)


def access(ref, *lead):
    def read(l):
        return ref[(*lead, l)]

    def write(l, value):
        ref[(*lead, l)] = value

    return read, write


def begin(start, field, tall=False):
    return lambda l: (FIRST.rows if tall else FIRST.sixteen)(start, field, l)


def own_write(ref, field):
    def write(l, value):
        if not isinstance(l, int):
            ref[field, l - REACH] = value[0:ROWS, 0:COLS]

    return write


def tracer_flat(tiles, u, v, l):
    rows = flat_flux(tiles(l)[:, 0:COLS], v(l)[:, 0:COLS], 0)[0:ROWS]
    return rows + flat_flux(tiles(l)[0:ROWS], u(l)[0:ROWS], 1)[:, 0:COLS]


def tracer_high(tiles, w, l):
    return level_flux(lambda m: tiles(m)[0:ROWS, 0:COLS], w(l)[0:ROWS, 0:COLS], l)


def two_sections(
    place_ref,
    speed,
    other_speed,
    start_in,
    flat,
    from_up,
    from_down,
    start,
    s2,
    down,
    up,
    dt_out,
    rate0,
    s1,
    rate1,
    fast,
):
    place, last = place_ref[0], place_ref[1]
    place_halo(FIRST, from_up, from_down, start, place, last)

    def write0(n, l, value):
        rate0[n, l] = value

    rates(FIRST, start, (C, PR), write0, 4, 4, flat)
    dt = courant_goal / (1.0 + jnp.max(jnp.maximum(speed[...], other_speed[...])))
    dt_out[0] = dt
    third = dt * (1.0 / 3.0)

    def tracer(levels, _):
        for l in levels:
            s1[C, l] = (FIRST.sixteen(start, C, l) + third * rate0[0, l]) * in_domain(
                l, place, last, False
            )
        return 0

    sweep(REACH - 4, LEVELS + 8, 4, tracer)
    acoustic(
        (begin(start, PR, True), access(s1, PR)[1]),
        (begin(start, U), access(s1, U)[1]),
        (begin(start, V, True), access(s1, V)[1]),
        (begin(start, W), access(s1, W)[1]),
        begin(start, C),
        access(rate0, 1)[0],
        third,
        REACH - 4,
        LEVELS + 8,
        place,
        last,
    )
    half = dt * 0.5
    tiles = access(s1, C)[0]
    winds = [access(s1, f)[0] for f in (U, V, W)]

    def own_tracer(levels, low):
        results = []
        for l in levels:
            high = tracer_high(tiles, winds[2], l)
            tendency = (tracer_flat(tiles, *winds[:2], l) + (high - low)) * SIXTIETH
            low = high
            results.append(start[FIRST.at[C, "o"], l, :, 0:COLS] + half * tendency)
        for l, value in zip(levels, results):
            s2[C, l - REACH] = value
        return low

    sweep(REACH, LEVELS, 8, own_tracer, tracer_high(tiles, winds[2], REACH - 1))

    def write(n, l, value):
        rate1[l] = value

    rates(SECTION, s1, (PR,), write, 1, 6)
    step = half / (NS // 2)
    acoustic(
        (begin(start, PR), access(fast, 0)[1]),
        (begin(start, U), access(fast, 1)[1]),
        (begin(start, V), access(fast, 2)[1]),
        (begin(start, W), access(fast, 3)[1]),
        access(s1, C)[0],
        access(rate1)[0],
        step,
        REACH - 1,
        LEVELS + 2,
        place,
        last,
    )
    acoustic(
        (access(fast, 0)[0], own_write(s2, PR)),
        (access(fast, 1)[0], own_write(s2, U)),
        (access(fast, 2)[0], own_write(s2, V)),
        (access(fast, 3)[0], own_write(s2, W)),
        access(s1, C)[0],
        access(rate1)[0],
        step,
        REACH,
        LEVELS,
        place,
        last,
    )

    def share(levels, _):
        made = [shared_rows(lambda f, k=k: s2[f, k]) for k in levels]
        for k, (to_down, to_up) in zip(levels, made):
            for n in range(3):
                down[n, k] = to_down[n]
                up[n, k] = to_up[n]
        return 0

    sweep(0, LEVELS, 4, share)


class Whole:
    def rows(self, ref, field, l):
        return ref[field, l]

    sixteen = rows


SECTION = Whole()


def second_own(own, above, below, from_right, from_left, ext, flat, tracer):
    place_own(SECOND, (own, above, below, from_right, from_left), ext)
    flat_own(SECOND, ext, (PR,), flat)
    tiles, u, v = (lambda l, f=f: SECOND.rows(ext, f, l) for f in (C, U, V))

    def some(levels, _):
        results = [tracer_flat(tiles, u, v, l) for l in levels]
        for l, value in zip(levels, results):
            tracer[l - REACH] = value
        return 0

    sweep(REACH, LEVELS, 4, some)


def last_tracer(
    place_ref, dt_ref, ext_in, flat, flat_tracer, from_up, from_down, initial, *rest
):
    *chunks, ext, tracer, landed, fallen, rate, warm, factor, by_depth, sem = rest
    dt = dt_ref[0]
    copies, first = [], 0
    for n, chunk in enumerate(chunks):
        there = by_depth.at[pl.ds(first, chunk.shape[0])]
        copies.append(pltpu.make_async_copy(chunk, there, sem.at[n]))
        first += chunk.shape[0]
    for copy in copies:
        copy.start()
    place_halo(SECOND, from_up, from_down, ext, place_ref[0], place_ref[1])

    def write(n, l, value):
        rate[l] = value

    rates(SECOND, ext, (PR,), write, 3, 3, flat)

    def keep(levels, _):
        for l in levels:
            warm[l] = SECOND.rows(ext, C, l)
        return 0

    sweep(REACH - 4, LEVELS + 8, 4, keep)
    tiles = lambda l: SECOND.rows(ext, C, l)
    w = lambda l: SECOND.rows(ext, W, l)

    def some(levels, low):
        results = []
        for l in levels:
            high = tracer_high(tiles, w, l)
            tendency = (flat_tracer[l - REACH] + (high - low)) * SIXTIETH
            low = high
            c = initial[C, l - REACH] + dt * tendency
            grown = jnp.exp(growth * c)
            results.append((c, grown, grown * jnp.exp((0.5 * growth) * c)))
        for l, (c, second, third) in zip(levels, results):
            tracer[l - REACH] = c
            factor[0, l - REACH] = second
            factor[1, l - REACH] = third
        return low

    sweep(REACH, LEVELS, 4, some, tracer_high(tiles, w, REACH - 1))
    for copy in copies:
        copy.wait()
    for target in range(-FMAX, LEVELS):
        for moment in range(3):
            total = None
            for depth in range(FMAX + 1):
                k = target + depth
                if 0 <= k < LEVELS:
                    value = by_depth[k, depth, moment]
                    if moment:
                        value = value * factor[moment - 1, k]
                    total = value if total is None else total + value
            if target < 0:
                fallen[moment, target + FMAX] = total
            else:
                landed[moment, target] = total


def last_section(place_ref, dt_ref, rate, warm, start, tracer, out, fast):
    place, last = place_ref[0], place_ref[1]
    step = dt_ref[0] / NS
    out[C] = tracer[...]
    names = (PR, U, V, W)
    for repeat in range(NS):
        reads = [
            begin(start, f) if repeat == 0 else access(fast, n)[0] for n, f in enumerate(names)
        ]
        writes = [
            own_write(out, f) if repeat == NS - 1 else access(fast, n)[1]
            for n, f in enumerate(names)
        ]
        acoustic(
            *zip(reads, writes),
            access(warm)[0],
            access(rate)[0],
            step,
            REACH - 3 + repeat,
            LEVELS + 6 - 2 * repeat,
            place,
            last,
        )


def land(place_ref, landed, arrived, out):
    keep = jnp.where(place_ref[0] < place_ref[1], 1.0, 0.0).astype(F32)
    out[:, 0 : LEVELS - FMAX] = landed[:, 0 : LEVELS - FMAX]
    out[:, LEVELS - FMAX :] = landed[:, LEVELS - FMAX :] + keep * arrived[...]


def deposit(radius, weight, column, counts, fall_depth, out):
    slots, levels = radius.shape[0], radius.shape[1]
    target = lax.broadcasted_iota(jnp.int32, (COLS, COLS), 0)
    row = lax.broadcasted_iota(jnp.int32, (ROWS, COLS), 0)
    per_step = 4

    for k in range(levels):
        out[k] = jnp.zeros(out.shape[1:], F32)
        live = counts[k]

        def some(step, _, k=k, live=live):
            sums = [[None] * 3 for _ in range(FMAX + 1)]
            for part in range(per_step):
                s = step * per_step + part
                r = radius[s, k]
                number = jnp.where(s < live, weight[s, k], 0.0)
                area = number * r * r
                terms = []
                for t in (number, area, area * r):
                    high = t.astype(jnp.bfloat16).astype(F32)
                    terms += [high, t - high]
                cols = column[s, k]
                left, right = [], []
                for j in range(ROWS):
                    left.append(
                        jnp.concatenate([jnp.where(row == j, t, 0.0) for t in terms], axis=0)
                    )
                    right.append(jnp.where(cols[j : j + 1] == target, 1.0, 0.0).astype(F32))
                sent = lax.dot_general(
                    jnp.concatenate(left, axis=1),
                    jnp.concatenate(right, axis=1),
                    (((1,), (1,)), ((), ())),
                    preferred_element_type=F32,
                )
                depth = jnp.broadcast_to(fall_depth[s, k], (ROWS, COLS))
                for d in range(FMAX + 1):
                    falls = depth == d
                    for m in range(3):
                        both = sent[16 * m : 16 * m + 8] + sent[16 * m + 8 : 16 * m + 16]
                        value = jnp.where(falls, both, 0.0)
                        sums[d][m] = value if sums[d][m] is None else sums[d][m] + value
            for d in range(FMAX + 1):
                for m in range(3):
                    out[k, d, m] += sums[d][m]
            return 0

        lax.fori_loop(0, slots // per_step, some, 0)


def vmem(n):
    return [pl.BlockSpec(memory_space=pltpu.VMEM)] * n


def smem(n):
    return [pl.BlockSpec(memory_space=pltpu.SMEM)] * n


def far(n):
    return [pl.BlockSpec(memory_space=pltpu.HBM)] * n


def shaped(*dims):
    return jax.ShapeDtypeStruct(dims, F32)


def held(*dims):
    return pltpu.VMEM(dims, F32)


def call(kernel, name, ins, outs, scratch=(), out_specs=None, flops=None, grant=4, alias=None):
    made = pl.pallas_call(
        kernel,
        name=name,
        in_specs=ins,
        out_specs=tuple(out_specs or vmem(len(outs))),
        out_shape=tuple(outs),
        scratch_shapes=list(scratch),
        input_output_aliases=alias or {},
        compiler_params=pltpu.CompilerParams(vmem_limit_bytes=grant << 20),
        cost_estimate=(
            pl.CostEstimate(flops=flops, bytes_accessed=0, transcendentals=0) if flops else None
        ),
    )

    def run(*operands):
        return made(
            *(
                pltpu.with_memory_space_constraint(value, spec.memory_space)
                if spec.memory_space != pltpu.SMEM
                else value
                for spec, value in zip(ins, operands)
            )
        )

    return run


def both_ways(down, axis, up):
    count = lax.axis_size(axis)
    return (
        lax.ppermute(down, axis, [((i + 1) % count, i) for i in range(count)]),
        lax.ppermute(up, axis, [(i, (i + 1) % count) for i in range(count)]),
    )


def exchange(plan, own, down, up, tokens=(), speed=None):
    above, below = both_ways(down, GY, up)
    extra = [] if speed is None else [speed]
    to_left, to_right = call(
        pack_columns(plan, bool(extra)),
        "pack_columns",
        vmem(3 + len(extra)) + far(len(tokens)),
        [held(LEVELS, ROWS, COLS)] * 2,
    )(own, above, below, *extra, *tokens)
    from_right, from_left = both_ways(to_left, "gx", to_right)
    tiles = len(plan.carried)
    to_down, to_up, *speeds = call(
        pack_levels(plan, bool(extra)),
        "pack_levels",
        vmem(5 + len(extra)),
        [held(tiles, ROWS, COLS)] * 2 + [held(ROWS, COLS)] * len(extra),
    )(own, above, below, from_right, from_left, *extra)
    from_up, from_down = both_ways(to_down, "gz", to_up)
    return above, below, from_right, from_left, from_up, from_down, to_down, *speeds


def prepare(place_ref, fields, speed, winds, sem):
    copy = pltpu.make_async_copy(fields.at[pl.ds(U, 3)], winds, sem)
    copy.start()
    copy.wait()
    keep = jnp.where(place_ref[0] == place_ref[1], 0.0, 1.0).astype(F32)
    most = jnp.zeros((ROWS, COLS), F32)
    for k in range(LEVELS):
        w = jnp.abs(winds[2, k])
        if k == LEVELS - 1:
            w = w * keep
        most = jnp.maximum(most, jnp.abs(winds[0, k]) + jnp.abs(winds[1, k]) + w)
    speed[...] = jnp.broadcast_to(jnp.max(most), speed.shape)


def hold(fields, own, sem):
    copy = pltpu.make_async_copy(fields, own, sem)
    copy.start()
    copy.wait()


def droplets(radius, weight, column, counts, fall_depth, first, count, after):
    slots, step = radius.shape[0], 2
    counts, _ = lax.optimization_barrier((counts, after))
    whole = pl.BlockSpec((slots, step, ROWS, COLS), lambda i: (0, first // step + i, 0, 0))
    return pl.pallas_call(
        deposit,
        name="deposit",
        grid=(count // step,),
        in_specs=[
            whole,
            whole,
            whole,
            pl.BlockSpec((step, ROWS, COLS), lambda i: (first // step + i, 0, 0)),
            pl.BlockSpec((slots, step, ROWS, 1), lambda i: (0, first // step + i, 0, 0)),
        ],
        out_specs=pl.BlockSpec((step, FMAX + 1, 3, ROWS, COLS), lambda i: (i, 0, 0, 0, 0)),
        out_shape=pltpu.HBM((count, FMAX + 1, 3, ROWS, COLS), F32),
        compiler_params=pltpu.CompilerParams(vmem_limit_bytes=12 << 20),
        cost_estimate=pl.CostEstimate(
            flops=100_000_000 * count, bytes_accessed=0, transcendentals=0
        ),
    )(
        *(
            pltpu.with_memory_space_constraint(value, pltpu.HBM)
            for value in (radius, weight, column, counts)
        ),
        fall_depth,
    )


def per_device(fields, radius, weight, column, counts, fall_depth):
    place = lax.axis_index("gz")
    last = lax.axis_size("gz") - 1
    where = jnp.stack([place, jnp.int32(last)]).astype(jnp.int32)
    def drops(first, count, after):
        return droplets(radius, weight, column, counts, fall_depth, first, count, after)

    plane = ("gy_hi", "gz")
    (speed,) = call(
        prepare,
        "prepare",
        smem(1) + far(1),
        [shaped(lax.axis_size(plane), 1, COLS)],
        scratch=[pltpu.VMEM((3, LEVELS, ROWS, COLS), F32), pltpu.SemaphoreType.DMA],
    )(where, fields)
    pair = [(i, i ^ 1) for i in range(lax.axis_size("gx"))]
    speed = jnp.maximum(speed, lax.ppermute(speed, "gx", pair))
    (own,) = call(
        hold,
        "hold",
        far(1),
        [held(5, LEVELS, ROWS, COLS)],
        scratch=[pltpu.SemaphoreType.DMA],
    )(lax.optimization_barrier((fields, speed))[0])
    early = drops(0, 8, own)
    speed = jnp.max(lax.all_to_all(speed, plane, 0, 0), axis=0)
    *near, from_up, from_down, _, speed = exchange(FIRST, own, fields, fields, [early], speed)
    other_speed = lax.ppermute(speed, "gy_lo", [(0, 1), (1, 0)])
    ext = held(len(FIRST.tiles), DEPTH, ROWS, WIDE)
    start, flat = call(
        first_own,
        "first_own",
        smem(1) + vmem(5),
        [ext, held(2, LEVELS, 2 * ROWS, WIDE)],
    )(where, own, *near)
    start, s2, down, up, dt = call(
        two_sections,
        "two_sections",
        smem(1) + vmem(6),
        [ext, held(5, LEVELS, ROWS, COLS)] + [held(3, LEVELS, ROWS, COLS)] * 2 + [shaped(1)],
        scratch=[
            pltpu.VMEM((2, DEPTH, 2 * ROWS, WIDE), F32),
            pltpu.VMEM((5, DEPTH, 2 * ROWS, WIDE), F32),
            pltpu.VMEM((DEPTH, 2 * ROWS, WIDE), F32),
            pltpu.VMEM((4, DEPTH, 2 * ROWS, WIDE), F32),
        ],
        out_specs=vmem(4) + smem(1),
        grant=12,
        alias={3: 0},
    )(where, speed, other_speed, start, flat, from_up, from_down)
    middle = drops(8, 6, s2)
    *near, from_up, from_down, sent = exchange(SECOND, s2, down, up, [middle])
    by_depth = [early, middle, drops(14, 2, sent)]
    ext = held(len(SECOND.tiles), DEPTH, ROWS, WIDE)
    around_s2, flat, flat_tracer = call(
        second_own,
        "second_own",
        vmem(5),
        [ext, held(1, LEVELS, 2 * ROWS, WIDE), held(LEVELS, ROWS, COLS)],
        flops=1_000_000_000,
    )(s2, *near)
    rows = held(DEPTH, 2 * ROWS, WIDE)
    _, tracer, landed, fallen, rate, warm = call(
        last_tracer,
        "last_tracer",
        smem(2) + vmem(6) + far(len(by_depth)),
        [
            ext,
            held(LEVELS, ROWS, COLS),
            held(3, LEVELS, ROWS, COLS),
            held(3, FMAX, ROWS, COLS),
            rows,
            rows,
        ],
        scratch=[
            pltpu.VMEM((2, LEVELS, ROWS, COLS), F32),
            pltpu.VMEM((LEVELS, FMAX + 1, 3, ROWS, COLS), F32),
            pltpu.SemaphoreType.DMA((len(by_depth),)),
        ],
        alias={2: 0},
    )(where, dt, around_s2, flat, flat_tracer, from_up, from_down, own, *by_depth)
    count = lax.axis_size("gz")
    arrived = lax.ppermute(fallen, "gz", [((i + 1) % count, i) for i in range(count)])
    (new_fields,) = call(
        last_section,
        "last_section",
        smem(2) + vmem(4),
        [shaped(5, LEVELS, ROWS, COLS)],
        scratch=[pltpu.VMEM((4, DEPTH, 2 * ROWS, WIDE), F32)],
        flops=1_000_000_000,
    )(where, dt, rate, warm, start, tracer)
    (moments,) = call(
        land, "land", smem(1) + vmem(2), [shaped(3, LEVELS, ROWS, COLS)]
    )(where, landed, arrived)
    return (new_fields, moments)


def solution(mesh):
    count = mesh.shape["gy"]
    split = Mesh(
        mesh.devices.reshape(mesh.shape["gx"], count // 2, 2, mesh.shape["gz"]),
        ("gx", *GY, "gz"),
    )
    spread = P(None, "gz", GY, "gx")
    return jax.shard_map(
        per_device,
        mesh=split,
        in_specs=(spread, spread, spread, spread, P("gz", GY, "gx"), spread),
        out_specs=(spread, spread),
        check_vma=False,
    )
```

```python
import jax
import jax.numpy as jnp
from jax import lax
from jax.experimental import pallas as pl
from jax.experimental.pallas import tpu as pltpu
from jax.sharding import Mesh
from jax.sharding import PartitionSpec as P

NS = 4
FMAX = 8
GY = ("gy_hi", "gy_lo")

sound_speed = 10.0
buoyancy = 0.5
courant_goal = 0.6
growth = 0.3

LEVELS, ROWS, COLS = 16, 8, 128
WIDE = 2 * COLS
REACH = 7
DEPTH = LEVELS + 2 * REACH
EDGE = 8
F32 = jnp.float32
C, PR, U, V, W = range(5)


class Plan:
    def __init__(self, tall, reach, sent):
        self.tall, self.reach = tall, reach
        self.tiles = [
            (field, part)
            for field in range(5)
            for part in ("oab" if field in tall else "on")
        ]
        self.at = {tile: n for n, tile in enumerate(self.tiles)}
        self.carried = []
        for a in range(reach):
            for field in range(5):
                for part in sent[field][a] if a < len(sent[field]) else "":
                    self.carried.append((a, (field, part), 0))
            if a < reach - 1:
                self.carried += [(a, None, 0), (a, None, 1)]

    def rows(self, ref, field, l):
        return jnp.concatenate(
            [
                ref[self.at[field, part], l]
                for part in ("oab" if field in self.tall else "on")
            ],
            axis=0,
        )

    def sixteen(self, ref, field, l):
        value = self.rows(ref, field, l)
        return sixteen(value) if field in self.tall else value


def lanes(shape):
    return lax.broadcasted_iota(jnp.int32, shape, len(shape) - 1)


def lower_rows(shape):
    return lax.broadcasted_iota(jnp.int32, shape, 0) < ROWS // 2


def around(above, below):
    return jnp.where(lower_rows(above.shape), above, below)


def sixteen(value):
    return jnp.concatenate(
        [value[0:ROWS], around(value[ROWS : 2 * ROWS], value[2 * ROWS :])], axis=0
    )


def raw_tile(refs, field, part, k):
    own, above, below = refs
    if part == "o":
        return own[field, k]
    if part == "n":
        return around(above[field, k], below[field, k])
    return (above if part == "a" else below)[field, k]


SHARED = {C: (1, 0), U: (1, 1), V: (2, 0), W: (2, 1)}


def shared_rows(read):
    down, up = [read(PR)], [read(PR)]
    for first, second in ((C, U), (V, W)):
        one, other = read(first), pltpu.roll(read(second), ROWS // 2, 0)
        down.append(around(one, other))
        up.append(around(other, one))
    return down, up


def shared_tile(refs, field, part, k):
    own, above, below = refs
    if part == "o":
        return own[field, k]
    if part == "n" and field == PR:
        return around(above[0, k], below[0, k])
    if part == "n":
        index, half = SHARED[field]
        if half == 0:
            return around(above[index, k], below[index, k])
        return pltpu.roll(around(below[index, k], above[index, k]), ROWS // 2, 0)
    return (above if part == "a" else below)[0, k]


THREE, TWO, ONE = "oab", "on", "o"
FIRST = Plan(
    (C, PR, V),
    7,
    {
        C: [THREE] + [TWO] * 4 + [ONE],
        PR: [THREE] * 2 + [TWO] * 4 + [ONE],
        U: [TWO] * 3 + [ONE],
        V: [TWO] * 4,
        W: [TWO] * 4 + [ONE],
    },
)
SECOND = Plan(
    (PR,),
    6,
    {
        C: [TWO] * 3 + [ONE],
        PR: [THREE] + [TWO] * 4 + [ONE],
        U: [TWO] * 3,
        V: [TWO] * 3,
        W: [TWO] * 3 + [ONE],
    },
)
TILE_OF = {FIRST: raw_tile, SECOND: shared_tile}


SPARE = 104


def pack_columns(plan, with_speed):
    def kernel(own, above, below, *rest):
        to_left, to_right = rest[-2:]
        lane = lanes((ROWS, COLS))
        filler = jnp.zeros((ROWS, COLS), F32)
        if with_speed:
            filler = filler + jnp.max(rest[0][...])

        def one(k, _):
            left = filler
            right = filler
            for n, (field, part) in enumerate(plan.tiles):
                start = n * EDGE
                here = (lane >= start) & (lane < start + EDGE)
                value = TILE_OF[plan]((own, above, below), field, part, k)
                first = pltpu.roll(value, start, 1) if start else value
                last = pltpu.roll(value, (start + EDGE) % COLS, 1)
                left = jnp.where(here, first, left)
                right = jnp.where(here, last, right)
            to_left[k] = left
            to_right[k] = right
            return 0

        def some(levels, _):
            for k in levels:
                one(k, 0)
            return 0

        sweep(0, LEVELS, 8, some)

    return kernel


def halo_columns(from_right, from_left, n):
    start = n * EDGE
    right = pltpu.roll(from_right, COLS - start, 1) if start else from_right
    left = pltpu.roll(from_left, (COLS - EDGE - start) % COLS, 1)
    return jnp.where(lanes((ROWS, COLS)) < COLS // 2, right, left)


def pack_levels(plan, with_speed):
    def kernel(own, above, below, from_right, from_left, *rest):
        if with_speed:
            speed, to_down, to_up, speeds = rest
            near = jnp.maximum(from_right[0], from_left[0])
            near = jnp.where(lanes((ROWS, COLS)) < SPARE, 0.0, near)
            top = jnp.maximum(jnp.max(near), jnp.max(speed[...]))
            speeds[...] = jnp.broadcast_to(top, speeds.shape)
        else:
            to_down, to_up = rest
        for index, (a, tile, side) in enumerate(plan.carried):
            for out, k in ((to_down, a), (to_up, LEVELS - 1 - a)):
                if tile:
                    out[index] = TILE_OF[plan]((own, above, below), *tile, k)
                else:
                    out[index] = (from_left if side else from_right)[k]

    return kernel


def place_own(plan, refs, ext):
    own, above, below, from_right, from_left = refs

    def middle(levels, _):
        for k in levels:
            right, left = from_right[k], from_left[k]
            for n, (field, part) in enumerate(plan.tiles):
                ext[n, REACH + k, :, 0:COLS] = TILE_OF[plan]((own, above, below), field, part, k)
                ext[n, REACH + k, :, COLS:WIDE] = halo_columns(right, left, n)
        return 0

    sweep(0, LEVELS, 4, middle)


def place_halo(plan, from_up, from_down, ext, place, last):
    columns = {(a, side): i for i, (a, tile, side) in enumerate(plan.carried) if not tile}
    for message, level, there in (
        (from_down, lambda a: REACH - 1 - a, place > 0),
        (from_up, lambda a: REACH + LEVELS + a, place < last),
    ):
        keep = jnp.where(there, 1.0, 0.0).astype(F32)
        for index, (a, tile, _) in enumerate(plan.carried):
            if not tile:
                continue
            field, part = tile
            value = message[index] * keep
            for kept in "ab" if part == "n" and field in plan.tall else part:
                n = plan.at[field, kept]
                ext[n, level(a), :, 0:COLS] = value
                if (a, 0) in columns:
                    ext[n, level(a), :, COLS:WIDE] = (
                        halo_columns(message[columns[a, 0]], message[columns[a, 1]], n) * keep
                    )


def shift(value, by, axis):
    return pltpu.roll(value, (-by) % value.shape[axis], axis)


def face_flux(q, wind):
    central = 37.0 * (q[2] + q[3]) - 8.0 * (q[1] + q[4]) + (q[0] + q[5])
    upwind = 10.0 * (q[3] - q[2]) - 5.0 * (q[4] - q[1]) + (q[5] - q[0])
    return wind * central - jnp.abs(wind) * upwind


def flat_flux(q, wind, axis):
    flux = face_flux([shift(q, by, axis) if by else q for by in range(-2, 4)], wind)
    return flux - shift(flux, -1, axis)


def rows_flux(q, wind):
    if wind.shape[0] == 24:
        return sixteen(flat_flux(q, wind, 0))
    if q.shape[0] == 24:
        flux = face_flux([sixteen(shift(q, by, 0) if by else q) for by in range(-2, 4)], wind)
        return flux - shift(flux, -1, 0)
    return flat_flux(q, wind, 0)


def level_flux(read, wind, l):
    return face_flux([read(l + by) for by in range(-2, 4)], wind)


def in_domain(l, place, last, lid):
    g = place * LEVELS + l - REACH
    top = (last + 1) * LEVELS - (1 if lid else 0)
    return jnp.where((g >= 0) & (g < top), 1.0, 0.0).astype(F32)


SIXTIETH = -1.0 / 60.0


def sweep(first, count, most, body, carry=0):
    size = max(n for n in range(1, most + 1) if count % n == 0)

    def run(i, carry):
        start = first + i * size
        return body([start + n for n in range(size)], carry)

    return lax.fori_loop(0, count // size, run, carry)


def flat_part(plan, ext, field, l):
    return flat_flux(plan.sixteen(ext, field, l), plan.sixteen(ext, U, l), 1) + rows_flux(
        plan.rows(ext, field, l), plan.rows(ext, V, l)
    )


def flat_own(plan, ext, fields, flat):
    def some(levels, _):
        results = [(n, l, flat_part(plan, ext, f, l)) for l in levels for n, f in enumerate(fields)]
        for n, l, value in results:
            flat[n, l - REACH] = value
        return 0

    sweep(REACH, LEVELS, 4, some)


def rates(plan, ext, fields, write, around_own, most, flat=None):
    reads = [lambda l, f=f: plan.sixteen(ext, f, l) for f in fields]

    def some(levels, lows, flat=None):
        results = []
        for l in levels:
            w = plan.sixteen(ext, W, l)
            highs = []
            for n, f in enumerate(fields):
                high = level_flux(reads[n], w, l)
                level = flat[n, l - REACH] if flat is not None else flat_part(plan, ext, f, l)
                results.append((n, l, (level + (high - lows[n])) * SIXTIETH))
                highs.append(high)
            lows = tuple(highs)
        for result in results:
            write(*result)
        return lows

    first = REACH - around_own
    w = plan.sixteen(ext, W, first - 1)
    lows = tuple(level_flux(read, w, first - 1) for read in reads)
    if flat is None:
        sweep(first, LEVELS + 2 * around_own, most, some, lows)
        return
    lows = sweep(first, around_own, most, some, lows)
    lows = sweep(REACH, LEVELS, 4, lambda levels, c: some(levels, c, flat), lows)
    sweep(REACH + LEVELS, around_own, most, some, lows)


def first_own(place_ref, own, above, below, from_right, from_left, ext, flat):
    place_own(FIRST, (own, above, below, from_right, from_left), ext)

    @pl.when(place_ref[0] == place_ref[1])
    def _():
        for part in "on":
            ext[FIRST.at[W, part], REACH + LEVELS - 1] = jnp.zeros((ROWS, WIDE), F32)

    flat_own(FIRST, ext, (C, PR), flat)


def acoustic(p, u, v, w, read_c, rate, step, first, count, place, last):
    pull = step * sound_speed

    def level(value):
        return sixteen(value) if value.shape[0] == 24 else value

    def wind_w(l, lift_low, lift_high, p_here, p_above):
        lift = (buoyancy * 0.5) * (lift_low + lift_high)
        return (w[0](l) + step * lift - pull * (p_above - p_here)) * in_domain(l, place, last, True)

    def some(levels, w_low):
        talls = [p[0](l) for l in (*levels, levels[-1] + 1)]
        cells = [level(value) for value in talls]
        warm = [read_c(l) for l in (*levels, levels[-1] + 1)]
        results = []
        for n, l in enumerate(levels):
            p_here = cells[n]
            w_new = wind_w(l, warm[n], warm[n + 1], p_here, cells[n + 1])
            u_new = u[0](l) - pull * (shift(p_here, 1, 1) - p_here)
            v_old = v[0](l)
            if v_old.shape[0] == 24:
                v_tall = v_old - pull * (shift(talls[n], 1, 0) - talls[n])
                v_new, v_flow = sixteen(v_tall), sixteen(v_tall - shift(v_tall, -1, 0))
            else:
                v_new = v_old - pull * (shift(p_here, 1, 0) - p_here)
                v_flow = v_new - shift(v_new, -1, 0)
            divergence = (u_new - shift(u_new, -1, 1)) + v_flow + (w_new - w_low)
            p_new = (p_here + step * rate(l) - pull * divergence) * in_domain(
                l, place, last, False
            )
            results.append((l, p_new, u_new, v_new, w_new))
            w_low = w_new
        for l, *news in results:
            for target, value in zip((p, u, v, w), news):
                target[1](l, value)
        return w_low

    low = first - 1
    w_low = wind_w(low, read_c(low), read_c(first), level(p[0](low)), level(p[0](first)))
    w[1](low, w_low)
    sweep(first, count, 12, some, w_low)


def access(ref, *lead):
    def read(l):
        return ref[(*lead, l)]

    def write(l, value):
        ref[(*lead, l)] = value

    return read, write


def begin(start, field, tall=False):
    return lambda l: (FIRST.rows if tall else FIRST.sixteen)(start, field, l)


def own_write(ref, field):
    def write(l, value):
        if not isinstance(l, int):
            ref[field, l - REACH] = value[0:ROWS, 0:COLS]

    return write


def tracer_flat(tiles, u, v, l):
    rows = flat_flux(tiles(l)[:, 0:COLS], v(l)[:, 0:COLS], 0)[0:ROWS]
    return rows + flat_flux(tiles(l)[0:ROWS], u(l)[0:ROWS], 1)[:, 0:COLS]


def tracer_high(tiles, w, l):
    return level_flux(lambda m: tiles(m)[0:ROWS, 0:COLS], w(l)[0:ROWS, 0:COLS], l)


def two_sections(
    place_ref,
    speed,
    other_speed,
    start_in,
    flat,
    from_up,
    from_down,
    start,
    s2,
    down,
    up,
    dt_out,
    rate0,
    s1,
    rate1,
    fast,
):
    place, last = place_ref[0], place_ref[1]
    place_halo(FIRST, from_up, from_down, start, place, last)

    def write0(n, l, value):
        rate0[n, l] = value

    rates(FIRST, start, (C, PR), write0, 4, 4, flat)
    dt = courant_goal / (1.0 + jnp.max(jnp.maximum(speed[...], other_speed[...])))
    dt_out[0] = dt
    third = dt * (1.0 / 3.0)

    def tracer(levels, _):
        for l in levels:
            s1[C, l] = (FIRST.sixteen(start, C, l) + third * rate0[0, l]) * in_domain(
                l, place, last, False
            )
        return 0

    sweep(REACH - 4, LEVELS + 8, 4, tracer)
    acoustic(
        (begin(start, PR, True), access(s1, PR)[1]),
        (begin(start, U), access(s1, U)[1]),
        (begin(start, V, True), access(s1, V)[1]),
        (begin(start, W), access(s1, W)[1]),
        begin(start, C),
        access(rate0, 1)[0],
        third,
        REACH - 4,
        LEVELS + 8,
        place,
        last,
    )
    half = dt * 0.5
    tiles = access(s1, C)[0]
    winds = [access(s1, f)[0] for f in (U, V, W)]

    def own_tracer(levels, low):
        results = []
        for l in levels:
            high = tracer_high(tiles, winds[2], l)
            tendency = (tracer_flat(tiles, *winds[:2], l) + (high - low)) * SIXTIETH
            low = high
            results.append(start[FIRST.at[C, "o"], l, :, 0:COLS] + half * tendency)
        for l, value in zip(levels, results):
            s2[C, l - REACH] = value
        return low

    sweep(REACH, LEVELS, 8, own_tracer, tracer_high(tiles, winds[2], REACH - 1))

    def write(n, l, value):
        rate1[l] = value

    rates(SECTION, s1, (PR,), write, 1, 6)
    step = half / (NS // 2)
    acoustic(
        (begin(start, PR), access(fast, 0)[1]),
        (begin(start, U), access(fast, 1)[1]),
        (begin(start, V), access(fast, 2)[1]),
        (begin(start, W), access(fast, 3)[1]),
        access(s1, C)[0],
        access(rate1)[0],
        step,
        REACH - 1,
        LEVELS + 2,
        place,
        last,
    )
    acoustic(
        (access(fast, 0)[0], own_write(s2, PR)),
        (access(fast, 1)[0], own_write(s2, U)),
        (access(fast, 2)[0], own_write(s2, V)),
        (access(fast, 3)[0], own_write(s2, W)),
        access(s1, C)[0],
        access(rate1)[0],
        step,
        REACH,
        LEVELS,
        place,
        last,
    )

    def share(levels, _):
        made = [shared_rows(lambda f, k=k: s2[f, k]) for k in levels]
        for k, (to_down, to_up) in zip(levels, made):
            for n in range(3):
                down[n, k] = to_down[n]
                up[n, k] = to_up[n]
        return 0

    sweep(0, LEVELS, 4, share)


class Whole:
    def rows(self, ref, field, l):
        return ref[field, l]

    sixteen = rows


SECTION = Whole()


def second_own(own, above, below, from_right, from_left, ext, flat, tracer):
    place_own(SECOND, (own, above, below, from_right, from_left), ext)
    flat_own(SECOND, ext, (PR,), flat)
    tiles, u, v = (lambda l, f=f: SECOND.rows(ext, f, l) for f in (C, U, V))

    def some(levels, _):
        results = [tracer_flat(tiles, u, v, l) for l in levels]
        for l, value in zip(levels, results):
            tracer[l - REACH] = value
        return 0

    sweep(REACH, LEVELS, 4, some)


def last_tracer(
    place_ref, dt_ref, ext_in, flat, flat_tracer, from_up, from_down, initial, *rest
):
    *chunks, ext, tracer, landed, fallen, rate, warm, factor, by_depth, sem = rest
    dt = dt_ref[0]
    copies, first = [], 0
    for n, chunk in enumerate(chunks):
        there = by_depth.at[pl.ds(first, chunk.shape[0])]
        copies.append(pltpu.make_async_copy(chunk, there, sem.at[n]))
        first += chunk.shape[0]
    for copy in copies:
        copy.start()
    place_halo(SECOND, from_up, from_down, ext, place_ref[0], place_ref[1])

    def write(n, l, value):
        rate[l] = value

    rates(SECOND, ext, (PR,), write, 3, 3, flat)

    def keep(levels, _):
        for l in levels:
            warm[l] = SECOND.rows(ext, C, l)
        return 0

    sweep(REACH - 4, LEVELS + 8, 4, keep)
    tiles = lambda l: SECOND.rows(ext, C, l)
    w = lambda l: SECOND.rows(ext, W, l)

    def some(levels, low):
        results = []
        for l in levels:
            high = tracer_high(tiles, w, l)
            tendency = (flat_tracer[l - REACH] + (high - low)) * SIXTIETH
            low = high
            c = initial[C, l - REACH] + dt * tendency
            grown = jnp.exp(growth * c)
            results.append((c, grown, grown * jnp.exp((0.5 * growth) * c)))
        for l, (c, second, third) in zip(levels, results):
            tracer[l - REACH] = c
            factor[0, l - REACH] = second
            factor[1, l - REACH] = third
        return low

    sweep(REACH, LEVELS, 4, some, tracer_high(tiles, w, REACH - 1))
    for copy in copies:
        copy.wait()
    for target in range(-FMAX, LEVELS):
        for moment in range(3):
            total = None
            for depth in range(FMAX + 1):
                k = target + depth
                if 0 <= k < LEVELS:
                    value = by_depth[k, depth, moment]
                    if moment:
                        value = value * factor[moment - 1, k]
                    total = value if total is None else total + value
            if target < 0:
                fallen[moment, target + FMAX] = total
            else:
                landed[moment, target] = total


def last_section(place_ref, dt_ref, rate, warm, start, tracer, out, fast):
    place, last = place_ref[0], place_ref[1]
    step = dt_ref[0] / NS
    out[C] = tracer[...]
    names = (PR, U, V, W)
    for repeat in range(NS):
        reads = [
            begin(start, f) if repeat == 0 else access(fast, n)[0] for n, f in enumerate(names)
        ]
        writes = [
            own_write(out, f) if repeat == NS - 1 else access(fast, n)[1]
            for n, f in enumerate(names)
        ]
        acoustic(
            *zip(reads, writes),
            access(warm)[0],
            access(rate)[0],
            step,
            REACH - 3 + repeat,
            LEVELS + 6 - 2 * repeat,
            place,
            last,
        )


def land(place_ref, landed, arrived, out):
    keep = jnp.where(place_ref[0] < place_ref[1], 1.0, 0.0).astype(F32)
    out[:, 0 : LEVELS - FMAX] = landed[:, 0 : LEVELS - FMAX]
    out[:, LEVELS - FMAX :] = landed[:, LEVELS - FMAX :] + keep * arrived[...]


def deposit(radius, weight, column, counts, fall_depth, out):
    slots, levels = radius.shape[0], radius.shape[1]
    target = lax.broadcasted_iota(jnp.int32, (COLS, COLS), 0)
    row = lax.broadcasted_iota(jnp.int32, (ROWS, COLS), 0)
    per_step = 4

    for k in range(levels):
        out[k] = jnp.zeros(out.shape[1:], F32)
        live = counts[k]

        def some(step, _, k=k, live=live):
            sums = [[None] * 3 for _ in range(FMAX + 1)]
            for part in range(per_step):
                s = step * per_step + part
                r = radius[s, k]
                number = jnp.where(s < live, weight[s, k], 0.0)
                area = number * r * r
                terms = []
                for t in (number, area, area * r):
                    high = t.astype(jnp.bfloat16).astype(F32)
                    terms += [high, t - high]
                cols = column[s, k]
                left, right = [], []
                for j in range(ROWS):
                    left.append(
                        jnp.concatenate([jnp.where(row == j, t, 0.0) for t in terms], axis=0)
                    )
                    right.append(jnp.where(cols[j : j + 1] == target, 1.0, 0.0).astype(F32))
                sent = lax.dot_general(
                    jnp.concatenate(left, axis=1),
                    jnp.concatenate(right, axis=1),
                    (((1,), (1,)), ((), ())),
                    preferred_element_type=F32,
                )
                depth = jnp.broadcast_to(fall_depth[s, k], (ROWS, COLS))
                for d in range(FMAX + 1):
                    falls = depth == d
                    for m in range(3):
                        both = sent[16 * m : 16 * m + 8] + sent[16 * m + 8 : 16 * m + 16]
                        value = jnp.where(falls, both, 0.0)
                        sums[d][m] = value if sums[d][m] is None else sums[d][m] + value
            for d in range(FMAX + 1):
                for m in range(3):
                    out[k, d, m] += sums[d][m]
            return 0

        lax.fori_loop(0, slots // per_step, some, 0)


def vmem(n):
    return [pl.BlockSpec(memory_space=pltpu.VMEM)] * n


def smem(n):
    return [pl.BlockSpec(memory_space=pltpu.SMEM)] * n


def far(n):
    return [pl.BlockSpec(memory_space=pltpu.HBM)] * n


def shaped(*dims):
    return jax.ShapeDtypeStruct(dims, F32)


def held(*dims):
    return pltpu.VMEM(dims, F32)


def call(kernel, name, ins, outs, scratch=(), out_specs=None, flops=None, grant=4, alias=None):
    made = pl.pallas_call(
        kernel,
        name=name,
        in_specs=ins,
        out_specs=tuple(out_specs or vmem(len(outs))),
        out_shape=tuple(outs),
        scratch_shapes=list(scratch),
        input_output_aliases=alias or {},
        compiler_params=pltpu.CompilerParams(vmem_limit_bytes=grant << 20),
        cost_estimate=(
            pl.CostEstimate(flops=flops, bytes_accessed=0, transcendentals=0) if flops else None
        ),
    )

    def run(*operands):
        return made(
            *(
                pltpu.with_memory_space_constraint(value, spec.memory_space)
                if spec.memory_space != pltpu.SMEM
                else value
                for spec, value in zip(ins, operands)
            )
        )

    return run


def both_ways(down, axis, up):
    count = lax.axis_size(axis)
    return (
        lax.ppermute(down, axis, [((i + 1) % count, i) for i in range(count)]),
        lax.ppermute(up, axis, [(i, (i + 1) % count) for i in range(count)]),
    )


def exchange(plan, own, down, up, tokens=(), speed=None):
    above, below = both_ways(down, GY, up)
    extra = [] if speed is None else [speed]
    to_left, to_right = call(
        pack_columns(plan, bool(extra)),
        "pack_columns",
        vmem(3 + len(extra)) + far(len(tokens)),
        [held(LEVELS, ROWS, COLS)] * 2,
    )(own, above, below, *extra, *tokens)
    from_right, from_left = both_ways(to_left, "gx", to_right)
    tiles = len(plan.carried)
    to_down, to_up, *speeds = call(
        pack_levels(plan, bool(extra)),
        "pack_levels",
        vmem(5 + len(extra)),
        [held(tiles, ROWS, COLS)] * 2 + [held(ROWS, COLS)] * len(extra),
    )(own, above, below, from_right, from_left, *extra)
    from_up, from_down = both_ways(to_down, "gz", to_up)
    return above, below, from_right, from_left, from_up, from_down, to_down, *speeds


def prepare(place_ref, fields, own, speed):
    own[...] = fields[...]
    keep = jnp.where(place_ref[0] == place_ref[1], 0.0, 1.0).astype(F32)
    most = jnp.zeros((ROWS, COLS), F32)
    for k in range(LEVELS):
        w = jnp.abs(fields[W, k])
        if k == LEVELS - 1:
            w = w * keep
        most = jnp.maximum(most, jnp.abs(fields[U, k]) + jnp.abs(fields[V, k]) + w)
    speed[...] = jnp.broadcast_to(jnp.max(most), speed.shape)


def droplets(radius, weight, column, counts, fall_depth, first, count, after):
    slots, step = radius.shape[0], 2
    counts, _ = lax.optimization_barrier((counts, after))
    whole = pl.BlockSpec((slots, step, ROWS, COLS), lambda i: (0, first // step + i, 0, 0))
    return pl.pallas_call(
        deposit,
        name="deposit",
        grid=(count // step,),
        in_specs=[
            whole,
            whole,
            whole,
            pl.BlockSpec((step, ROWS, COLS), lambda i: (first // step + i, 0, 0)),
            pl.BlockSpec((slots, step, ROWS, 1), lambda i: (0, first // step + i, 0, 0)),
        ],
        out_specs=pl.BlockSpec((step, FMAX + 1, 3, ROWS, COLS), lambda i: (i, 0, 0, 0, 0)),
        out_shape=pltpu.HBM((count, FMAX + 1, 3, ROWS, COLS), F32),
        compiler_params=pltpu.CompilerParams(vmem_limit_bytes=12 << 20),
        cost_estimate=pl.CostEstimate(
            flops=100_000_000 * count, bytes_accessed=0, transcendentals=0
        ),
    )(
        *(
            pltpu.with_memory_space_constraint(value, pltpu.HBM)
            for value in (radius, weight, column, counts)
        ),
        fall_depth,
    )


def per_device(fields, radius, weight, column, counts, fall_depth):
    place = lax.axis_index("gz")
    last = lax.axis_size("gz") - 1
    where = jnp.stack([place, jnp.int32(last)]).astype(jnp.int32)
    def drops(first, count, after):
        return droplets(radius, weight, column, counts, fall_depth, first, count, after)

    own, speed = pl.pallas_call(
        prepare,
        name="prepare",
        in_specs=smem(1) + vmem(1),
        out_specs=tuple(vmem(2)),
        out_shape=(held(5, LEVELS, ROWS, COLS), shaped(ROWS, COLS)),
        compiler_params=pltpu.CompilerParams(vmem_limit_bytes=4 << 20),
    )(where, fields)
    pair = [(i, i ^ 1) for i in range(lax.axis_size("gx"))]
    speed = jnp.maximum(speed, lax.ppermute(speed, "gx", pair))
    plane = ("gy_hi", "gz")
    early = drops(0, 8, speed)
    speed = jnp.broadcast_to(speed[0:1], (lax.axis_size(plane), 1, COLS))
    speed = jnp.max(lax.all_to_all(speed, plane, 0, 0), axis=0)
    *near, from_up, from_down, _, speed = exchange(FIRST, own, fields, fields, [early], speed)
    other_speed = lax.ppermute(speed, "gy_lo", [(0, 1), (1, 0)])
    ext = held(len(FIRST.tiles), DEPTH, ROWS, WIDE)
    start, flat = call(
        first_own,
        "first_own",
        smem(1) + vmem(5),
        [ext, held(2, LEVELS, 2 * ROWS, WIDE)],
    )(where, own, *near)
    start, s2, down, up, dt = call(
        two_sections,
        "two_sections",
        smem(1) + vmem(6),
        [ext, held(5, LEVELS, ROWS, COLS)] + [held(3, LEVELS, ROWS, COLS)] * 2 + [shaped(1)],
        scratch=[
            pltpu.VMEM((2, DEPTH, 2 * ROWS, WIDE), F32),
            pltpu.VMEM((5, DEPTH, 2 * ROWS, WIDE), F32),
            pltpu.VMEM((DEPTH, 2 * ROWS, WIDE), F32),
            pltpu.VMEM((4, DEPTH, 2 * ROWS, WIDE), F32),
        ],
        out_specs=vmem(4) + smem(1),
        grant=12,
        alias={3: 0},
    )(where, speed, other_speed, start, flat, from_up, from_down)
    middle = drops(8, 8, s2)
    *near, from_up, from_down, _ = exchange(SECOND, s2, down, up, [middle])
    by_depth = [early, middle]
    ext = held(len(SECOND.tiles), DEPTH, ROWS, WIDE)
    around_s2, flat, flat_tracer = call(
        second_own,
        "second_own",
        vmem(5),
        [ext, held(1, LEVELS, 2 * ROWS, WIDE), held(LEVELS, ROWS, COLS)],
        flops=1_000_000_000,
    )(s2, *near)
    rows = held(DEPTH, 2 * ROWS, WIDE)
    _, tracer, landed, fallen, rate, warm = call(
        last_tracer,
        "last_tracer",
        smem(2) + vmem(6) + far(len(by_depth)),
        [
            ext,
            held(LEVELS, ROWS, COLS),
            held(3, LEVELS, ROWS, COLS),
            held(3, FMAX, ROWS, COLS),
            rows,
            rows,
        ],
        scratch=[
            pltpu.VMEM((2, LEVELS, ROWS, COLS), F32),
            pltpu.VMEM((LEVELS, FMAX + 1, 3, ROWS, COLS), F32),
            pltpu.SemaphoreType.DMA((len(by_depth),)),
        ],
        alias={2: 0},
    )(where, dt, around_s2, flat, flat_tracer, from_up, from_down, own, *by_depth)
    count = lax.axis_size("gz")
    arrived = lax.ppermute(fallen, "gz", [((i + 1) % count, i) for i in range(count)])
    (new_fields,) = call(
        last_section,
        "last_section",
        smem(2) + vmem(4),
        [shaped(5, LEVELS, ROWS, COLS)],
        scratch=[pltpu.VMEM((4, DEPTH, 2 * ROWS, WIDE), F32)],
        flops=1_000_000_000,
    )(where, dt, rate, warm, start, tracer)
    (moments,) = call(
        land, "land", smem(1) + vmem(2), [shaped(3, LEVELS, ROWS, COLS)]
    )(where, landed, arrived)
    return (new_fields, moments)


def solution(mesh):
    count = mesh.shape["gy"]
    split = Mesh(
        mesh.devices.reshape(mesh.shape["gx"], count // 2, 2, mesh.shape["gz"]),
        ("gx", *GY, "gz"),
    )
    spread = P(None, "gz", GY, "gx")
    return jax.shard_map(
        per_device,
        mesh=split,
        in_specs=(spread, spread, spread, spread, P("gz", GY, "gx"), spread),
        out_specs=(spread, spread),
        check_vma=False,
    )
```
